8 devices in a mesh: dp: 1 (over z), sp: 8 (over y, x, core).
Axes of the slice: x: 2, y: 2, z: 1, core: 2. Of those that a mesh axis runs over, the one named last changes fastest.
Arguments:
- hidden_in: bfloat16 [8192, 1152], P(('dp', 'sp'))
- w_query: bfloat16 [1152, 4, 256], replicated
- w_key: bfloat16 [1152, 1, 256], replicated
- w_value: bfloat16 [1152, 1, 256], replicated
- w_out: bfloat16 [4, 256, 1152], replicated
- w_up: bfloat16 [1152, 6912], replicated
- w_down: bfloat16 [6912, 1152], replicated
- rel_bias: float32 [4, 1025], replicated
- glob_pos: int32 [256], P('dp')
Outputs:
- output 1: bfloat16 [8192, 1152], P(('dp', 'sp'))
- output 2: bfloat16 [256, 1152], P('dp')
All inputs are finite; a program needn't handle non-finite values.
Results may differ from the reference program's by a relative error of at most 0.00846168.
Values are sent between devices in bfloat16 or wider.
A program may use at most 1 GiB of HBM per device.

```python
import jax
import jax.numpy as jnp
from jax import lax

SEQ_LEN = 8192
MODEL_DIM = 1152
QUERY_HEADS = 4
KV_HEADS = 1
HEAD_DIM = 256
FFN_DIM = 6912
WINDOW = 512
GLOBAL_TOKENS = 256
ROW_SPAN = 1024


def draw_positions(key):
    inner = jax.random.permutation(key, SEQ_LEN - 2)[: GLOBAL_TOKENS - 2] + 1
    ends = jnp.array([0, SEQ_LEN - 1], dtype=jnp.int32)
    return jnp.sort(jnp.concatenate([ends, inner.astype(jnp.int32)]))


def setup_inputs(seed: int = 0, part: int = 0) -> dict:
    shared = jax.random.key(seed)
    part_key = jax.random.fold_in(shared, part)
    weight_keys = jax.random.split(shared, 8)
    qk_scale = 1.7 * MODEL_DIM ** -0.5
    hidden_in = jax.random.normal(jax.random.fold_in(part_key, 1), (SEQ_LEN, MODEL_DIM), jnp.float32)
    w_query = jax.random.normal(weight_keys[0], (MODEL_DIM, QUERY_HEADS, HEAD_DIM), jnp.float32) * qk_scale
    w_key = jax.random.normal(weight_keys[1], (MODEL_DIM, KV_HEADS, HEAD_DIM), jnp.float32) * qk_scale
    w_value = jax.random.normal(weight_keys[2], (MODEL_DIM, KV_HEADS, HEAD_DIM), jnp.float32) * MODEL_DIM ** -0.5
    w_out = jax.random.normal(weight_keys[3], (QUERY_HEADS, HEAD_DIM, MODEL_DIM), jnp.float32) * (QUERY_HEADS * HEAD_DIM) ** -0.5
    w_up = jax.random.normal(weight_keys[4], (MODEL_DIM, FFN_DIM), jnp.float32) * MODEL_DIM ** -0.5
    w_down = jax.random.normal(weight_keys[5], (FFN_DIM, MODEL_DIM), jnp.float32) * FFN_DIM ** -0.5
    rel_bias = jax.random.normal(weight_keys[6], (QUERY_HEADS, 2 * WINDOW + 1), jnp.float32)
    glob_pos = draw_positions(jax.random.fold_in(part_key, 2))
    return {
        'hidden_in': hidden_in.astype(jnp.bfloat16),
        'w_query': w_query.astype(jnp.bfloat16),
        'w_key': w_key.astype(jnp.bfloat16),
        'w_value': w_value.astype(jnp.bfloat16),
        'w_out': w_out.astype(jnp.bfloat16),
        'w_up': w_up.astype(jnp.bfloat16),
        'w_down': w_down.astype(jnp.bfloat16),
        'rel_bias': rel_bias,
        'glob_pos': glob_pos,
    }


def reference(hidden_in, w_query, w_key, w_value, w_out, w_up, w_down, rel_bias, glob_pos):
    group = QUERY_HEADS // KV_HEADS
    n_blocks = ROW_SPAN // WINDOW
    queries = (jnp.dot(hidden_in, w_query.reshape(MODEL_DIM, QUERY_HEADS * HEAD_DIM), preferred_element_type=jnp.float32) * HEAD_DIM ** -0.5).astype(jnp.bfloat16)
    keys_all = jnp.dot(hidden_in, w_key.reshape(MODEL_DIM, KV_HEADS * HEAD_DIM), preferred_element_type=jnp.float32).astype(jnp.bfloat16)
    vals_all = jnp.dot(hidden_in, w_value.reshape(MODEL_DIM, KV_HEADS * HEAD_DIM), preferred_element_type=jnp.float32).astype(jnp.bfloat16)
    queries = queries.reshape(SEQ_LEN, KV_HEADS, group, HEAD_DIM).astype(jnp.float32)
    keys_all = keys_all.reshape(SEQ_LEN, KV_HEADS, HEAD_DIM).astype(jnp.float32)
    vals_all = vals_all.reshape(SEQ_LEN, KV_HEADS, HEAD_DIM).astype(jnp.float32)
    glob_flag = jnp.zeros((SEQ_LEN,), jnp.int32).at[glob_pos].set(1)
    key_ok_pad = jnp.pad(1 - glob_flag, (WINDOW, WINDOW)) > 0
    keys_pad = jnp.pad(keys_all, ((WINDOW, WINDOW), (0, 0), (0, 0)))
    vals_pad = jnp.pad(vals_all, ((WINDOW, WINDOW), (0, 0), (0, 0)))
    key_glob = keys_all[glob_pos]
    val_glob = vals_all[glob_pos]
    row_idx = jnp.arange(WINDOW)[:, None]
    col_idx = jnp.arange(3 * WINDOW)[None, :]
    band = jnp.abs(col_idx - row_idx - WINDOW) <= WINDOW
    bias = jnp.take(rel_bias, jnp.clip(col_idx - row_idx, 0, 2 * WINDOW), axis=1).reshape(KV_HEADS, group, WINDOW, 3 * WINDOW)

    def three_blocks(ext):
        blocks = ext.reshape((n_blocks + 2, WINDOW) + ext.shape[1:])
        return jnp.concatenate([blocks[:-2], blocks[1:-1], blocks[2:]], axis=1)

    def span_attention(start):
        query_blk = lax.dynamic_slice_in_dim(queries, start, ROW_SPAN, 0).reshape(n_blocks, WINDOW, KV_HEADS, group, HEAD_DIM)
        key_win = three_blocks(lax.dynamic_slice_in_dim(keys_pad, start, ROW_SPAN + 2 * WINDOW, 0))
        val_win = three_blocks(lax.dynamic_slice_in_dim(vals_pad, start, ROW_SPAN + 2 * WINDOW, 0))
        ok_win = three_blocks(lax.dynamic_slice_in_dim(key_ok_pad, start, ROW_SPAN + 2 * WINDOW, 0))
        mask = band & ok_win[:, None, None, None, :]
        score_win = jnp.where(mask, jnp.einsum('bqgrd,bkgd->bgrqk', query_blk, key_win) + bias, -1e30)
        score_glob = jnp.einsum('bqgrd,ngd->bgrqn', query_blk, key_glob)
        top = jnp.maximum(score_win.max(-1), score_glob.max(-1))[..., None]
        prob_win = jnp.exp(score_win - top)
        prob_glob = jnp.exp(score_glob - top)
        norm_sum = prob_win.sum(-1) + prob_glob.sum(-1)
        weighted = jnp.einsum('bgrqk,bkgd->bgrqd', prob_win.astype(jnp.bfloat16).astype(jnp.float32), val_win)
        weighted = weighted + jnp.einsum('bgrqn,ngd->bgrqd', prob_glob.astype(jnp.bfloat16).astype(jnp.float32), val_glob)
        result = weighted / norm_sum[..., None]
        return jnp.transpose(result, (0, 3, 1, 2, 4)).reshape(ROW_SPAN, QUERY_HEADS * HEAD_DIM)

    starts = jnp.arange(SEQ_LEN // ROW_SPAN) * ROW_SPAN
    attended = lax.map(span_attention, starts).reshape(SEQ_LEN, QUERY_HEADS * HEAD_DIM)
    query_glob = queries[glob_pos]
    score_full = jnp.einsum('ngrd,tgd->ngrt', query_glob, keys_all)
    prob_full = jnp.exp(score_full - score_full.max(-1, keepdims=True))
    out_glob = jnp.einsum('ngrt,tgd->ngrd', prob_full.astype(jnp.bfloat16).astype(jnp.float32), vals_all) / prob_full.sum(-1)[..., None]
    attended = attended.at[glob_pos].set(out_glob.reshape(GLOBAL_TOKENS, QUERY_HEADS * HEAD_DIM)).astype(jnp.bfloat16)
    hidden = (hidden_in.astype(jnp.float32) + jnp.dot(attended, w_out.reshape(QUERY_HEADS * HEAD_DIM, MODEL_DIM), preferred_element_type=jnp.float32)).astype(jnp.bfloat16)
    upper = jax.nn.gelu(jnp.dot(hidden, w_up, preferred_element_type=jnp.float32)).astype(jnp.bfloat16)
    y_out = (hidden.astype(jnp.float32) + jnp.dot(upper, w_down, preferred_element_type=jnp.float32)).astype(jnp.bfloat16)
    return y_out, y_out[glob_pos]
```

```python
import functools
import math

import jax
import jax.numpy as jnp
from jax import lax
from jax.experimental import pallas as pl
from jax.experimental.pallas import tpu as pltpu
from jax.sharding import PartitionSpec as P

BF16 = jnp.bfloat16
F32 = jnp.float32
NEG = -math.inf
BLK = 256


def mm(a, b):
    return jnp.dot(a, b, preferred_element_type=F32)


def mm_nt(a, b):
    return lax.dot_general(a, b, (((1,), (1,)), ((), ())), preferred_element_type=F32)


def remote(src, dst, send, recv, dev):
    return pltpu.make_async_remote_copy(
        src_ref=src, dst_ref=dst, send_sem=send, recv_sem=recv,
        device_id={'sp': dev}, device_id_type=pl.DeviceIdType.MESH)


def entry_barrier(me, n_dev):
    barrier = pltpu.get_barrier_semaphore()
    for k in range(1, n_dev):
        pl.semaphore_signal(barrier, inc=1, device_id={'sp': lax.rem(me + k, n_dev)}, device_id_type=pl.DeviceIdType.MESH)
    pl.semaphore_wait(barrier, n_dev - 1)


def to_column(row):
    n = row.shape[1]
    wide = jnp.broadcast_to(row.astype(F32), (n, n))
    diag = lax.broadcasted_iota(jnp.int32, (n, n), 0) == lax.broadcasted_iota(jnp.int32, (n, n), 1)
    return jnp.sum(jnp.where(diag, wide, 0.0), axis=1, keepdims=True).astype(jnp.int32)


def front_kernel(n_dev, heads, width,
                 x_hbm, wq_hbm, wk_hbm, wv_hbm, wo_hbm, rb_ref, gp_ref, hid_ref,
                 x_s, wq_s, wk_s, wv_s, wo_s, q_s, kv_s, kvl_s, kvr_s, bias_s, row_s, mask_s,
                 xg_send, xg_recv, xg_all, qg_s, kvg_s, o_s, m_s, l_s, att_s, rs_send, rs_recv,
                 in_sem, x1_send, x1_recv, x2_send, x2_recv, halo_send, halo_recv, rs_ssem, rs_rsem):
    rows, dim = x_s.shape
    head = wk_s.shape[1]
    n_glob = gp_ref.shape[1]
    per = n_glob // n_dev
    n_blk = rows // BLK
    ext = BLK + 2 * width
    me = lax.axis_index('sp')
    start = me * rows

    loads = [pltpu.make_async_copy(src, dst, in_sem.at[i]) for i, (src, dst) in enumerate(
        [(x_hbm, x_s), (wk_hbm, wk_s), (wv_hbm, wv_s), (wq_hbm, wq_s), (wo_hbm, wo_s)])]
    for c in loads:
        c.start()
    entry_barrier(me, n_dev)

    gp_row = gp_ref[...]
    gp_col = to_column(gp_row)
    loads[0].wait()
    x = x_s[...]

    own = gp_col == start + lax.broadcasted_iota(jnp.int32, (n_glob, rows), 1)
    xg_send[...] = mm(own.astype(F32).astype(BF16), x).astype(BF16)
    x1 = []
    for k in range(1, n_dev):
        peer = lax.rem(me + k, n_dev)
        c = remote(xg_send.at[pl.ds(peer * per, per)], xg_recv.at[k], x1_send.at[k], x1_recv.at[k], peer)
        c.start()
        x1.append(c)

    loads[1].wait()
    loads[2].wait()
    kv_s[:, :head] = mm(x, wk_s[...]).astype(BF16)
    kv_s[:, head:] = mm(x, wv_s[...]).astype(BF16)

    to_right = remote(kv_s.at[pl.ds(rows - width, width)], kvl_s, halo_send.at[0], halo_recv.at[0], lax.rem(me + 1, n_dev))
    to_left = remote(kv_s.at[pl.ds(0, width)], kvr_s, halo_send.at[1], halo_recv.at[1], lax.rem(me + n_dev - 1, n_dev))

    @pl.when(me < n_dev - 1)
    def _():
        to_right.start()

    @pl.when(me > 0)
    def _():
        to_left.start()

    @pl.when(me == 0)
    def _():
        kvl_s[...] = jnp.zeros_like(kvl_s)

    @pl.when(me == n_dev - 1)
    def _():
        kvr_s[...] = jnp.zeros_like(kvr_s)

    loads[3].wait()
    for h in range(heads):
        qh = (mm(x, wq_s[:, h * head:(h + 1) * head]) * head ** -0.5).astype(BF16)
        for b in range(n_blk):
            q_s[b, h * BLK:(h + 1) * BLK, :] = qh[b * BLK:(b + 1) * BLK]

    pos = start - width + lax.broadcasted_iota(jnp.int32, (1, rows + 2 * width), 1)
    hit = jnp.max((gp_col == pos).astype(F32), axis=0, keepdims=True) > 0.0
    bad = hit | (pos < 0) | (pos >= rows * n_dev)
    mask_s[...] = jnp.broadcast_to(jnp.where(bad, NEG, 0.0), mask_s.shape)

    row_s[...] = jnp.full(row_s.shape, NEG, F32)
    row_s[:heads, :2 * width] = rb_ref[:, :2 * width]
    last = jnp.broadcast_to(rb_ref[:, 2 * width:], (heads, 128))
    row_s[:heads, 2 * width:2 * width + 128] = jnp.where(lax.broadcasted_iota(jnp.int32, (heads, 128), 1) == 0, last, NEG)
    for h in range(heads):
        wide = jnp.broadcast_to(row_s[h:h + 1, :], (BLK, ext))
        bias_s[h * BLK:(h + 1) * BLK, :] = pltpu.roll(wide, 0, 1, stride=1, stride_axis=0)

    def local_part(b):
        lo = max(0, b * BLK - width)
        hi = min(rows, (b + 1) * BLK + width)
        c0 = lo - b * BLK + width
        for h in range(heads):
            rs = slice(h * BLK, (h + 1) * BLK)
            s = mm_nt(q_s[b, rs, :], kv_s[lo:hi, :head])
            s = s + bias_s[rs, c0:c0 + hi - lo] + mask_s[0:1, width + lo:width + hi]
            top = jnp.max(s, axis=1, keepdims=True)
            p = jnp.exp(s - top)
            l_s[b, rs, :] = jnp.broadcast_to(jnp.sum(p, axis=1, keepdims=True), (BLK, 128))
            m_s[b, rs, :] = jnp.broadcast_to(top, (BLK, 128))
            o_s[b, rs, :] = mm(p.astype(BF16), kv_s[lo:hi, head:])

    def far_part(b):
        if b * BLK < width:
            ref, lo, hi, c0 = kvl_s, b * BLK, width, 0
            mask0 = lo
        else:
            ref, lo, hi = kvr_s, 0, (b + 1) * BLK + width - rows
            c0 = ext - hi
            mask0 = width + rows
        for h in range(heads):
            rs = slice(h * BLK, (h + 1) * BLK)
            q = q_s[b, rs, :]
            sw = mm_nt(q, ref[lo:hi, :head])
            sw = sw + bias_s[rs, c0:c0 + hi - lo] + mask_s[0:1, mask0:mask0 + hi - lo]
            sg = mm_nt(q, kvg_s[:, :head])
            m1 = m_s[b, rs, 0:1]
            top = jnp.maximum(m1, jnp.maximum(jnp.max(sw, axis=1, keepdims=True), jnp.max(sg, axis=1, keepdims=True)))
            pw = jnp.exp(sw - top)
            pg = jnp.exp(sg - top)
            fac = jnp.exp(m1 - top)
            tot = l_s[b, rs, 0:1] * fac + jnp.sum(pw, axis=1, keepdims=True) + jnp.sum(pg, axis=1, keepdims=True)
            o = o_s[b, rs, :] * fac + mm(pw.astype(BF16), ref[lo:hi, head:]) + mm(pg.astype(BF16), kvg_s[:, head:])
            att_s[b * BLK:(b + 1) * BLK, h * head:(h + 1) * head] = (o / tot).astype(BF16)

    local_part(0)
    local_part(1)

    for c in x1:
        c.wait_recv()
    acc = xg_send[pl.ds(me * per, per), :].astype(F32)
    for k in range(1, n_dev):
        acc = acc + xg_recv[k].astype(F32)
    xg_all[pl.ds(me * per, per), :] = acc.astype(BF16)
    x2 = []
    for k in range(1, n_dev):
        peer = lax.rem(me + k, n_dev)
        mine = xg_all.at[pl.ds(me * per, per)]
        c = remote(mine, mine, x2_send.at[k], x2_recv.at[k], peer)
        c.start()
        x2.append(c)

    local_part(2)
    local_part(3)

    for k in range(1, n_dev):
        src = lax.rem(me + n_dev - k, n_dev)
        got = xg_all.at[pl.ds(src * per, per)]
        remote(got, got, x2_send.at[k], x2_recv.at[k], src).wait_recv()
    xg = xg_all[...]
    kvg_s[:, :head] = mm(xg, wk_s[...]).astype(BF16)
    kvg_s[:, head:] = mm(xg, wv_s[...]).astype(BF16)
    for h in range(heads):
        qh = (mm(xg, wq_s[:, h * head:(h + 1) * head]) * head ** -0.5).astype(BF16)
        for j in range(n_dev):
            at = (j * heads + h) * per
            qg_s[at:at + per, :] = qh[j * per:(j + 1) * per]

    slab = heads * per
    for r in range(0, n_dev * slab, BLK):
        s = mm_nt(qg_s[r:r + BLK, :], kv_s[:, :head])
        top = jnp.max(s, axis=1, keepdims=True)
        p = jnp.exp(s - top)
        tot = jnp.sum(p, axis=1, keepdims=True)
        rs_send[r:r + BLK, :head] = mm(p.astype(BF16), kv_s[:, head:])
        lane = lax.broadcasted_iota(jnp.int32, (BLK, 128), 1)
        rs_send[r:r + BLK, head:] = jnp.where(lane < 64, top, tot)
    rs = []
    for k in range(1, n_dev):
        peer = lax.rem(me + k, n_dev)
        c = remote(rs_send.at[pl.ds(peer * slab, slab)], rs_recv.at[k], rs_ssem.at[k], rs_rsem.at[k], peer)
        c.start()
        rs.append(c)

    @pl.when(me > 0)
    def _():
        to_right.wait_recv()

    @pl.when(me < n_dev - 1)
    def _():
        to_left.wait_recv()

    for b in range(n_blk):
        far_part(b)

    loads[4].wait()
    for b in range(n_blk):
        r = slice(b * BLK, (b + 1) * BLK)
        hid_ref[r, :] = (x_s[r, :].astype(F32) + mm(att_s[r, :], wo_s[...])).astype(BF16)

    for c in rs:
        c.wait_recv()
    rs_recv[0] = rs_send[pl.ds(me * slab, slab), :]
    top = rs_recv[0, :, head:head + 1]
    for k in range(1, n_dev):
        top = jnp.maximum(top, rs_recv[k, :, head:head + 1])
    tot = jnp.zeros((slab, 1), F32)
    o = jnp.zeros((slab, head), F32)
    for k in range(n_dev):
        fac = jnp.exp(rs_recv[k, :, head:head + 1] - top)
        tot = tot + rs_recv[k, :, head + 64:head + 65] * fac
        o = o + rs_recv[k, :, :head] * fac
    o = (o / tot).astype(BF16)
    hg = xg_all[pl.ds(me * per, per), :].astype(F32)
    for h in range(heads):
        hg = hg + mm(o[h * per:(h + 1) * per], wo_s[h * head:(h + 1) * head, :])
    hid_ref[rows:, :] = hg.astype(BF16)

    for c in x1 + x2 + rs:
        c.wait_send()

    @pl.when(me < n_dev - 1)
    def _():
        to_right.wait_send()

    @pl.when(me > 0)
    def _():
        to_left.wait_send()


def front(x, wq, wk, wv, wo, rel_bias, gp, n_dev, heads):
    rows, dim = x.shape
    head = wk.shape[1]
    width = (rel_bias.shape[1] - 1) // 2
    n_glob = gp.shape[1]
    per = n_glob // n_dev
    n_blk = rows // BLK
    slab = heads * per
    any_spec = pl.BlockSpec(memory_space=pl.ANY)
    vmem_spec = pl.BlockSpec(memory_space=pltpu.VMEM)
    dma = pltpu.SemaphoreType.DMA
    return pl.pallas_call(
        functools.partial(front_kernel, n_dev, heads, width),
        name='front',
        out_shape=jax.ShapeDtypeStruct((rows + per, dim), BF16),
        in_specs=[any_spec] * 5 + [vmem_spec] * 2,
        out_specs=vmem_spec,
        scratch_shapes=[
            pltpu.VMEM(x.shape, BF16), pltpu.VMEM(wq.shape, BF16), pltpu.VMEM(wk.shape, BF16),
            pltpu.VMEM(wv.shape, BF16), pltpu.VMEM(wo.shape, BF16),
            pltpu.VMEM((n_blk, heads * BLK, head), BF16),
            pltpu.VMEM((rows, 2 * head), BF16), pltpu.VMEM((width, 2 * head), BF16), pltpu.VMEM((width, 2 * head), BF16),
            pltpu.VMEM((heads * BLK, BLK + 2 * width), F32), pltpu.VMEM((8, BLK + 2 * width), F32),
            pltpu.VMEM((8, rows + 2 * width), F32),
            pltpu.VMEM((n_glob, dim), BF16), pltpu.VMEM((n_dev, per, dim), BF16), pltpu.VMEM((n_glob, dim), BF16),
            pltpu.VMEM((n_dev * slab, head), BF16), pltpu.VMEM((n_glob, 2 * head), BF16),
            pltpu.VMEM((n_blk, heads * BLK, head), F32), pltpu.VMEM((n_blk, heads * BLK, 128), F32),
            pltpu.VMEM((n_blk, heads * BLK, 128), F32),
            pltpu.VMEM((rows, heads * head), BF16),
            pltpu.VMEM((n_dev * slab, head + 128), F32), pltpu.VMEM((n_dev, slab, head + 128), F32),
            dma((5,)), dma((n_dev,)), dma((n_dev,)), dma((n_dev,)), dma((n_dev,)), dma((2,)), dma((2,)), dma((n_dev,)), dma((n_dev,)),
        ],
        compiler_params=pltpu.CompilerParams(collective_id=0, has_side_effects=True, vmem_limit_bytes=62 << 20),
    )(x, wq, wk, wv, wo, rel_bias, gp)


def ffn_kernel(n_dev, rows, hid_ref, w1_ref, w2_ref, gp_ref, y_ref, yg_ref, acc_s, send_s, yg_s, u_s, ssem, rsem):
    step = pl.program_id(0)
    total = hid_ref.shape[0]
    n_glob = gp_ref.shape[1]
    per = n_glob // n_dev
    me = lax.axis_index('sp')
    tile = w1_ref.shape[1]

    @pl.when(step == 0)
    def _():
        entry_barrier(me, n_dev)
        acc_s[...] = hid_ref[...].astype(F32)

    for c in range(0, tile, BLK):
        u_s[:, c:c + BLK] = jax.nn.gelu(mm(hid_ref[...], w1_ref[:, c:c + BLK]), approximate=True).astype(BF16)
    acc_s[...] += mm(u_s[...], w2_ref[...])

    @pl.when(step == pl.num_programs(0) - 1)
    def _():
        send_s[...] = acc_s[rows:, :].astype(BF16)
        copies = []
        for k in range(1, n_dev):
            peer = lax.rem(me + k, n_dev)
            c = remote(send_s, yg_s.at[pl.ds(me * per, per)], ssem.at[k], rsem.at[k], peer)
            c.start()
            copies.append(c)
        yg_s[pl.ds(me * per, per), :] = send_s[...]
        for k in range(1, n_dev):
            src = lax.rem(me + n_dev - k, n_dev)
            remote(send_s, yg_s.at[pl.ds(src * per, per)], ssem.at[k], rsem.at[k], src).wait_recv()
        yg_ref[...] = yg_s[...]
        gp = gp_ref[...]
        for r in range(0, rows, BLK):
            hit = gp == me * rows + r + lax.broadcasted_iota(jnp.int32, (BLK, n_glob), 0)
            sel = hit.astype(F32)
            placed = mm(sel.astype(BF16), yg_s[...])
            is_glob = jnp.max(sel, axis=1, keepdims=True) > 0.0
            y_ref[r:r + BLK, :] = jnp.where(is_glob, placed, acc_s[r:r + BLK, :]).astype(BF16)
        for c in copies:
            c.wait_send()


def ffn(hid, w1, w2, gp, rows, n_dev, tile):
    total, dim = hid.shape
    wide = w1.shape[1]
    n_glob = gp.shape[1]
    dma = pltpu.SemaphoreType.DMA
    return pl.pallas_call(
        functools.partial(ffn_kernel, n_dev, rows),
        name='ffn',
        grid=(wide // tile,),
        out_shape=(jax.ShapeDtypeStruct((rows, dim), BF16), jax.ShapeDtypeStruct((n_glob, dim), BF16)),
        in_specs=[pl.BlockSpec((total, dim), lambda i: (0, 0)), pl.BlockSpec((dim, tile), lambda i: (0, i)),
                  pl.BlockSpec((tile, dim), lambda i: (i, 0)), pl.BlockSpec((1, n_glob), lambda i: (0, 0))],
        out_specs=(pl.BlockSpec(memory_space=pltpu.VMEM), pl.BlockSpec(memory_space=pltpu.VMEM)),
        scratch_shapes=[pltpu.VMEM((total, dim), F32), pltpu.VMEM((n_glob // n_dev, dim), BF16),
                        pltpu.VMEM((n_glob, dim), BF16), pltpu.VMEM((total, tile), BF16), dma((n_dev,)), dma((n_dev,))],
        compiler_params=pltpu.CompilerParams(
            dimension_semantics=('arbitrary',), collective_id=1, has_side_effects=True, vmem_limit_bytes=60 << 20),
    )(hid, w1, w2, gp)


def solution(mesh):
    n_dev = mesh.shape['sp']

    def shard_layer(hidden_in, w_query, w_key, w_value, w_out, w_up, w_down, rel_bias, glob_pos):
        rows, dim = hidden_in.shape
        heads, head = w_query.shape[1], w_query.shape[2]
        gp = glob_pos.reshape(1, -1)
        hid = front(hidden_in, w_query.reshape(dim, heads * head), w_key.reshape(dim, head), w_value.reshape(dim, head),
                    w_out.reshape(heads * head, dim), rel_bias, gp, n_dev, heads)
        return ffn(hid, w_up, w_down, gp, rows, n_dev, 768)

    return jax.shard_map(
        shard_layer, mesh=mesh,
        in_specs=(P(('dp', 'sp'), None), P(), P(), P(), P(), P(), P(), P(), P('dp')),
        out_specs=(P(('dp', 'sp'), None), P('dp', None)),
        check_vma=False)
```

```python
import functools
import math

import jax
import jax.numpy as jnp
from jax import lax
from jax.experimental import pallas as pl
from jax.experimental.pallas import tpu as pltpu
from jax.sharding import PartitionSpec as P

BF16 = jnp.bfloat16
F32 = jnp.float32
NEG = -math.inf
BLK = 256


def mm(a, b):
    return jnp.dot(a, b, preferred_element_type=F32)


def mm_nt(a, b):
    return lax.dot_general(a, b, (((1,), (1,)), ((), ())), preferred_element_type=F32)


def remote(src, dst, send, recv, dev):
    return pltpu.make_async_remote_copy(
        src_ref=src, dst_ref=dst, send_sem=send, recv_sem=recv,
        device_id={'sp': dev}, device_id_type=pl.DeviceIdType.MESH)


def entry_barrier(me, n_dev):
    barrier = pltpu.get_barrier_semaphore()
    for k in range(1, n_dev):
        pl.semaphore_signal(barrier, inc=1, device_id={'sp': lax.rem(me + k, n_dev)}, device_id_type=pl.DeviceIdType.MESH)
    pl.semaphore_wait(barrier, n_dev - 1)


def diagonal(n):
    return lax.broadcasted_iota(jnp.int32, (n, n), 0) == lax.broadcasted_iota(jnp.int32, (n, n), 1)


def row_to_column(row):
    n = row.shape[1]
    return jnp.sum(jnp.where(diagonal(n), jnp.broadcast_to(row, (n, n)), 0.0), axis=1, keepdims=True)


def column_to_row(col):
    n = col.shape[0]
    return jnp.sum(jnp.where(diagonal(n), jnp.broadcast_to(col, (n, n)), 0.0), axis=0, keepdims=True)


def front_kernel(n_dev, heads, width,
                 x_hbm, wq_hbm, wk_hbm, wv_hbm, wo_hbm, rb_ref, gp_ref, hid_ref,
                 x_s, wq_s, wk_s, wv_s, wo_s, q_s, kv_s, halo_s, bias_s, row_s, mask_s,
                 xg_send, xp_recv, xh_s, xa_recv, xh2_s, xb_recv, xg_all, qg_s, kvg_s, o_s, m_s, l_s, att_s,
                 rs_send, rs_recv, st_send, st_recv,
                 in_sem, x_ssem, x_rsem, halo_send, halo_recv, rs_ssem, rs_rsem, st_ssem, st_rsem):
    rows, dim = x_s.shape
    head = wk_s.shape[1]
    n_glob = gp_ref.shape[1]
    per = n_glob // n_dev
    n_blk = rows // BLK
    ext = BLK + 2 * width
    me = lax.axis_index('sp')
    start = me * rows
    core = lax.rem(me, 2)
    chip = me // 2
    partner = me + 1 - 2 * core
    x_peer = 2 * (chip + 1 - 2 * lax.rem(chip, 2)) + core
    y_peer = 2 * lax.rem(chip + 2, 4) + core
    half = n_glob // 2
    quart = n_glob // 4

    loads = [pltpu.make_async_copy(src, dst, in_sem.at[i]) for i, (src, dst) in enumerate(
        [(x_hbm, x_s), (wk_hbm, wk_s), (wv_hbm, wv_s), (wq_hbm, wq_s), (wo_hbm, wo_s)])]
    for c in loads:
        c.start()
    entry_barrier(me, n_dev)

    gp_row = gp_ref[...]
    gp_col = row_to_column(gp_row.astype(F32)).astype(jnp.int32)
    loads[0].wait()
    x = x_s[...]

    own = gp_col == start + lax.broadcasted_iota(jnp.int32, (n_glob, rows), 1)
    xg_send[...] = mm(own.astype(F32).astype(BF16), x).astype(BF16)
    pair = remote(xg_send.at[pl.ds((1 - core) * half, half)], xp_recv, x_ssem.at[0], x_rsem.at[0], partner)
    pair.start()

    loads[1].wait()
    loads[2].wait()
    kv_s[:, :head] = mm(x, wk_s[...]).astype(BF16)
    kv_s[:, head:] = mm(x, wv_s[...]).astype(BF16)

    near, far = 1 - core, core
    has_far = (me > 0) & (me < n_dev - 1)
    to_near = remote(kv_s.at[pl.ds(near * width, width)], halo_s.at[core], halo_send.at[0], halo_recv.at[0], partner)
    to_far = remote(kv_s.at[pl.ds(far * width, width)], halo_s.at[1 - core], halo_send.at[1], halo_recv.at[1],
                    lax.rem(me + n_dev - 1 + 2 * core, n_dev))
    to_near.start()

    pair.wait_recv()
    xh_s[...] = (xg_send[pl.ds(core * half, half), :].astype(F32) + xp_recv[...].astype(F32)).astype(BF16)
    swap = [remote(xh_s.at[pl.ds(0, quart)], xa_recv.at[0], x_ssem.at[1], x_rsem.at[1], x_peer),
            remote(xh_s.at[pl.ds(quart, quart)], xa_recv.at[1], x_ssem.at[2], x_rsem.at[2], y_peer)]
    for c in swap:
        c.start()

    loads[3].wait()
    for h in range(heads):
        qh = (mm(x, wq_s[:, h * head:(h + 1) * head]) * head ** -0.5).astype(BF16)
        for b in range(n_blk):
            q_s[b, h * BLK:(h + 1) * BLK, :] = qh[b * BLK:(b + 1) * BLK]

    pos = start - width + lax.broadcasted_iota(jnp.int32, (1, rows + 2 * width), 1)
    hit = jnp.max((gp_col == pos).astype(F32), axis=0, keepdims=True) > 0.0
    bad = hit | (pos < 0) | (pos >= rows * n_dev)
    mask_s[...] = jnp.broadcast_to(jnp.where(bad, NEG, 0.0), mask_s.shape)

    row_s[...] = jnp.full(row_s.shape, NEG, F32)
    row_s[:heads, :2 * width] = rb_ref[:, :2 * width]
    last = jnp.broadcast_to(rb_ref[:, 2 * width:], (heads, 128))
    row_s[:heads, 2 * width:2 * width + 128] = jnp.where(lax.broadcasted_iota(jnp.int32, (heads, 128), 1) == 0, last, NEG)
    for h in range(heads):
        wide = jnp.broadcast_to(row_s[h:h + 1, :], (BLK, ext))
        bias_s[h * BLK:(h + 1) * BLK, :] = pltpu.roll(wide, 0, 1, stride=1, stride_axis=0)

    def local_part(b):
        lo = max(0, b * BLK - width)
        hi = min(rows, (b + 1) * BLK + width)
        c0 = lo - b * BLK + width
        for h in range(heads):
            rs = slice(h * BLK, (h + 1) * BLK)
            s = mm_nt(q_s[b, rs, :], kv_s[lo:hi, :head])
            s = s + bias_s[rs, c0:c0 + hi - lo] + mask_s[0:1, width + lo:width + hi]
            top = jnp.max(s, axis=1, keepdims=True)
            p = jnp.exp(s - top)
            l_s[b, rs, :] = jnp.broadcast_to(jnp.sum(p, axis=1, keepdims=True), (BLK, 128))
            m_s[b, rs, :] = jnp.broadcast_to(top, (BLK, 128))
            o_s[b, rs, :] = mm(p.astype(BF16), kv_s[lo:hi, head:])

    def far_part(side, n_keys):
        if n_keys == width:
            b, key0 = side * (n_blk - 1), 0
            mask0 = side * (width + rows)
        else:
            b, key0 = 1 + side * (n_blk - 3), (1 - side) * BLK
            mask0 = side * (width + rows) + key0
        c0 = side * (ext - n_keys)
        keys = pl.ds(pl.multiple_of(key0, BLK), n_keys)
        for h in range(heads):
            rs = slice(h * BLK, (h + 1) * BLK)
            q = q_s[b, rs, :]
            sw = mm_nt(q, halo_s[side, keys, :head])
            sw = sw + bias_s[rs, pl.ds(pl.multiple_of(c0, BLK), n_keys)] + mask_s[0:1, pl.ds(pl.multiple_of(mask0, BLK), n_keys)]
            sg = mm_nt(q, kvg_s[:, :head])
            m1 = m_s[b, rs, 0:1]
            top = jnp.maximum(m1, jnp.maximum(jnp.max(sw, axis=1, keepdims=True), jnp.max(sg, axis=1, keepdims=True)))
            pw = jnp.exp(sw - top)
            pg = jnp.exp(sg - top)
            fac = jnp.exp(m1 - top)
            tot = l_s[b, rs, 0:1] * fac + jnp.sum(pw, axis=1, keepdims=True) + jnp.sum(pg, axis=1, keepdims=True)
            o = o_s[b, rs, :] * fac + mm(pw.astype(BF16), halo_s[side, keys, head:]) + mm(pg.astype(BF16), kvg_s[:, head:])
            att_s[pl.ds(pl.multiple_of(b * BLK, BLK), BLK), h * head:(h + 1) * head] = (o / tot).astype(BF16)

    local_part(0)

    for c in swap:
        c.wait_recv()
    xh2_s[:quart, :] = (xh_s[:quart, :].astype(F32) + xa_recv[0].astype(F32)).astype(BF16)
    xh2_s[quart:, :] = (xh_s[quart:, :].astype(F32) + xa_recv[1].astype(F32)).astype(BF16)
    swap2 = [remote(xh2_s.at[pl.ds(0, quart)], xb_recv.at[0], x_ssem.at[3], x_rsem.at[3], y_peer),
             remote(xh2_s.at[pl.ds(quart, quart)], xb_recv.at[1], x_ssem.at[4], x_rsem.at[4], x_peer)]
    for c in swap2:
        c.start()

    @pl.when(has_far)
    def _():
        to_far.start()

    @pl.when(jnp.logical_not(has_far))
    def _():
        halo_s[core] = jnp.zeros(halo_s.shape[1:], BF16)

    local_part(1)
    local_part(2)

    for c in swap2:
        c.wait_recv()
    mine = core * half
    xg_all[pl.ds(mine, quart), :] = (xh2_s[:quart, :].astype(F32) + xb_recv[0].astype(F32)).astype(BF16)
    xg_all[pl.ds(mine + quart, quart), :] = (xh2_s[quart:, :].astype(F32) + xb_recv[1].astype(F32)).astype(BF16)
    spread = remote(xg_all.at[pl.ds(mine, half)], xg_all.at[pl.ds(mine, half)], x_ssem.at[5], x_rsem.at[5], partner)
    spread.start()

    local_part(3)

    remote(xg_all.at[pl.ds(half - mine, half)], xg_all.at[pl.ds(half - mine, half)], x_ssem.at[5], x_rsem.at[5], partner).wait_recv()
    xg = xg_all[...]
    kvg_s[:, :head] = mm(xg, wk_s[...]).astype(BF16)
    kvg_s[:, head:] = mm(xg, wv_s[...]).astype(BF16)
    for h in range(heads):
        qh = (mm(xg, wq_s[:, h * head:(h + 1) * head]) * head ** -0.5).astype(BF16)
        for j in range(n_dev):
            at = (j * heads + h) * per
            qg_s[at:at + per, :] = qh[j * per:(j + 1) * per]

    slab = heads * per
    for r in range(0, n_dev * slab, BLK):
        s = mm_nt(qg_s[r:r + BLK, :], kv_s[:, :head])
        top = jnp.max(s, axis=1, keepdims=True)
        p = jnp.exp(s - top)
        tot = jnp.sum(p, axis=1, keepdims=True)
        rs_send[r:r + BLK, :] = mm(p.astype(BF16), kv_s[:, head:])
        for j in range(BLK // slab):
            cut = slice(j * slab, (j + 1) * slab)
            st_send[r // slab + j, 0:1, :] = column_to_row(top[cut])
            st_send[r // slab + j, 1:2, :] = column_to_row(tot[cut])
    rs = []
    for k in range(1, n_dev):
        peer = lax.rem(me + k, n_dev)
        c = remote(rs_send.at[pl.ds(peer * slab, slab)], rs_recv.at[k], rs_ssem.at[k], rs_rsem.at[k], peer)
        c.start()
        rs.append(c)
        c = remote(st_send.at[peer], st_recv.at[k], st_ssem.at[k], st_rsem.at[k], peer)
        c.start()
        rs.append(c)

    to_near.wait_recv()
    far_part(near, width)
    far_part(near, width // 2)

    @pl.when(has_far)
    def _():
        to_far.wait_recv()

    far_part(far, width)
    far_part(far, width // 2)

    loads[4].wait()
    for b in range(n_blk):
        r = slice(b * BLK, (b + 1) * BLK)
        at = b * BLK + (per if b * BLK >= rows // 2 else 0)
        hid_ref[at:at + BLK, :] = (x_s[r, :].astype(F32) + mm(att_s[r, :], wo_s[...])).astype(BF16)

    for c in rs:
        c.wait_recv()
    rs_recv[0] = rs_send[pl.ds(me * slab, slab), :]
    st_recv[0] = st_send[me]
    top = st_recv[0, 0:1, :]
    for k in range(1, n_dev):
        top = jnp.maximum(top, st_recv[k, 0:1, :])
    tot = jnp.zeros((1, slab), F32)
    o = jnp.zeros((slab, head), F32)
    for k in range(n_dev):
        fac = jnp.exp(st_recv[k, 0:1, :] - top)
        tot = tot + st_recv[k, 1:2, :] * fac
        o = o + rs_recv[k] * row_to_column(fac)
    o = (o / row_to_column(tot)).astype(BF16)
    hg = xg_all[pl.ds(me * per, per), :].astype(F32)
    for h in range(heads):
        hg = hg + mm(o[h * per:(h + 1) * per], wo_s[h * head:(h + 1) * head, :])
    hid_ref[rows // 2:rows // 2 + per, :] = hg.astype(BF16)

    for c in [pair] + swap + swap2 + [spread] + rs + [to_near]:
        c.wait_send()

    @pl.when(has_far)
    def _():
        to_far.wait_send()


def front(x, wq, wk, wv, wo, rel_bias, gp, n_dev, heads):
    rows, dim = x.shape
    head = wk.shape[1]
    width = (rel_bias.shape[1] - 1) // 2
    n_glob = gp.shape[1]
    per = n_glob // n_dev
    n_blk = rows // BLK
    slab = heads * per
    any_spec = pl.BlockSpec(memory_space=pl.ANY)
    vmem_spec = pl.BlockSpec(memory_space=pltpu.VMEM)
    dma = pltpu.SemaphoreType.DMA
    return pl.pallas_call(
        functools.partial(front_kernel, n_dev, heads, width),
        name='front',
        out_shape=jax.ShapeDtypeStruct((rows + per, dim), BF16),
        in_specs=[any_spec] * 5 + [vmem_spec] * 2,
        out_specs=vmem_spec,
        scratch_shapes=[
            pltpu.VMEM(x.shape, BF16), pltpu.VMEM(wq.shape, BF16), pltpu.VMEM(wk.shape, BF16),
            pltpu.VMEM(wv.shape, BF16), pltpu.VMEM(wo.shape, BF16),
            pltpu.VMEM((n_blk, heads * BLK, head), BF16),
            pltpu.VMEM((rows, 2 * head), BF16), pltpu.VMEM((2, width, 2 * head), BF16),
            pltpu.VMEM((heads * BLK, BLK + 2 * width), F32), pltpu.VMEM((8, BLK + 2 * width), F32),
            pltpu.VMEM((8, rows + 2 * width), F32),
            pltpu.VMEM((n_glob, dim), BF16), pltpu.VMEM((n_glob // 2, dim), BF16), pltpu.VMEM((n_glob // 2, dim), BF16),
            pltpu.VMEM((2, n_glob // 4, dim), BF16), pltpu.VMEM((n_glob // 2, dim), BF16), pltpu.VMEM((2, n_glob // 4, dim), BF16),
            pltpu.VMEM((n_glob, dim), BF16),
            pltpu.VMEM((n_dev * slab, head), BF16), pltpu.VMEM((n_glob, 2 * head), BF16),
            pltpu.VMEM((n_blk, heads * BLK, head), F32), pltpu.VMEM((n_blk, heads * BLK, 128), F32),
            pltpu.VMEM((n_blk, heads * BLK, 128), F32),
            pltpu.VMEM((rows, heads * head), BF16),
            pltpu.VMEM((n_dev * slab, head), F32), pltpu.VMEM((n_dev, slab, head), F32),
            pltpu.VMEM((n_dev, 8, slab), F32), pltpu.VMEM((n_dev, 8, slab), F32),
            dma((5,)), dma((6,)), dma((6,)), dma((2,)), dma((2,)), dma((n_dev,)), dma((n_dev,)), dma((n_dev,)), dma((n_dev,)),
        ],
        compiler_params=pltpu.CompilerParams(collective_id=0, has_side_effects=True, vmem_limit_bytes=62 << 20),
    )(x, wq, wk, wv, wo, rel_bias, gp)


def gelu(x):
    scale = math.sqrt(2.0 / math.pi)
    part = 0.5 * x
    return part + part * jnp.tanh(x * (scale + (scale * 0.044715) * (x * x)))


def ffn_kernel(n_dev, hid_ref, w1_ref, w2_ref, ys_ref, yg_ref, acc_s, send_s, yg_s, ssem, rsem):
    part, step = pl.program_id(0), pl.program_id(1)
    last = step == pl.num_programs(1) - 1
    n_glob = yg_s.shape[0]
    per = n_glob // n_dev
    me = lax.axis_index('sp')
    tile = w1_ref.shape[1]
    rows = ys_ref.shape[0]

    def layer(lo, size):
        hi = lo + size

        @pl.when(step == 0)
        def _():
            acc_s[:size, :] = hid_ref[lo:hi, :].astype(F32)

        before = None
        for c in range(0, tile, BLK):
            s = mm(hid_ref[lo:hi, :], w1_ref[:, c:c + BLK])
            if before is not None:
                acc_s[:size, :] += mm(before, w2_ref[c - BLK:c, :])
            before = gelu(s).astype(BF16)
        acc_s[:size, :] += mm(before, w2_ref[tile - BLK:, :])

        @pl.when(last)
        def _():
            ys_ref[...] = acc_s[:rows, :].astype(BF16)

    def copy(k, peer, owner):
        return remote(send_s, yg_s.at[pl.ds(owner * per, per)], ssem.at[k], rsem.at[k], peer)

    @pl.when((part == 0) & (step == 0))
    def _():
        entry_barrier(me, n_dev)

    @pl.when(part == 0)
    def _():
        layer(0, rows + per)

    @pl.when((part == 0) & last)
    def _():
        send_s[...] = acc_s[rows:, :].astype(BF16)
        for k in range(1, n_dev):
            copy(k, lax.rem(me + k, n_dev), me).start()
        yg_s[pl.ds(me * per, per), :] = send_s[...]

    @pl.when(part == 1)
    def _():
        layer(rows + per, rows)

    @pl.when((part == 1) & last)
    def _():
        for k in range(1, n_dev):
            src = lax.rem(me + n_dev - k, n_dev)
            copy(k, src, src).wait_recv()
        yg_ref[...] = yg_s[...]
        for k in range(1, n_dev):
            copy(k, lax.rem(me + k, n_dev), me).wait_send()


def ffn(hid, w1, w2, n_glob, n_dev, tile):
    total, dim = hid.shape
    wide = w1.shape[1]
    per = n_glob // n_dev
    rows = (total - per) // 2
    dma = pltpu.SemaphoreType.DMA
    return pl.pallas_call(
        functools.partial(ffn_kernel, n_dev),
        name='ffn',
        grid=(2, wide // tile),
        out_shape=(jax.ShapeDtypeStruct((2 * rows, dim), BF16), jax.ShapeDtypeStruct((n_glob, dim), BF16)),
        in_specs=[pl.BlockSpec((total, dim), lambda p, i: (0, 0)), pl.BlockSpec((dim, tile), lambda p, i: (0, i)),
                  pl.BlockSpec((tile, dim), lambda p, i: (i, 0))],
        out_specs=(pl.BlockSpec((rows, dim), lambda p, i: (p, 0)), pl.BlockSpec((n_glob, dim), lambda p, i: (0, 0))),
        scratch_shapes=[pltpu.VMEM((rows + per, dim), F32), pltpu.VMEM((per, dim), BF16),
                        pltpu.VMEM((n_glob, dim), BF16), dma((n_dev,)), dma((n_dev,))],
        compiler_params=pltpu.CompilerParams(
            dimension_semantics=('arbitrary', 'arbitrary'), collective_id=1, has_side_effects=True, vmem_limit_bytes=60 << 20),
    )(hid, w1, w2)


def place_kernel(ys_ref, yg_ref, gp_ref, y_ref, yo_ref):
    step = pl.program_id(0)
    size = ys_ref.shape[0]
    first = (lax.axis_index('sp') * pl.num_programs(0) + step) * size
    hit = gp_ref[...] == first + lax.broadcasted_iota(jnp.int32, (size, gp_ref.shape[1]), 0)
    sel = hit.astype(F32)
    placed = mm(sel.astype(BF16), yg_ref[...]).astype(BF16)
    is_glob = jnp.max(sel, axis=1, keepdims=True) > 0.0
    y_ref[...] = jnp.where(is_glob, placed, ys_ref[...])

    @pl.when(step == 0)
    def _():
        yo_ref[...] = yg_ref[...]


def place(ys, yg, gp):
    rows, dim = ys.shape
    n_glob = yg.shape[0]
    return pl.pallas_call(
        place_kernel,
        name='place',
        grid=(rows // BLK,),
        out_shape=(jax.ShapeDtypeStruct(ys.shape, BF16), jax.ShapeDtypeStruct(yg.shape, BF16)),
        in_specs=[pl.BlockSpec((BLK, dim), lambda i: (i, 0)), pl.BlockSpec((n_glob, dim), lambda i: (0, 0)),
                  pl.BlockSpec((1, n_glob), lambda i: (0, 0))],
        out_specs=(pl.BlockSpec((BLK, dim), lambda i: (i, 0)), pl.BlockSpec((n_glob, dim), lambda i: (0, 0))),
        compiler_params=pltpu.CompilerParams(dimension_semantics=('arbitrary',)),
    )(ys, yg, gp)


def solution(mesh):
    n_dev = mesh.shape['sp']

    def shard_layer(hidden_in, w_query, w_key, w_value, w_out, w_up, w_down, rel_bias, glob_pos):
        rows, dim = hidden_in.shape
        heads, head = w_query.shape[1], w_query.shape[2]
        gp = glob_pos.reshape(1, -1)
        hid = front(hidden_in, w_query.reshape(dim, heads * head), w_key.reshape(dim, head), w_value.reshape(dim, head),
                    w_out.reshape(heads * head, dim), rel_bias, gp, n_dev, heads)
        ys, yg = ffn(hid, w_up, w_down, gp.shape[1], n_dev, 768)
        return place(ys, yg, gp)

    return jax.shard_map(
        shard_layer, mesh=mesh,
        in_specs=(P(('dp', 'sp'), None), P(), P(), P(), P(), P(), P(), P(), P('dp')),
        out_specs=(P(('dp', 'sp'), None), P('dp', None)),
        check_vma=False)
```

```python
import functools
import math

import jax
import jax.numpy as jnp
from jax import lax
from jax.experimental import pallas as pl
from jax.experimental.pallas import tpu as pltpu
from jax.sharding import PartitionSpec as P

BF16 = jnp.bfloat16
F32 = jnp.float32
NEG = -math.inf
BLK = 256
ROW = 32
TILE = 768
PARTS = 3


def mm(a, b):
    return jnp.dot(a, b, preferred_element_type=F32)


def mm_nt(a, b):
    return lax.dot_general(a, b, (((1,), (1,)), ((), ())), preferred_element_type=F32)


def remote(src, dst, send, recv, dev):
    return pltpu.make_async_remote_copy(
        src_ref=src, dst_ref=dst, send_sem=send, recv_sem=recv,
        device_id={'sp': dev}, device_id_type=pl.DeviceIdType.MESH)


def entry_barrier(me, n_dev):
    barrier = pltpu.get_barrier_semaphore()
    for k in range(1, n_dev):
        pl.semaphore_signal(barrier, inc=1, device_id={'sp': lax.rem(me + k, n_dev)}, device_id_type=pl.DeviceIdType.MESH)
    pl.semaphore_wait(barrier, n_dev - 1)


def diagonal(n):
    return lax.broadcasted_iota(jnp.int32, (n, n), 0) == lax.broadcasted_iota(jnp.int32, (n, n), 1)


def row_to_column(row):
    n = row.shape[1]
    return jnp.sum(jnp.where(diagonal(n), jnp.broadcast_to(row, (n, n)), 0.0), axis=1, keepdims=True)


def column_to_row(col):
    n = col.shape[0]
    return jnp.sum(jnp.where(diagonal(n), jnp.broadcast_to(col, (n, n)), 0.0), axis=0, keepdims=True)


def layer_kernel(n_dev, heads, width,
                 x_hbm, wq_hbm, wk_hbm, wv_hbm, wo_hbm, w1_hbm, w2_hbm, rb_ref, gp_ref, ys_hbm, yg_hbm,
                 x_s, wq3_s, wk_s, wv_s, wo_s, kv_s, halo_s, row_s, mask_s,
                 xg_send, xp_recv, xh_s, xa_recv, xh2_s, xb_recv, xg_all, rs_send, rs_recv, st_send, st_recv,
                 hid_s, yg_s, w1_s, w2_s,
                 in_sem, x_ssem, x_rsem, halo_ssem, halo_rsem, rs_ssem, rs_rsem, st_ssem, st_rsem, yg_ssem, yg_rsem,
                 w1_sem, w2_sem, out_sem):
    rows, dim = x_s.shape
    head = wk_s.shape[1]
    n_glob = gp_ref.shape[1]
    per = n_glob // n_dev
    slab = heads * per
    n_blk = rows // BLK
    stack = heads * BLK
    unit = stack // 2
    ext = BLK + 2 * width
    part = (rows + per) // PARTS
    split = part * (PARTS - 1) - per
    n_tile = w1_hbm.shape[1] // TILE
    me = lax.axis_index('sp')
    start = me * rows
    core = lax.rem(me, 2)
    chip = me // 2
    partner = me + 1 - 2 * core
    x_peer = 2 * (chip + 1 - 2 * lax.rem(chip, 2)) + core
    y_peer = 2 * lax.rem(chip + 2, 4) + core
    half = n_glob // 2
    quart = n_glob // 4

    def w_copies(t, slot):
        at = lax.rem(t, n_tile) * TILE
        return (pltpu.make_async_copy(w1_hbm.at[:, pl.ds(at, TILE)], w1_s.at[slot], w1_sem.at[slot]),
                pltpu.make_async_copy(w2_hbm.at[pl.ds(at, TILE), :], w2_s.at[slot], w2_sem.at[slot]))

    def rs_copies(k):
        peer = lax.rem(me + k, n_dev)
        return (remote(rs_send.at[pl.ds(peer * slab, slab)], rs_recv.at[k], rs_ssem.at[k], rs_rsem.at[k], peer),
                remote(st_send.at[peer], st_recv.at[k], st_ssem.at[k], st_rsem.at[k], peer))

    def front(wq_s, q_s, bias_s, s0, s1, p0, p1, o_s, m_s, l_s, mg_s, lg_s, att_s, qg_s):
        loads = [pltpu.make_async_copy(src, dst, in_sem.at[i]) for i, (src, dst) in enumerate(
            [(x_hbm, x_s), (wk_hbm, wk_s), (wv_hbm, wv_s), (wq_hbm, wq3_s), (wo_hbm, wo_s)])]
        for c in loads:
            c.start()
        for t in range(2):
            for c in w_copies(t, t):
                c.start()
        entry_barrier(me, n_dev)

        gp_col = row_to_column(gp_ref[...].astype(F32)).astype(jnp.int32)
        own = gp_col == start + lax.broadcasted_iota(jnp.int32, (n_glob, rows), 1)
        loads[0].wait()
        x = x_s[...]

        xg_send[...] = mm(own.astype(F32).astype(BF16), x).astype(BF16)
        pair = remote(xg_send.at[pl.ds((1 - core) * half, half)], xp_recv, x_ssem.at[0], x_rsem.at[0], partner)
        pair.start()

        loads[1].wait()
        loads[2].wait()
        kv_s[:, :head] = mm(x, wk_s[...]).astype(BF16)
        kv_s[:, head:] = mm(x, wv_s[...]).astype(BF16)

        near, far = 1 - core, core
        has_far = (me > 0) & (me < n_dev - 1)
        far_peer = lax.rem(me + n_dev - 1 + 2 * core, n_dev)

        def halo_copies(mine, theirs, peer, sem):
            return [remote(kv_s.at[pl.ds(mine * width + i * BLK, BLK)],
                           halo_s.at[theirs, pl.ds((i + theirs - 2 * i * theirs) * BLK, BLK)],
                           halo_ssem.at[sem + i], halo_rsem.at[sem + i], peer) for i in range(2)]

        to_near = halo_copies(near, core, partner, 0)
        to_far = halo_copies(far, 1 - core, far_peer, 2)
        for c in to_near:
            c.start()

        loads[3].wait()
        wq_s[...] = wq3_s[...].reshape(wq_s.shape)
        pair.wait_recv()
        xh_s[...] = (xg_send[pl.ds(core * half, half), :].astype(F32) + xp_recv[...].astype(F32)).astype(BF16)
        swap = [remote(xh_s.at[pl.ds(0, quart)], xa_recv.at[0], x_ssem.at[1], x_rsem.at[1], x_peer),
                remote(xh_s.at[pl.ds(quart, quart)], xa_recv.at[1], x_ssem.at[2], x_rsem.at[2], y_peer)]
        for c in swap:
            c.start()

        for h in range(heads):
            qh = (mm(x, wq_s[:, h * head:(h + 1) * head]) * head ** -0.5).astype(BF16)
            for b in range(n_blk):
                q_s[b, h * BLK:(h + 1) * BLK, :] = qh[b * BLK:(b + 1) * BLK]

        pos = start - width + lax.broadcasted_iota(jnp.int32, (1, rows + 2 * width), 1)
        hit = jnp.max((gp_col == pos).astype(F32), axis=0, keepdims=True) > 0.0
        bad = hit | (pos < 0) | (pos >= rows * n_dev)
        mask_s[...] = jnp.broadcast_to(jnp.where(bad, NEG, 0.0), mask_s.shape)

        row_s[...] = jnp.full(row_s.shape, NEG, F32)
        row_s[:heads, :2 * width] = rb_ref[:, :2 * width]
        last = jnp.broadcast_to(rb_ref[:, 2 * width:], (heads, 128))
        row_s[:heads, 2 * width:2 * width + 128] = jnp.where(lax.broadcasted_iota(jnp.int32, (heads, 128), 1) == 0, last, NEG)
        for h in range(heads):
            wide = jnp.broadcast_to(row_s[h:h + 1, :], (BLK, ext))
            bias_s[h * BLK:(h + 1) * BLK, :] = pltpu.roll(wide, 0, 1, stride=1, stride_axis=0)

        class Local:
            def __init__(self, b, g, before=None):
                self.b, self.r0, self.before = b, g * unit, before
                self.lo, self.hi = max(0, b * BLK - width), min(rows, (b + 1) * BLK + width)

            def score(self, s_ref):
                s_ref[:, :self.hi - self.lo] = mm_nt(q_s[self.b, self.r0:self.r0 + unit], kv_s[self.lo:self.hi, :head])

            def soft(self, s_ref, p_ref):
                n, c0 = self.hi - self.lo, self.lo - self.b * BLK + width
                for r in range(0, unit, ROW):
                    rs, ra = slice(r, r + ROW), slice(self.r0 + r, self.r0 + r + ROW)
                    s = s_ref[rs, :n] + bias_s[ra, c0:c0 + n] + mask_s[0:1, width + self.lo:width + self.hi]
                    top = jnp.max(s, axis=1, keepdims=True)
                    p = jnp.exp(s - top)
                    p_ref[rs, :n] = p.astype(BF16)
                    m_s[self.b, ra, :] = jnp.broadcast_to(top, (ROW, 128))
                    l_s[self.b, ra, :] = jnp.broadcast_to(jnp.sum(p, axis=1, keepdims=True), (ROW, 128))

            def value(self, p_ref):
                o_s[self.b, self.r0:self.r0 + unit] = mm(p_ref[:, :self.hi - self.lo], kv_s[self.lo:self.hi, head:])

        class Global:
            def __init__(self, g, before=None):
                self.r0, self.before = g * unit, before

            def score(self, s_ref):
                s_ref[...] = mm_nt(qg_s[self.r0:self.r0 + unit, :], kv_s[:, :head])

            def soft(self, s_ref, p_ref):
                for r in range(0, unit, ROW):
                    rs = slice(r, r + ROW)
                    s = s_ref[rs, :]
                    top = jnp.max(s, axis=1, keepdims=True)
                    p = jnp.exp(s - top)
                    p_ref[rs, :] = p.astype(BF16)
                    mg_s[rs, :] = jnp.broadcast_to(top, (ROW, 128))
                    lg_s[rs, :] = jnp.broadcast_to(jnp.sum(p, axis=1, keepdims=True), (ROW, 128))
                for j in range(unit // slab):
                    cut, to = slice(j * slab, (j + 1) * slab), self.r0 // slab + j
                    st_send[to, 0:1, :] = jnp.sum(jnp.where(diagonal(slab), mg_s[cut, :], 0.0), axis=0, keepdims=True)
                    st_send[to, 1:2, :] = jnp.sum(jnp.where(diagonal(slab), lg_s[cut, :], 0.0), axis=0, keepdims=True)

            def value(self, p_ref):
                rs_send[self.r0:self.r0 + unit, :] = mm(p_ref[...], kv_s[:, head:])

        class Far:
            def __init__(self, side, inner, g, before=None):
                self.side, self.inner, self.r0, self.before = side, inner, g * unit, before
                self.b = 1 + side * (n_blk - 3) if inner else side * (n_blk - 1)
                self.k0, self.n = (BLK, 2 * BLK) if inner else (0, 3 * BLK)

            def score(self, s_ref):
                s_ref[:, :self.n] = mm_nt(q_s[self.b, self.r0:self.r0 + unit], halo_s[self.side, self.k0:, :head])

            def soft(self, s_ref, p_ref):
                side, n = self.side, self.n
                near_mask = BLK + side * (rows + BLK)
                if self.inner:
                    cuts = [(side * (ext - BLK), near_mask)]
                else:
                    cuts = [(side * (ext - BLK), side * (rows + width + BLK)), (BLK + side * (ext - 3 * BLK), near_mask)]
                for r in range(0, unit, ROW):
                    rs, ra = slice(r, r + ROW), slice(self.r0 + r, self.r0 + r + ROW)
                    pieces = []
                    for i, (c0, m0) in enumerate(cuts):
                        pieces.append(s_ref[rs, i * BLK:(i + 1) * BLK] + bias_s[ra, pl.ds(pl.multiple_of(c0, BLK), BLK)]
                                      + mask_s[0:1, pl.ds(pl.multiple_of(m0, BLK), BLK)])
                    pieces.append(s_ref[rs, n - BLK:n])
                    s = jnp.concatenate(pieces, axis=1)
                    m1 = m_s[self.b, ra, :]
                    top = jnp.maximum(m1, jnp.broadcast_to(jnp.max(s, axis=1, keepdims=True), (ROW, 128)))
                    p = jnp.exp(s - jnp.concatenate([top] * (n // 128), axis=1))
                    p_ref[rs, :n] = p.astype(BF16)
                    fac = jnp.exp(m1 - top)
                    inv = 1.0 / (l_s[self.b, ra, :] * fac + jnp.broadcast_to(jnp.sum(p, axis=1, keepdims=True), (ROW, 128)))
                    m_s[self.b, ra, :] = fac * inv
                    l_s[self.b, ra, :] = inv

            def value(self, p_ref):
                at = pl.ds(pl.multiple_of(self.b * BLK, BLK), BLK)
                new = mm(p_ref[:, :self.n], halo_s[self.side, self.k0:, head:])
                for h in range(unit // BLK):
                    ra = slice(self.r0 + h * BLK, self.r0 + (h + 1) * BLK)
                    fac, inv = m_s[self.b, ra, :], l_s[self.b, ra, :]
                    o = (o_s[self.b, ra, :] * jnp.concatenate([fac] * (head // 128), axis=1)
                         + new[h * BLK:(h + 1) * BLK] * jnp.concatenate([inv] * (head // 128), axis=1))
                    col = (self.r0 // BLK + h) * head
                    att_s[at, col:col + head] = o.astype(BF16)

        swap2 = [remote(xh2_s.at[pl.ds(0, quart)], xb_recv.at[0], x_ssem.at[3], x_rsem.at[3], y_peer),
                 remote(xh2_s.at[pl.ds(quart, quart)], xb_recv.at[1], x_ssem.at[4], x_rsem.at[4], x_peer)]
        mine = core * half
        spread = remote(xg_all.at[pl.ds(mine, half)], xg_all.at[pl.ds(mine, half)], x_ssem.at[5], x_rsem.at[5], partner)

        def second_swap():
            for c in swap:
                c.wait_recv()
            xh2_s[:quart, :] = (xh_s[:quart, :].astype(F32) + xa_recv[0].astype(F32)).astype(BF16)
            xh2_s[quart:, :] = (xh_s[quart:, :].astype(F32) + xa_recv[1].astype(F32)).astype(BF16)
            for c in swap2:
                c.start()

            @pl.when(has_far)
            def _():
                for c in to_far:
                    c.start()

            @pl.when(jnp.logical_not(has_far))
            def _():
                halo_s[core, :2 * BLK, :] = jnp.zeros((2 * BLK, 2 * head), BF16)

        def share():
            for c in swap2:
                c.wait_recv()
            xg_all[pl.ds(mine, quart), :] = (xh2_s[:quart, :].astype(F32) + xb_recv[0].astype(F32)).astype(BF16)
            xg_all[pl.ds(mine + quart, quart), :] = (xh2_s[quart:, :].astype(F32) + xb_recv[1].astype(F32)).astype(BF16)
            spread.start()

        def project_global():
            theirs = xg_all.at[pl.ds(half - mine, half)]
            remote(theirs, theirs, x_ssem.at[5], x_rsem.at[5], partner).wait_recv()
            xg = xg_all[...]
            for h in range(heads):
                qh = (mm(xg, wq_s[:, h * head:(h + 1) * head]) * head ** -0.5).astype(BF16)
                for j in range(n_dev):
                    at = (j * heads + h) * per
                    qg_s[at:at + per, :] = qh[j * per:(j + 1) * per]
            for j, w in enumerate((wk_s, wv_s)):
                both = mm(xg, w[...]).astype(BF16)
                for side in range(2):
                    halo_s[side, 2 * BLK:, j * head:(j + 1) * head] = both

        def near_ready():
            for c in to_near:
                c.wait_recv()

        def start_partials():
            for k in range(1, n_dev):
                for c in rs_copies(k):
                    c.start()

        def wait_far():
            @pl.when(has_far)
            def _():
                for c in to_far:
                    c.wait_recv()

        hooks = {2: second_swap, 7: share}
        units = [Local(i // 2, i % 2, hooks.get(i)) for i in range(2 * n_blk)]
        units += [Global(0, project_global), Global(1)]
        units += [Far(near, False, 0, near_ready), Far(near, False, 1, start_partials), Far(near, True, 0), Far(near, True, 1)]
        units += [Far(far, False, 0, wait_far), Far(far, False, 1), Far(far, True, 0), Far(far, True, 1)]
        s_refs, p_refs = (s0, s1), (p0, p1)
        for i, u in enumerate(units):
            for k in ((0, 1) if i == 0 else (i + 1,)):
                if k < len(units):
                    if units[k].before is not None:
                        units[k].before()
                    units[k].score(s_refs[k % 2])
            u.soft(s_refs[i % 2], p_refs[i % 2])
            u.value(p_refs[i % 2])

        loads[4].wait()
        for b in range(n_blk):
            r0, r1 = b * BLK, (b + 1) * BLK
            res = (x_s[r0:r1, :].astype(F32) + mm(att_s[r0:r1, :], wo_s[...])).astype(BF16)
            cut = min(max(split - r0, 0), BLK)
            if cut:
                hid_s[r0:r0 + cut, :] = res[:cut]
            if cut < BLK:
                hid_s[r0 + cut + per:r1 + per, :] = res[cut:]

        for c in [pair] + swap + swap2 + [spread] + to_near:
            c.wait_send()

        @pl.when(has_far)
        def _():
            for c in to_far:
                c.wait_send()

    def finish_global():
        for k in range(1, n_dev):
            for c in rs_copies(k):
                c.wait()
        rs_recv[0] = rs_send[pl.ds(me * slab, slab), :]
        st_recv[0] = st_send[me]
        top = st_recv[0, 0:1, :]
        for k in range(1, n_dev):
            top = jnp.maximum(top, st_recv[k, 0:1, :])
        tot = jnp.zeros((1, slab), F32)
        o = jnp.zeros((slab, head), F32)
        for k in range(n_dev):
            fac = jnp.exp(st_recv[k, 0:1, :] - top)
            tot = tot + st_recv[k, 1:2, :] * fac
            o = o + rs_recv[k] * row_to_column(fac)
        o = (o / row_to_column(tot)).astype(BF16)
        hg = xg_all[pl.ds(me * per, per), :].astype(F32)
        for h in range(heads):
            hg = hg + mm(o[h * per:(h + 1) * per], wo_s[h * head:(h + 1) * head, :])
        hid_s[split:split + per, :] = hg.astype(BF16)

    def yg_copy(k, peer, owner):
        return remote(hid_s.at[pl.ds(split, per)], yg_s.at[pl.ds(owner * per, per)], yg_ssem.at[k], yg_rsem.at[k], peer)

    def out_copy(p):
        lo, hi = p * part, min((p + 1) * part, split) if p < PARTS - 1 else rows
        if p == PARTS - 1:
            lo = split
        shift = per if p == PARTS - 1 else 0
        return pltpu.make_async_copy(hid_s.at[pl.ds(lo + shift, hi - lo)], ys_hbm.at[pl.ds(lo, hi - lo)], out_sem.at[p])

    def feed_forward(acc_s, u_s):
        for p in range(PARTS):
            r0, r1 = p * part, (p + 1) * part
            if p == PARTS - 2:
                finish_global()
            acc_s[...] = hid_s[r0:r1, :].astype(F32)
            u_s[...] = jnp.zeros_like(u_s)

            def step(i, carry):
                t = p * n_tile + i
                slot, prev = lax.rem(t, 3), lax.rem(t + 2, 3)
                for c in w_copies(t, slot):
                    c.wait()
                s = mm(hid_s[r0:r1, :], w1_s[slot, :, :BLK])
                acc_s[...] += mm(u_s[...], w2_s[prev, TILE - BLK:, :])
                u = gelu(s).astype(BF16)
                for c in range(BLK, TILE, BLK):
                    s = mm(hid_s[r0:r1, :], w1_s[slot, :, c:c + BLK])
                    acc_s[...] += mm(u, w2_s[slot, c - BLK:c, :])
                    u = gelu(s).astype(BF16)
                u_s[...] = u

                @pl.when(t + 2 < PARTS * n_tile)
                def _():
                    for c in w_copies(t + 2, prev):
                        c.start()

                return carry

            lax.fori_loop(0, n_tile, step, 0)
            slot = ((p + 1) * n_tile - 1) % 3
            hid_s[r0:r1, :] = (acc_s[...] + mm(u_s[...], w2_s[slot, TILE - BLK:, :])).astype(BF16)
            out_copy(p).start()
            if p == PARTS - 2:
                for k in range(1, n_dev):
                    yg_copy(k, lax.rem(me + k, n_dev), me).start()
                yg_s[pl.ds(me * per, per), :] = hid_s[split:split + per, :]

    w2_s[2, TILE - BLK:, :] = jnp.zeros((BLK, dim), BF16)
    pl.run_scoped(
        front,
        pltpu.VMEM((dim, heads * head), BF16), pltpu.VMEM((n_blk, stack, head), BF16), pltpu.VMEM((stack, ext), F32),
        pltpu.VMEM((unit, rows), F32), pltpu.VMEM((unit, rows), F32), pltpu.VMEM((unit, rows), BF16), pltpu.VMEM((unit, rows), BF16),
        pltpu.VMEM((n_blk, stack, head), F32), pltpu.VMEM((n_blk, stack, 128), F32), pltpu.VMEM((n_blk, stack, 128), F32),
        pltpu.VMEM((unit, 128), F32), pltpu.VMEM((unit, 128), F32),
        pltpu.VMEM((rows, heads * head), BF16), pltpu.VMEM((n_dev * slab, head), BF16))
    pl.run_scoped(feed_forward, pltpu.VMEM((part, dim), F32), pltpu.VMEM((part, BLK), BF16))
    for k in range(1, n_dev):
        src = lax.rem(me + n_dev - k, n_dev)
        yg_copy(k, src, src).wait_recv()
    last = pltpu.make_async_copy(yg_s, yg_hbm, out_sem.at[PARTS])
    last.start()
    for k in range(1, n_dev):
        yg_copy(k, lax.rem(me + k, n_dev), me).wait_send()
    for p in range(PARTS):
        out_copy(p).wait()
    last.wait()


def gelu(x):
    scale = math.sqrt(2.0 / math.pi)
    part = 0.5 * x
    return part + part * jnp.tanh(x * (scale + (scale * 0.044715) * (x * x)))


def layer(x, wq, wk, wv, wo, w1, w2, rel_bias, gp, n_dev):
    rows, dim = x.shape
    heads, head = wq.shape[1:]
    width = (rel_bias.shape[1] - 1) // 2
    n_glob = gp.shape[1]
    per = n_glob // n_dev
    slab = heads * per
    any_spec = pl.BlockSpec(memory_space=pl.ANY)
    vmem_spec = pl.BlockSpec(memory_space=pltpu.VMEM)
    dma = pltpu.SemaphoreType.DMA
    return pl.pallas_call(
        functools.partial(layer_kernel, n_dev, heads, width),
        name='layer',
        out_shape=(jax.ShapeDtypeStruct((rows, dim), BF16), jax.ShapeDtypeStruct((n_glob, dim), BF16)),
        in_specs=[any_spec] * 7 + [vmem_spec] * 2,
        out_specs=(any_spec, any_spec),
        scratch_shapes=[
            pltpu.VMEM(x.shape, BF16), pltpu.VMEM(wq.shape, BF16), pltpu.VMEM(wk.shape, BF16),
            pltpu.VMEM(wv.shape, BF16), pltpu.VMEM(wo.shape, BF16),
            pltpu.VMEM((rows, 2 * head), BF16), pltpu.VMEM((2, 3 * BLK, 2 * head), BF16),
            pltpu.VMEM((8, BLK + 2 * width), F32), pltpu.VMEM((8, rows + 2 * width), F32),
            pltpu.VMEM((n_glob, dim), BF16), pltpu.VMEM((n_glob // 2, dim), BF16), pltpu.VMEM((n_glob // 2, dim), BF16),
            pltpu.VMEM((2, n_glob // 4, dim), BF16), pltpu.VMEM((n_glob // 2, dim), BF16), pltpu.VMEM((2, n_glob // 4, dim), BF16),
            pltpu.VMEM((n_glob, dim), BF16),
            pltpu.VMEM((n_dev * slab, head), F32), pltpu.VMEM((n_dev, slab, head), F32),
            pltpu.VMEM((n_dev, 8, slab), F32), pltpu.VMEM((n_dev, 8, slab), F32),
            pltpu.VMEM((rows + per, dim), BF16), pltpu.VMEM((n_glob, dim), BF16),
            pltpu.VMEM((3, dim, TILE), BF16), pltpu.VMEM((3, TILE, dim), BF16),
            dma((5,)), dma((6,)), dma((6,)), dma((4,)), dma((4,)), dma((n_dev,)), dma((n_dev,)), dma((n_dev,)), dma((n_dev,)),
            dma((n_dev,)), dma((n_dev,)), dma((3,)), dma((3,)), dma((PARTS + 1,)),
        ],
        compiler_params=pltpu.CompilerParams(collective_id=0, has_side_effects=True, vmem_limit_bytes=67043328),
    )(x, wq, wk, wv, wo, w1, w2, rel_bias, gp)


def place_kernel(ys_hbm, yg_hbm, gp_ref, y_hbm, yo_hbm, ys_s, y_s, yg_s, in_sem, out_sem):
    n = ys_s.shape[0]
    n_glob = gp_ref.shape[1]
    gets = [pltpu.make_async_copy(ys_hbm.at[pl.ds(i * BLK, BLK)], ys_s.at[i], in_sem.at[i]) for i in range(n)]
    puts = [pltpu.make_async_copy(y_s.at[i], y_hbm.at[pl.ds(i * BLK, BLK)], out_sem.at[i]) for i in range(n)]
    get_g = pltpu.make_async_copy(yg_hbm, yg_s, in_sem.at[n])
    put_g = pltpu.make_async_copy(yg_s, yo_hbm, out_sem.at[n])
    get_g.start()
    for c in gets:
        c.start()
    get_g.wait()
    put_g.start()
    for i in range(n):
        first = (lax.axis_index('sp') * n + i) * BLK
        hit = gp_ref[...] == first + lax.broadcasted_iota(jnp.int32, (BLK, n_glob), 0)
        sel = hit.astype(F32)
        placed = mm(sel.astype(BF16), yg_s[...]).astype(BF16)
        is_glob = jnp.max(sel, axis=1, keepdims=True) > 0.0
        gets[i].wait()
        y_s[i] = jnp.where(is_glob, placed, ys_s[i])
        puts[i].start()
    for c in puts:
        c.wait()
    put_g.wait()


def place(ys, yg, gp):
    rows, dim = ys.shape
    n = rows // BLK
    any_spec = pl.BlockSpec(memory_space=pl.ANY)
    dma = pltpu.SemaphoreType.DMA
    return pl.pallas_call(
        place_kernel,
        name='place',
        out_shape=(jax.ShapeDtypeStruct(ys.shape, BF16), jax.ShapeDtypeStruct(yg.shape, BF16)),
        in_specs=[any_spec, any_spec, pl.BlockSpec(memory_space=pltpu.VMEM)],
        out_specs=(any_spec, any_spec),
        scratch_shapes=[pltpu.VMEM((n, BLK, dim), BF16), pltpu.VMEM((n, BLK, dim), BF16), pltpu.VMEM(yg.shape, BF16),
                        dma((n + 1,)), dma((n + 1,))],
        compiler_params=pltpu.CompilerParams(vmem_limit_bytes=60 << 20),
    )(ys, yg, gp)


def solution(mesh):
    n_dev = mesh.shape['sp']

    def shard_layer(hidden_in, w_query, w_key, w_value, w_out, w_up, w_down, rel_bias, glob_pos):
        dim = hidden_in.shape[1]
        heads, head = w_query.shape[1], w_query.shape[2]
        gp = glob_pos.reshape(1, -1)
        ys, yg = layer(hidden_in, w_query, w_key.reshape(dim, head), w_value.reshape(dim, head),
                       w_out.reshape(heads * head, dim), w_up, w_down, rel_bias, gp, n_dev)
        return place(ys, yg, gp)

    return jax.shard_map(
        shard_layer, mesh=mesh,
        in_specs=(P(('dp', 'sp'), None), P(), P(), P(), P(), P(), P(), P(), P('dp')),
        out_specs=(P(('dp', 'sp'), None), P('dp', None)),
        check_vma=False)
```

```python
import functools
import math

import jax
import jax.numpy as jnp
from jax import lax
from jax.experimental import pallas as pl
from jax.experimental.pallas import tpu as pltpu
from jax.sharding import PartitionSpec as P

BF16 = jnp.bfloat16
F32 = jnp.float32
NEG = -math.inf
BLK = 256
ROW = 32
PIECE = 128
PARTS = 3
UNROLL = 9
W1_CUT = ((0, 5), (5, 4))
W2_CUT = ((0, 4), (4, 4), (8, 1))


def mm(a, b):
    return jnp.dot(a, b, preferred_element_type=F32)


def mm_nt(a, b):
    return lax.dot_general(a, b, (((1,), (1,)), ((), ())), preferred_element_type=F32)


def remote(src, dst, send, recv, dev):
    return pltpu.make_async_remote_copy(
        src_ref=src, dst_ref=dst, send_sem=send, recv_sem=recv,
        device_id={'sp': dev}, device_id_type=pl.DeviceIdType.MESH)


def entry_barrier(me, n_dev):
    barrier = pltpu.get_barrier_semaphore()
    for k in range(1, n_dev):
        pl.semaphore_signal(barrier, inc=1, device_id={'sp': lax.rem(me + k, n_dev)}, device_id_type=pl.DeviceIdType.MESH)
    pl.semaphore_wait(barrier, n_dev - 1)


def diagonal(n):
    return lax.broadcasted_iota(jnp.int32, (n, n), 0) == lax.broadcasted_iota(jnp.int32, (n, n), 1)


def row_to_column(row):
    n = row.shape[1]
    return jnp.sum(jnp.where(diagonal(n), jnp.broadcast_to(row, (n, n)), 0.0), axis=1, keepdims=True)


def column_to_row(col):
    n = col.shape[0]
    return jnp.sum(jnp.where(diagonal(n), jnp.broadcast_to(col, (n, n)), 0.0), axis=0, keepdims=True)


def lane_max(s):
    best = s[:, :128]
    for c in range(128, s.shape[1], 128):
        best = jnp.maximum(best, s[:, c:c + 128])
    return best


def layer_kernel(n_dev, heads, width,
                 x_hbm, wq_hbm, wk_hbm, wv_hbm, wo_hbm, w1_hbm, w2_hbm, rb_ref, gp_ref, ys_hbm, yg_hbm,
                 x_s, wq3_s, wk_s, wv_s, wo_s, kv_s, halo_s, row_s, mask_s,
                 xg_send, xp_recv, xh_s, xa_recv, xh2_s, xb_recv, xg_all, rs_send, rs_recv, st_send, st_recv,
                 hid_s, yg_s, w1_s, w2_s,
                 in_sem, x_ssem, x_rsem, halo_ssem, halo_rsem, rs_ssem, rs_rsem, st_ssem, st_rsem, yg_ssem, yg_rsem,
                 w1_sem, w2_sem, out_sem):
    rows, dim = x_s.shape
    head = wk_s.shape[1]
    n_glob = gp_ref.shape[1]
    per = n_glob // n_dev
    slab = heads * per
    n_blk = rows // BLK
    stack = heads * BLK
    unit = stack // 2
    ext = BLK + 2 * width
    part = (rows + per) // PARTS
    split = part * (PARTS - 1) - per
    n_chunk = w1_hbm.shape[1] // BLK
    me = lax.axis_index('sp')
    start = me * rows
    core = lax.rem(me, 2)
    chip = me // 2
    partner = me + 1 - 2 * core
    x_peer = 2 * (chip + 1 - 2 * lax.rem(chip, 2)) + core
    y_peer = 2 * lax.rem(chip + 2, 4) + core
    half = n_glob // 2
    quart = n_glob // 4

    n_part = n_chunk // UNROLL

    def w1_copy(i, turn):
        lo, n = W1_CUT[i]
        at = lax.rem(turn, n_part) * (UNROLL * BLK) + lo * BLK
        return pltpu.make_async_copy(w1_hbm.at[:, pl.ds(at, n * BLK)], w1_s.at[:, pl.ds(lo * BLK, n * BLK)], w1_sem.at[i])

    def w2_copy(i, turn):
        lo, n = W2_CUT[i]
        at = lax.rem(turn, n_part) * (UNROLL * BLK) + lo * BLK
        return pltpu.make_async_copy(w2_hbm.at[pl.ds(at, n * BLK), :], w2_s.at[pl.ds(lo * BLK, n * BLK), :], w2_sem.at[i])

    def first_weights():
        return [w1_copy(0, 0), w2_copy(2, 0), w2_copy(0, 0), w1_copy(1, 0), w2_copy(1, 0)]

    def rs_copies(k):
        peer = lax.rem(me + k, n_dev)
        return (remote(rs_send.at[pl.ds(peer * slab, slab)], rs_recv.at[k], rs_ssem.at[k], rs_rsem.at[k], peer),
                remote(st_send.at[peer], st_recv.at[k], st_ssem.at[k], st_rsem.at[k], peer))

    def front(wq_s, q_s, bias_s, s0, s1, t0, t1, p0, p1, o_s, m_s, l_s, mg_s, lg_s, att_s, qg_s):
        loads = [pltpu.make_async_copy(src, dst, in_sem.at[i]) for i, (src, dst) in enumerate(
            [(x_hbm, x_s), (wk_hbm, wk_s), (wv_hbm, wv_s), (wq_hbm, wq3_s), (wo_hbm, wo_s)])]
        for c in loads[:3]:
            c.start()
        entry_barrier(me, n_dev)

        gp_col = row_to_column(gp_ref[...].astype(F32)).astype(jnp.int32)
        own = gp_col == start + lax.broadcasted_iota(jnp.int32, (n_glob, rows), 1)
        pos = start - width + lax.broadcasted_iota(jnp.int32, (1, rows + 2 * width), 1)
        hit = jnp.max((gp_col == pos).astype(F32), axis=0, keepdims=True) > 0.0
        bad = hit | (pos < 0) | (pos >= rows * n_dev)
        mask_s[...] = jnp.broadcast_to(jnp.where(bad, NEG, 0.0), mask_s.shape)

        row_s[...] = jnp.full(row_s.shape, NEG, F32)
        row_s[:heads, :2 * width] = rb_ref[:, :2 * width]
        last = jnp.broadcast_to(rb_ref[:, 2 * width:], (heads, 128))
        row_s[:heads, 2 * width:2 * width + 128] = jnp.where(lax.broadcasted_iota(jnp.int32, (heads, 128), 1) == 0, last, NEG)
        for h in range(heads):
            wide = jnp.broadcast_to(row_s[h:h + 1, :], (BLK, ext))
            bias_s[h * BLK:(h + 1) * BLK, :] = pltpu.roll(wide, 0, 1, stride=1, stride_axis=0)

        loads[0].wait()
        loads[3].start()
        x = x_s[...]

        xg_send[...] = mm(own.astype(F32).astype(BF16), x).astype(BF16)
        pair = remote(xg_send.at[pl.ds((1 - core) * half, half)], xp_recv, x_ssem.at[0], x_rsem.at[0], partner)
        pair.start()

        loads[1].wait()
        loads[2].wait()
        kv_s[:, :head] = mm(x, wk_s[...]).astype(BF16)
        kv_s[:, head:] = mm(x, wv_s[...]).astype(BF16)

        near, far = 1 - core, core
        has_far = (me > 0) & (me < n_dev - 1)
        far_peer = lax.rem(me + n_dev - 1 + 2 * core, n_dev)

        def halo_copies(mine, theirs, peer, sem):
            return [remote(kv_s.at[pl.ds(mine * width + i * BLK, BLK)],
                           halo_s.at[theirs, pl.ds((i + theirs - 2 * i * theirs) * BLK, BLK)],
                           halo_ssem.at[sem + i], halo_rsem.at[sem + i], peer) for i in range(2)]

        loads[4].start()
        for c in first_weights():
            c.start()
        to_near = halo_copies(near, core, partner, 0)
        to_far = halo_copies(far, 1 - core, far_peer, 2)
        for c in to_near:
            c.start()

        loads[3].wait()
        wq_s[...] = wq3_s[...].reshape(wq_s.shape)
        pair.wait_recv()
        xh_s[...] = (xg_send[pl.ds(core * half, half), :].astype(F32) + xp_recv[...].astype(F32)).astype(BF16)
        swap = [remote(xh_s.at[pl.ds(0, quart)], xa_recv.at[0], x_ssem.at[1], x_rsem.at[1], x_peer),
                remote(xh_s.at[pl.ds(quart, quart)], xa_recv.at[1], x_ssem.at[2], x_rsem.at[2], y_peer)]
        for c in swap:
            c.start()

        for h in range(heads):
            qh = (mm(x, wq_s[:, h * head:(h + 1) * head]) * head ** -0.5).astype(BF16)
            for b in range(n_blk):
                q_s[b, h * BLK:(h + 1) * BLK, :] = qh[b * BLK:(b + 1) * BLK]

        class Local:
            def __init__(self, b, g, before=None):
                self.b, self.r0, self.before = b, g * unit, before
                self.lo, self.hi = max(0, b * BLK - width), min(rows, (b + 1) * BLK + width)

            def score(self, s_ref, t_ref):
                n, c0 = self.hi - self.lo, self.lo - self.b * BLK + width
                s = mm_nt(q_s[self.b, self.r0:self.r0 + unit], kv_s[self.lo:self.hi, :head])
                s = s + bias_s[self.r0:self.r0 + unit, c0:c0 + n] + mask_s[0:1, width + self.lo:width + self.hi]
                s_ref[:, :n] = s
                t_ref[...] = lane_max(s)

            def soft(self, s_ref, t_ref, p_ref):
                n = self.hi - self.lo
                for r in range(0, unit, ROW):
                    rs, ra = slice(r, r + ROW), slice(self.r0 + r, self.r0 + r + ROW)
                    top = jnp.max(t_ref[rs, :], axis=1, keepdims=True)
                    p = jnp.exp(s_ref[rs, :n] - top)
                    p_ref[rs, :n] = p.astype(BF16)
                    m_s[self.b, ra, :] = jnp.broadcast_to(top, (ROW, 128))
                    l_s[self.b, ra, :] = jnp.broadcast_to(jnp.sum(p, axis=1, keepdims=True), (ROW, 128))

            def value(self, p_ref):
                o_s[self.b, self.r0:self.r0 + unit] = mm(p_ref[:, :self.hi - self.lo], kv_s[self.lo:self.hi, head:])

        class Global:
            def __init__(self, g, before=None):
                self.r0, self.before = g * unit, before

            def score(self, s_ref, t_ref):
                s = mm_nt(qg_s[self.r0:self.r0 + unit, :], kv_s[:, :head])
                s_ref[...] = s
                t_ref[...] = lane_max(s)

            def soft(self, s_ref, t_ref, p_ref):
                for r in range(0, unit, ROW):
                    rs = slice(r, r + ROW)
                    top = jnp.max(t_ref[rs, :], axis=1, keepdims=True)
                    p = jnp.exp(s_ref[rs, :] - top)
                    p_ref[rs, :] = p.astype(BF16)
                    mg_s[rs, :] = jnp.broadcast_to(top, (ROW, 128))
                    lg_s[rs, :] = jnp.broadcast_to(jnp.sum(p, axis=1, keepdims=True), (ROW, 128))
                for j in range(unit // slab):
                    cut, to = slice(j * slab, (j + 1) * slab), self.r0 // slab + j
                    st_send[to, 0:1, :] = jnp.sum(jnp.where(diagonal(slab), mg_s[cut, :], 0.0), axis=0, keepdims=True)
                    st_send[to, 1:2, :] = jnp.sum(jnp.where(diagonal(slab), lg_s[cut, :], 0.0), axis=0, keepdims=True)

            def value(self, p_ref):
                rs_send[self.r0:self.r0 + unit, :] = mm(p_ref[...], kv_s[:, head:])

        class Far:
            def __init__(self, side, inner, g, before=None):
                self.side, self.inner, self.r0, self.before = side, inner, g * unit, before
                self.b = 1 + side * (n_blk - 3) if inner else side * (n_blk - 1)
                self.k0, self.n = (BLK, 2 * BLK) if inner else (0, 3 * BLK)

            def score(self, s_ref, t_ref):
                side, n = self.side, self.n
                near_mask = BLK + side * (rows + BLK)
                if self.inner:
                    cuts = [(side * (ext - BLK), near_mask)]
                else:
                    cuts = [(side * (ext - BLK), side * (rows + width + BLK)), (BLK + side * (ext - 3 * BLK), near_mask)]
                s = mm_nt(q_s[self.b, self.r0:self.r0 + unit], halo_s[side, self.k0:, :head])
                best = lane_max(s[:, n - BLK:])
                s_ref[:, n - BLK:n] = s[:, n - BLK:]
                for i, (c0, m0) in enumerate(cuts):
                    cut = (s[:, i * BLK:(i + 1) * BLK] + bias_s[self.r0:self.r0 + unit, pl.ds(pl.multiple_of(c0, BLK), BLK)]
                           + mask_s[0:1, pl.ds(pl.multiple_of(m0, BLK), BLK)])
                    s_ref[:, i * BLK:(i + 1) * BLK] = cut
                    best = jnp.maximum(best, lane_max(cut))
                t_ref[...] = best

            def soft(self, s_ref, t_ref, p_ref):
                n = self.n
                for r in range(0, unit, ROW):
                    rs, ra = slice(r, r + ROW), slice(self.r0 + r, self.r0 + r + ROW)
                    m1 = m_s[self.b, ra, :]
                    top = jnp.maximum(m1, jnp.broadcast_to(jnp.max(t_ref[rs, :], axis=1, keepdims=True), (ROW, 128)))
                    s = s_ref[rs, :n]
                    p = jnp.exp(s - jnp.concatenate([top] * (n // 128), axis=1))
                    p_ref[rs, :n] = p.astype(BF16)
                    fac = jnp.exp(m1 - top)
                    inv = 1.0 / (l_s[self.b, ra, :] * fac + jnp.broadcast_to(jnp.sum(p, axis=1, keepdims=True), (ROW, 128)))
                    m_s[self.b, ra, :] = fac * inv
                    l_s[self.b, ra, :] = inv

            def value(self, p_ref):
                at = pl.ds(pl.multiple_of(self.b * BLK, BLK), BLK)
                new = mm(p_ref[:, :self.n], halo_s[self.side, self.k0:, head:])
                for h in range(unit // BLK):
                    ra = slice(self.r0 + h * BLK, self.r0 + (h + 1) * BLK)
                    fac, inv = m_s[self.b, ra, :], l_s[self.b, ra, :]
                    o = (o_s[self.b, ra, :] * jnp.concatenate([fac] * (head // 128), axis=1)
                         + new[h * BLK:(h + 1) * BLK] * jnp.concatenate([inv] * (head // 128), axis=1))
                    col = (self.r0 // BLK + h) * head
                    att_s[at, col:col + head] = o.astype(BF16)

        swap2 = [remote(xh2_s.at[pl.ds(0, quart)], xb_recv.at[0], x_ssem.at[3], x_rsem.at[3], y_peer),
                 remote(xh2_s.at[pl.ds(quart, quart)], xb_recv.at[1], x_ssem.at[4], x_rsem.at[4], x_peer)]
        mine = core * half
        spread = remote(xg_all.at[pl.ds(mine, half)], xg_all.at[pl.ds(mine, half)], x_ssem.at[5], x_rsem.at[5], partner)

        def second_swap():
            for c in swap:
                c.wait_recv()
            xh2_s[:quart, :] = (xh_s[:quart, :].astype(F32) + xa_recv[0].astype(F32)).astype(BF16)
            xh2_s[quart:, :] = (xh_s[quart:, :].astype(F32) + xa_recv[1].astype(F32)).astype(BF16)
            for c in swap2:
                c.start()

            @pl.when(has_far)
            def _():
                for c in to_far:
                    c.start()

            @pl.when(jnp.logical_not(has_far))
            def _():
                halo_s[core, :2 * BLK, :] = jnp.zeros((2 * BLK, 2 * head), BF16)

        def share():
            for c in swap2:
                c.wait_recv()
            xg_all[pl.ds(mine, quart), :] = (xh2_s[:quart, :].astype(F32) + xb_recv[0].astype(F32)).astype(BF16)
            xg_all[pl.ds(mine + quart, quart), :] = (xh2_s[quart:, :].astype(F32) + xb_recv[1].astype(F32)).astype(BF16)
            spread.start()

        def project_global():
            theirs = xg_all.at[pl.ds(half - mine, half)]
            remote(theirs, theirs, x_ssem.at[5], x_rsem.at[5], partner).wait_recv()
            xg = xg_all[...]
            for h in range(heads):
                qh = (mm(xg, wq_s[:, h * head:(h + 1) * head]) * head ** -0.5).astype(BF16)
                for j in range(n_dev):
                    at = (j * heads + h) * per
                    qg_s[at:at + per, :] = qh[j * per:(j + 1) * per]
            for j, w in enumerate((wk_s, wv_s)):
                both = mm(xg, w[...]).astype(BF16)
                for side in range(2):
                    halo_s[side, 2 * BLK:, j * head:(j + 1) * head] = both

        def near_ready():
            for c in to_near:
                c.wait_recv()

        def start_partials():
            for k in range(1, n_dev):
                for c in rs_copies(k):
                    c.start()

        def wait_far():
            @pl.when(has_far)
            def _():
                for c in to_far:
                    c.wait_recv()

        hooks = {2: second_swap, 7: share}
        units = [Local(i // 2, i % 2, hooks.get(i)) for i in range(2 * n_blk)]
        units += [Global(0, project_global), Global(1)]
        units += [Far(near, False, 0, near_ready), Far(near, False, 1, start_partials), Far(near, True, 0), Far(near, True, 1)]
        units += [Far(far, False, 0, wait_far), Far(far, False, 1), Far(far, True, 0), Far(far, True, 1)]
        s_refs, t_refs, p_refs = (s0, s1), (t0, t1), (p0, p1)
        for i, u in enumerate(units):
            for k in ((0, 1) if i == 0 else (i + 1,)):
                if k < len(units):
                    if units[k].before is not None:
                        units[k].before()
                    units[k].score(s_refs[k % 2], t_refs[k % 2])
            u.soft(s_refs[i % 2], t_refs[i % 2], p_refs[i % 2])
            u.value(p_refs[i % 2])

        loads[4].wait()
        for b in range(n_blk):
            r0, r1 = b * BLK, (b + 1) * BLK
            res = (x_s[r0:r1, :].astype(F32) + mm(att_s[r0:r1, :], wo_s[...])).astype(BF16)
            cut = min(max(split - r0, 0), BLK)
            if cut:
                hid_s[r0:r0 + cut, :] = res[:cut]
            if cut < BLK:
                hid_s[r0 + cut + per:r1 + per, :] = res[cut:]

        for c in [pair] + swap + swap2 + [spread] + to_near:
            c.wait_send()

        @pl.when(has_far)
        def _():
            for c in to_far:
                c.wait_send()

    def finish_global():
        for k in range(1, n_dev):
            for c in rs_copies(k):
                c.wait()
        rs_recv[0] = rs_send[pl.ds(me * slab, slab), :]
        st_recv[0] = st_send[me]
        top = st_recv[0, 0:1, :]
        for k in range(1, n_dev):
            top = jnp.maximum(top, st_recv[k, 0:1, :])
        tot = jnp.zeros((1, slab), F32)
        o = jnp.zeros((slab, head), F32)
        for k in range(n_dev):
            fac = jnp.exp(st_recv[k, 0:1, :] - top)
            tot = tot + st_recv[k, 1:2, :] * fac
            o = o + rs_recv[k] * row_to_column(fac)
        o = (o / row_to_column(tot)).astype(BF16)
        hg = xg_all[pl.ds(me * per, per), :].astype(F32)
        for h in range(heads):
            hg = hg + mm(o[h * per:(h + 1) * per], wo_s[h * head:(h + 1) * head, :])
        hid_s[split:split + per, :] = hg.astype(BF16)

    def yg_copy(k, peer, owner):
        return remote(hid_s.at[pl.ds(split, per)], yg_s.at[pl.ds(owner * per, per)], yg_ssem.at[k], yg_rsem.at[k], peer)

    def out_copy(p):
        lo, hi = p * part, min((p + 1) * part, split) if p < PARTS - 1 else rows
        if p == PARTS - 1:
            lo = split
        shift = per if p == PARTS - 1 else 0
        return pltpu.make_async_copy(hid_s.at[pl.ds(lo + shift, hi - lo)], ys_hbm.at[pl.ds(lo, hi - lo)], out_sem.at[p])

    def feed_forward(acc_s, u_s):
        def turn_step(turn, carry):
            p, it = turn // n_part, lax.rem(turn, n_part)
            r = pl.ds(pl.multiple_of(p * part, 16), part)

            @pl.when(turn == (PARTS - 2) * n_part)
            def _():
                finish_global()

            @pl.when(it == 0)
            def _():
                acc_s[...] = hid_s[r, :].astype(F32)
                u_s[...] = jnp.zeros_like(u_s)

            def chunk(j, u):
                s = mm(hid_s[r, :], w1_s[:, j * BLK:(j + 1) * BLK])
                k = (j - 1) % UNROLL
                acc_s[...] += mm(u, w2_s[k * BLK:(k + 1) * BLK, :])
                return gelu(s).astype(BF16)

            u = u_s[...]
            for c in (w1_copy(0, turn), w2_copy(2, turn), w2_copy(0, turn)):
                c.wait()
            for j in range(W1_CUT[0][1]):
                u = chunk(j, u)
            for c in (w1_copy(1, turn), w2_copy(1, turn)):
                c.wait()
            for c in (w1_copy(0, turn + 1), w2_copy(2, turn), w2_copy(0, turn + 1)):
                c.start()
            for j in range(W1_CUT[0][1], UNROLL):
                u = chunk(j, u)
            u_s[...] = u
            for c in (w1_copy(1, turn + 1), w2_copy(1, turn + 1)):
                c.start()

            @pl.when(it == n_part - 1)
            def _():
                tail = w2_copy(2, turn)
                tail.wait()
                hid_s[r, :] = (acc_s[...] + mm(u_s[...], w2_s[(UNROLL - 1) * BLK:, :])).astype(BF16)
                tail.start()

            for q in range(PARTS):
                @pl.when(turn == (q + 1) * n_part - 1)
                def _():
                    out_copy(q).start()
                    if q == PARTS - 2:
                        for k in range(1, n_dev):
                            yg_copy(k, lax.rem(me + k, n_dev), me).start()
                        yg_s[pl.ds(me * per, per), :] = hid_s[split:split + per, :]

            return carry

        lax.fori_loop(0, PARTS * n_part, turn_step, 0)

    pl.run_scoped(
        front,
        pltpu.VMEM((dim, heads * head), BF16), pltpu.VMEM((n_blk, stack, head), BF16), pltpu.VMEM((stack, ext), F32),
        pltpu.VMEM((unit, rows), F32), pltpu.VMEM((unit, rows), F32),
        pltpu.VMEM((unit, 128), F32), pltpu.VMEM((unit, 128), F32), pltpu.VMEM((unit, rows), BF16), pltpu.VMEM((unit, rows), BF16),
        pltpu.VMEM((n_blk, stack, head), F32), pltpu.VMEM((n_blk, stack, 128), F32), pltpu.VMEM((n_blk, stack, 128), F32),
        pltpu.VMEM((unit, 128), F32), pltpu.VMEM((unit, 128), F32),
        pltpu.VMEM((rows, heads * head), BF16), pltpu.VMEM((n_dev * slab, head), BF16))
    pl.run_scoped(feed_forward, pltpu.VMEM((part, dim), F32), pltpu.VMEM((part, BLK), BF16))
    for k in range(1, n_dev):
        src = lax.rem(me + n_dev - k, n_dev)
        yg_copy(k, src, src).wait_recv()
    last = pltpu.make_async_copy(yg_s, yg_hbm, out_sem.at[PARTS])
    last.start()
    for k in range(1, n_dev):
        yg_copy(k, lax.rem(me + k, n_dev), me).wait_send()
    for c in first_weights():
        c.wait()
    for p in range(PARTS):
        out_copy(p).wait()
    last.wait()


def gelu(x):
    scale = math.sqrt(2.0 / math.pi)
    part = 0.5 * x
    return part + part * jnp.tanh(x * (scale + (scale * 0.044715) * (x * x)))


def layer(x, wq, wk, wv, wo, w1, w2, rel_bias, gp, n_dev):
    rows, dim = x.shape
    heads, head = wq.shape[1:]
    width = (rel_bias.shape[1] - 1) // 2
    n_glob = gp.shape[1]
    per = n_glob // n_dev
    slab = heads * per
    any_spec = pl.BlockSpec(memory_space=pl.ANY)
    vmem_spec = pl.BlockSpec(memory_space=pltpu.VMEM)
    dma = pltpu.SemaphoreType.DMA
    return pl.pallas_call(
        functools.partial(layer_kernel, n_dev, heads, width),
        name='layer',
        out_shape=(jax.ShapeDtypeStruct((rows, dim), BF16), jax.ShapeDtypeStruct((n_glob, dim), BF16)),
        in_specs=[any_spec] * 7 + [vmem_spec] * 2,
        out_specs=(any_spec, any_spec),
        scratch_shapes=[
            pltpu.VMEM(x.shape, BF16), pltpu.VMEM(wq.shape, BF16), pltpu.VMEM(wk.shape, BF16),
            pltpu.VMEM(wv.shape, BF16), pltpu.VMEM(wo.shape, BF16),
            pltpu.VMEM((rows, 2 * head), BF16), pltpu.VMEM((2, 3 * BLK, 2 * head), BF16),
            pltpu.VMEM((8, BLK + 2 * width), F32), pltpu.VMEM((8, rows + 2 * width), F32),
            pltpu.VMEM((n_glob, dim), BF16), pltpu.VMEM((n_glob // 2, dim), BF16), pltpu.VMEM((n_glob // 2, dim), BF16),
            pltpu.VMEM((2, n_glob // 4, dim), BF16), pltpu.VMEM((n_glob // 2, dim), BF16), pltpu.VMEM((2, n_glob // 4, dim), BF16),
            pltpu.VMEM((n_glob, dim), BF16),
            pltpu.VMEM((n_dev * slab, head), F32), pltpu.VMEM((n_dev, slab, head), F32),
            pltpu.VMEM((n_dev, 8, slab), F32), pltpu.VMEM((n_dev, 8, slab), F32),
            pltpu.VMEM((rows + per, dim), BF16), pltpu.VMEM((n_glob, dim), BF16),
            pltpu.VMEM((dim, UNROLL * BLK), BF16), pltpu.VMEM((UNROLL * BLK, dim), BF16),
            dma((5,)), dma((6,)), dma((6,)), dma((4,)), dma((4,)), dma((n_dev,)), dma((n_dev,)), dma((n_dev,)), dma((n_dev,)),
            dma((n_dev,)), dma((n_dev,)), dma((2,)), dma((3,)), dma((PARTS + 1,)),
        ],
        compiler_params=pltpu.CompilerParams(collective_id=0, has_side_effects=True, vmem_limit_bytes=67043328),
    )(x, wq, wk, wv, wo, w1, w2, rel_bias, gp)


def place_kernel(ys_hbm, yg_hbm, gp_ref, y_hbm, yo_hbm, ys_s, y_s, yg_s, in_sem, out_sem):
    n = ys_s.shape[0]
    n_glob = gp_ref.shape[1]
    gets = [pltpu.make_async_copy(ys_hbm.at[pl.ds(i * PIECE, PIECE)], ys_s.at[i], in_sem.at[i]) for i in range(n)]
    puts = [pltpu.make_async_copy(y_s.at[i], y_hbm.at[pl.ds(i * PIECE, PIECE)], out_sem.at[i]) for i in range(n)]
    get_g = pltpu.make_async_copy(yg_hbm, yg_s, in_sem.at[n])
    put_g = pltpu.make_async_copy(yg_s, yo_hbm, out_sem.at[n])
    get_g.start()
    for c in gets:
        c.start()
    get_g.wait()
    put_g.start()
    for i in range(n):
        first = (lax.axis_index('sp') * n + i) * PIECE
        hit = gp_ref[...] == first + lax.broadcasted_iota(jnp.int32, (PIECE, n_glob), 0)
        sel = hit.astype(F32)
        placed = mm(sel.astype(BF16), yg_s[...]).astype(BF16)
        is_glob = jnp.max(sel, axis=1, keepdims=True) > 0.0
        gets[i].wait()
        y_s[i] = jnp.where(is_glob, placed, ys_s[i])
        puts[i].start()
    for c in puts:
        c.wait()
    put_g.wait()


def place(ys, yg, gp):
    rows, dim = ys.shape
    n = rows // PIECE
    any_spec = pl.BlockSpec(memory_space=pl.ANY)
    dma = pltpu.SemaphoreType.DMA
    return pl.pallas_call(
        place_kernel,
        name='place',
        out_shape=(jax.ShapeDtypeStruct(ys.shape, BF16), jax.ShapeDtypeStruct(yg.shape, BF16)),
        in_specs=[any_spec, any_spec, pl.BlockSpec(memory_space=pltpu.VMEM)],
        out_specs=(any_spec, any_spec),
        scratch_shapes=[pltpu.VMEM((n, PIECE, dim), BF16), pltpu.VMEM((n, PIECE, dim), BF16), pltpu.VMEM(yg.shape, BF16),
                        dma((n + 1,)), dma((n + 1,))],
        compiler_params=pltpu.CompilerParams(vmem_limit_bytes=60 << 20),
    )(ys, yg, gp)


def solution(mesh):
    n_dev = mesh.shape['sp']

    def shard_layer(hidden_in, w_query, w_key, w_value, w_out, w_up, w_down, rel_bias, glob_pos):
        dim = hidden_in.shape[1]
        heads, head = w_query.shape[1], w_query.shape[2]
        gp = glob_pos.reshape(1, -1)
        ys, yg = layer(hidden_in, w_query, w_key.reshape(dim, head), w_value.reshape(dim, head),
                       w_out.reshape(heads * head, dim), w_up, w_down, rel_bias, gp, n_dev)
        return place(ys, yg, gp)

    return jax.shard_map(
        shard_layer, mesh=mesh,
        in_specs=(P(('dp', 'sp'), None), P(), P(), P(), P(), P(), P(), P(), P('dp')),
        out_specs=(P(('dp', 'sp'), None), P('dp', None)),
        check_vma=False)
```

```python
import functools
import math

import jax
import jax.numpy as jnp
from jax import lax
from jax.experimental import pallas as pl
from jax.experimental.pallas import tpu as pltpu
from jax.sharding import PartitionSpec as P

BF16 = jnp.bfloat16
F32 = jnp.float32
NEG = -math.inf
BLK = 256
ROW = 32
PIECE = 256
PARTS = 3
UNROLL = 9
W1_CUT = ((0, 3), (3, 3), (6, 3))
W2_CUT = ((0, 2), (2, 3), (5, 3), (8, 1))


def mm(a, b):
    return jnp.dot(a, b, preferred_element_type=F32)


def mm_nt(a, b):
    return lax.dot_general(a, b, (((1,), (1,)), ((), ())), preferred_element_type=F32)


def remote(src, dst, send, recv, dev):
    return pltpu.make_async_remote_copy(
        src_ref=src, dst_ref=dst, send_sem=send, recv_sem=recv,
        device_id={'sp': dev}, device_id_type=pl.DeviceIdType.MESH)


def entry_barrier(me, n_dev):
    barrier = pltpu.get_barrier_semaphore()
    for k in range(1, n_dev):
        pl.semaphore_signal(barrier, inc=1, device_id={'sp': lax.rem(me + k, n_dev)}, device_id_type=pl.DeviceIdType.MESH)
    pl.semaphore_wait(barrier, n_dev - 1)


def diagonal(n):
    return lax.broadcasted_iota(jnp.int32, (n, n), 0) == lax.broadcasted_iota(jnp.int32, (n, n), 1)


def row_to_column(row):
    n = row.shape[1]
    return jnp.sum(jnp.where(diagonal(n), jnp.broadcast_to(row, (n, n)), 0.0), axis=1, keepdims=True)


def column_to_row(col):
    n = col.shape[0]
    return jnp.sum(jnp.where(diagonal(n), jnp.broadcast_to(col, (n, n)), 0.0), axis=0, keepdims=True)


def lane_max(s):
    best = s[:, :128]
    for c in range(128, s.shape[1], 128):
        best = jnp.maximum(best, s[:, c:c + 128])
    return best


def layer_kernel(n_dev, heads, width,
                 x_hbm, wq_hbm, wk_hbm, wv_hbm, wo_hbm, w1_hbm, w2_hbm, rb_ref, gp_ref, ys_hbm, yg_hbm,
                 x_s, wq3_s, wk_s, wv_s, wo_s, kv_s, halo_s, row_s, mask_s,
                 xg_send, xp_recv, xh_s, xa_recv, xh2_s, xb_recv, xg_all, rs_send, rs_recv, st_send, st_recv,
                 hid_s, yg_s, w1_s, w2_s,
                 in_sem, x_ssem, x_rsem, halo_ssem, halo_rsem, rs_ssem, rs_rsem, st_ssem, st_rsem, yg_ssem, yg_rsem,
                 w1_sem, w2_sem, out_sem):
    rows, dim = x_s.shape
    head = wk_s.shape[1]
    n_glob = gp_ref.shape[1]
    per = n_glob // n_dev
    slab = heads * per
    n_blk = rows // BLK
    stack = heads * BLK
    unit = stack // 2
    ext = BLK + 2 * width
    part = (rows + per) // PARTS
    split = part * (PARTS - 1) - per
    n_chunk = w1_hbm.shape[1] // BLK
    me = lax.axis_index('sp')
    start = me * rows
    core = lax.rem(me, 2)
    chip = me // 2
    partner = me + 1 - 2 * core
    x_peer = 2 * (chip + 1 - 2 * lax.rem(chip, 2)) + core
    y_peer = 2 * lax.rem(chip + 2, 4) + core
    half = n_glob // 2
    quart = n_glob // 4

    n_part = n_chunk // UNROLL

    def w1_copy(i, turn):
        lo, n = W1_CUT[i]
        at = lax.rem(turn, n_part) * (UNROLL * BLK) + lo * BLK
        return pltpu.make_async_copy(w1_hbm.at[:, pl.ds(at, n * BLK)], w1_s.at[:, pl.ds(lo * BLK, n * BLK)], w1_sem.at[i])

    def w2_copy(i, turn):
        lo, n = W2_CUT[i]
        at = lax.rem(turn, n_part) * (UNROLL * BLK) + lo * BLK
        return pltpu.make_async_copy(w2_hbm.at[pl.ds(at, n * BLK), :], w2_s.at[pl.ds(lo * BLK, n * BLK), :], w2_sem.at[i])

    def group(k, turn):
        if k == 0:
            return [w1_copy(0, turn), w2_copy(3, turn - 1), w2_copy(0, turn)]
        return [w1_copy(k, turn), w2_copy(k, turn)]

    def rs_copies(k):
        peer = lax.rem(me + k, n_dev)
        return (remote(rs_send.at[pl.ds(peer * slab, slab)], rs_recv.at[k], rs_ssem.at[k], rs_rsem.at[k], peer),
                remote(st_send.at[peer], st_recv.at[k], st_ssem.at[k], st_rsem.at[k], peer))

    def front(wq_s, q_s, bias_s, s0, s1, t0, t1, p0, p1, o_s, m_s, l_s, mg_s, lg_s, att_s, qg_s):
        loads = [pltpu.make_async_copy(src, dst, in_sem.at[i]) for i, (src, dst) in enumerate(
            [(x_hbm, x_s), (wk_hbm, wk_s), (wv_hbm, wv_s), (wq_hbm, wq3_s), (wo_hbm, wo_s)])]
        for c in loads[:3]:
            c.start()
        entry_barrier(me, n_dev)

        gp_col = row_to_column(gp_ref[...].astype(F32)).astype(jnp.int32)
        own = gp_col == start + lax.broadcasted_iota(jnp.int32, (n_glob, rows), 1)
        pos = start - width + lax.broadcasted_iota(jnp.int32, (1, rows + 2 * width), 1)
        hit = jnp.max((gp_col == pos).astype(F32), axis=0, keepdims=True) > 0.0
        bad = hit | (pos < 0) | (pos >= rows * n_dev)
        mask_s[...] = jnp.broadcast_to(jnp.where(bad, NEG, 0.0), mask_s.shape)

        row_s[...] = jnp.full(row_s.shape, NEG, F32)
        row_s[:heads, :2 * width] = rb_ref[:, :2 * width]
        last = jnp.broadcast_to(rb_ref[:, 2 * width:], (heads, 128))
        row_s[:heads, 2 * width:2 * width + 128] = jnp.where(lax.broadcasted_iota(jnp.int32, (heads, 128), 1) == 0, last, NEG)
        for h in range(heads):
            wide = jnp.broadcast_to(row_s[h:h + 1, :], (BLK, ext))
            bias_s[h * BLK:(h + 1) * BLK, :] = pltpu.roll(wide, 0, 1, stride=1, stride_axis=0)

        loads[0].wait()
        loads[3].start()
        x = x_s[...]

        xg_send[...] = mm(own.astype(F32).astype(BF16), x).astype(BF16)
        pair = remote(xg_send.at[pl.ds((1 - core) * half, half)], xp_recv, x_ssem.at[0], x_rsem.at[0], partner)
        pair.start()

        loads[1].wait()
        loads[2].wait()
        kv_s[:, :head] = mm(x, wk_s[...]).astype(BF16)
        kv_s[:, head:] = mm(x, wv_s[...]).astype(BF16)

        near, far = 1 - core, core
        has_far = (me > 0) & (me < n_dev - 1)
        far_peer = lax.rem(me + n_dev - 1 + 2 * core, n_dev)

        def halo_copies(mine, theirs, peer, sem):
            return [remote(kv_s.at[pl.ds(mine * width + i * BLK, BLK)],
                           halo_s.at[theirs, pl.ds((i + theirs - 2 * i * theirs) * BLK, BLK)],
                           halo_ssem.at[sem + i], halo_rsem.at[sem + i], peer) for i in range(2)]

        loads[4].start()
        for k in range(3):
            for c in group(k, n_part):
                c.start()
        to_near = halo_copies(near, core, partner, 0)
        to_far = halo_copies(far, 1 - core, far_peer, 2)
        for c in to_near:
            c.start()

        loads[3].wait()
        wq_s[...] = wq3_s[...].reshape(wq_s.shape)
        pair.wait_recv()
        xh_s[...] = (xg_send[pl.ds(core * half, half), :].astype(F32) + xp_recv[...].astype(F32)).astype(BF16)
        swap = [remote(xh_s.at[pl.ds(0, quart)], xa_recv.at[0], x_ssem.at[1], x_rsem.at[1], x_peer),
                remote(xh_s.at[pl.ds(quart, quart)], xa_recv.at[1], x_ssem.at[2], x_rsem.at[2], y_peer)]
        for c in swap:
            c.start()

        for h in range(heads):
            qh = (mm(x, wq_s[:, h * head:(h + 1) * head]) * head ** -0.5).astype(BF16)
            for b in range(n_blk):
                q_s[b, h * BLK:(h + 1) * BLK, :] = qh[b * BLK:(b + 1) * BLK]

        class Local:
            def __init__(self, b, g, before=None):
                self.b, self.r0, self.before = b, g * unit, before
                self.lo, self.hi = max(0, b * BLK - width), min(rows, (b + 1) * BLK + width)

            def score(self, s_ref, t_ref):
                n, c0 = self.hi - self.lo, self.lo - self.b * BLK + width
                s = mm_nt(q_s[self.b, self.r0:self.r0 + unit], kv_s[self.lo:self.hi, :head])
                s = s + bias_s[self.r0:self.r0 + unit, c0:c0 + n] + mask_s[0:1, width + self.lo:width + self.hi]
                s_ref[:, :n] = s
                t_ref[...] = lane_max(s)

            def soft(self, s_ref, t_ref, p_ref):
                n = self.hi - self.lo
                for r in range(0, unit, ROW):
                    rs, ra = slice(r, r + ROW), slice(self.r0 + r, self.r0 + r + ROW)
                    top = jnp.max(t_ref[rs, :], axis=1, keepdims=True)
                    p = jnp.exp(s_ref[rs, :n] - top)
                    p_ref[rs, :n] = p.astype(BF16)
                    m_s[self.b, ra, :] = jnp.broadcast_to(top, (ROW, 128))
                    l_s[self.b, ra, :] = jnp.broadcast_to(jnp.sum(p, axis=1, keepdims=True), (ROW, 128))

            def value(self, p_ref):
                o_s[self.b, self.r0:self.r0 + unit] = mm(p_ref[:, :self.hi - self.lo], kv_s[self.lo:self.hi, head:])

        class Global:
            def __init__(self, g, before=None):
                self.r0, self.before = g * unit, before

            def score(self, s_ref, t_ref):
                s = mm_nt(qg_s[self.r0:self.r0 + unit, :], kv_s[:, :head])
                s_ref[...] = s
                t_ref[...] = lane_max(s)

            def soft(self, s_ref, t_ref, p_ref):
                for r in range(0, unit, ROW):
                    rs = slice(r, r + ROW)
                    top = jnp.max(t_ref[rs, :], axis=1, keepdims=True)
                    p = jnp.exp(s_ref[rs, :] - top)
                    p_ref[rs, :] = p.astype(BF16)
                    mg_s[rs, :] = jnp.broadcast_to(top, (ROW, 128))
                    lg_s[rs, :] = jnp.broadcast_to(jnp.sum(p, axis=1, keepdims=True), (ROW, 128))
                for j in range(unit // slab):
                    cut, to = slice(j * slab, (j + 1) * slab), self.r0 // slab + j
                    st_send[to, 0:1, :] = jnp.sum(jnp.where(diagonal(slab), mg_s[cut, :], 0.0), axis=0, keepdims=True)
                    st_send[to, 1:2, :] = jnp.sum(jnp.where(diagonal(slab), lg_s[cut, :], 0.0), axis=0, keepdims=True)

            def value(self, p_ref):
                rs_send[self.r0:self.r0 + unit, :] = mm(p_ref[...], kv_s[:, head:])

        class Far:
            def __init__(self, side, inner, g, before=None):
                self.side, self.inner, self.r0, self.before = side, inner, g * unit, before
                self.b = 1 + side * (n_blk - 3) if inner else side * (n_blk - 1)
                self.k0, self.n = (BLK, 2 * BLK) if inner else (0, 3 * BLK)

            def score(self, s_ref, t_ref):
                side, n = self.side, self.n
                near_mask = BLK + side * (rows + BLK)
                if self.inner:
                    cuts = [(side * (ext - BLK), near_mask)]
                else:
                    cuts = [(side * (ext - BLK), side * (rows + width + BLK)), (BLK + side * (ext - 3 * BLK), near_mask)]
                s = mm_nt(q_s[self.b, self.r0:self.r0 + unit], halo_s[side, self.k0:, :head])
                best = lane_max(s[:, n - BLK:])
                s_ref[:, n - BLK:n] = s[:, n - BLK:]
                for i, (c0, m0) in enumerate(cuts):
                    cut = (s[:, i * BLK:(i + 1) * BLK] + bias_s[self.r0:self.r0 + unit, pl.ds(pl.multiple_of(c0, BLK), BLK)]
                           + mask_s[0:1, pl.ds(pl.multiple_of(m0, BLK), BLK)])
                    s_ref[:, i * BLK:(i + 1) * BLK] = cut
                    best = jnp.maximum(best, lane_max(cut))
                t_ref[...] = best

            def soft(self, s_ref, t_ref, p_ref):
                n = self.n
                for r in range(0, unit, ROW):
                    rs, ra = slice(r, r + ROW), slice(self.r0 + r, self.r0 + r + ROW)
                    m1 = m_s[self.b, ra, :]
                    top = jnp.maximum(m1, jnp.broadcast_to(jnp.max(t_ref[rs, :], axis=1, keepdims=True), (ROW, 128)))
                    s = s_ref[rs, :n]
                    p = jnp.exp(s - jnp.concatenate([top] * (n // 128), axis=1))
                    p_ref[rs, :n] = p.astype(BF16)
                    fac = jnp.exp(m1 - top)
                    inv = 1.0 / (l_s[self.b, ra, :] * fac + jnp.broadcast_to(jnp.sum(p, axis=1, keepdims=True), (ROW, 128)))
                    m_s[self.b, ra, :] = fac * inv
                    l_s[self.b, ra, :] = inv

            def value(self, p_ref):
                at = pl.ds(pl.multiple_of(self.b * BLK, BLK), BLK)
                new = mm(p_ref[:, :self.n], halo_s[self.side, self.k0:, head:])
                for h in range(unit // BLK):
                    ra = slice(self.r0 + h * BLK, self.r0 + (h + 1) * BLK)
                    fac, inv = m_s[self.b, ra, :], l_s[self.b, ra, :]
                    o = (o_s[self.b, ra, :] * jnp.concatenate([fac] * (head // 128), axis=1)
                         + new[h * BLK:(h + 1) * BLK] * jnp.concatenate([inv] * (head // 128), axis=1))
                    col = (self.r0 // BLK + h) * head
                    att_s[at, col:col + head] = o.astype(BF16)

        swap2 = [remote(xh2_s.at[pl.ds(0, quart)], xb_recv.at[0], x_ssem.at[3], x_rsem.at[3], y_peer),
                 remote(xh2_s.at[pl.ds(quart, quart)], xb_recv.at[1], x_ssem.at[4], x_rsem.at[4], x_peer)]
        mine = core * half
        spread = remote(xg_all.at[pl.ds(mine, half)], xg_all.at[pl.ds(mine, half)], x_ssem.at[5], x_rsem.at[5], partner)

        def second_swap():
            for c in swap:
                c.wait_recv()
            xh2_s[:quart, :] = (xh_s[:quart, :].astype(F32) + xa_recv[0].astype(F32)).astype(BF16)
            xh2_s[quart:, :] = (xh_s[quart:, :].astype(F32) + xa_recv[1].astype(F32)).astype(BF16)
            for c in swap2:
                c.start()

            @pl.when(has_far)
            def _():
                for c in to_far:
                    c.start()

            @pl.when(jnp.logical_not(has_far))
            def _():
                halo_s[core, :2 * BLK, :] = jnp.zeros((2 * BLK, 2 * head), BF16)

        def share():
            for c in swap2:
                c.wait_recv()
            xg_all[pl.ds(mine, quart), :] = (xh2_s[:quart, :].astype(F32) + xb_recv[0].astype(F32)).astype(BF16)
            xg_all[pl.ds(mine + quart, quart), :] = (xh2_s[quart:, :].astype(F32) + xb_recv[1].astype(F32)).astype(BF16)
            spread.start()

        def project_global():
            theirs = xg_all.at[pl.ds(half - mine, half)]
            remote(theirs, theirs, x_ssem.at[5], x_rsem.at[5], partner).wait_recv()
            xg = xg_all[...]
            for h in range(heads):
                qh = (mm(xg, wq_s[:, h * head:(h + 1) * head]) * head ** -0.5).astype(BF16)
                for j in range(n_dev):
                    at = (j * heads + h) * per
                    qg_s[at:at + per, :] = qh[j * per:(j + 1) * per]
            for j, w in enumerate((wk_s, wv_s)):
                both = mm(xg, w[...]).astype(BF16)
                for side in range(2):
                    halo_s[side, 2 * BLK:, j * head:(j + 1) * head] = both

        def near_ready():
            for c in to_near:
                c.wait_recv()

        def start_partials():
            for k in range(1, n_dev):
                for c in rs_copies(k):
                    c.start()

        def wait_far():
            @pl.when(has_far)
            def _():
                for c in to_far:
                    c.wait_recv()

        hooks = {2: second_swap, 7: share}
        units = [Local(i // 2, i % 2, hooks.get(i)) for i in range(2 * n_blk)]
        units += [Global(0, project_global), Global(1)]
        units += [Far(near, False, 0, near_ready), Far(near, False, 1, start_partials), Far(near, True, 0), Far(near, True, 1)]
        units += [Far(far, False, 0, wait_far), Far(far, False, 1), Far(far, True, 0), Far(far, True, 1)]
        s_refs, t_refs, p_refs = (s0, s1), (t0, t1), (p0, p1)
        for i, u in enumerate(units):
            for k in ((0, 1) if i == 0 else (i + 1,)):
                if k < len(units):
                    if units[k].before is not None:
                        units[k].before()
                    units[k].score(s_refs[k % 2], t_refs[k % 2])
            u.soft(s_refs[i % 2], t_refs[i % 2], p_refs[i % 2])
            u.value(p_refs[i % 2])

        loads[4].wait()
        for b in range(n_blk):
            r0, r1 = b * BLK, (b + 1) * BLK
            res = (x_s[r0:r1, :].astype(F32) + mm(att_s[r0:r1, :], wo_s[...])).astype(BF16)
            cut = min(max(split - r0, 0), BLK)
            if cut:
                hid_s[r0:r0 + cut, :] = res[:cut]
            if cut < BLK:
                hid_s[r0 + cut + per:r1 + per, :] = res[cut:]

        for c in [pair] + swap + swap2 + [spread] + to_near:
            c.wait_send()

        @pl.when(has_far)
        def _():
            for c in to_far:
                c.wait_send()

    def finish_global():
        for k in range(1, n_dev):
            for c in rs_copies(k):
                c.wait()
        rs_recv[0] = rs_send[pl.ds(me * slab, slab), :]
        st_recv[0] = st_send[me]
        top = st_recv[0, 0:1, :]
        for k in range(1, n_dev):
            top = jnp.maximum(top, st_recv[k, 0:1, :])
        tot = jnp.zeros((1, slab), F32)
        o = jnp.zeros((slab, head), F32)
        for k in range(n_dev):
            fac = jnp.exp(st_recv[k, 0:1, :] - top)
            tot = tot + st_recv[k, 1:2, :] * fac
            o = o + rs_recv[k] * row_to_column(fac)
        o = (o / row_to_column(tot)).astype(BF16)
        hg = xg_all[pl.ds(me * per, per), :].astype(F32)
        for h in range(heads):
            hg = hg + mm(o[h * per:(h + 1) * per], wo_s[h * head:(h + 1) * head, :])
        hid_s[split:split + per, :] = hg.astype(BF16)

    def yg_copy(k, peer, owner):
        return remote(hid_s.at[pl.ds(split, per)], yg_s.at[pl.ds(owner * per, per)], yg_ssem.at[k], yg_rsem.at[k], peer)

    def out_copy(p):
        lo, hi = p * part, min((p + 1) * part, split) if p < PARTS - 1 else rows
        if p == PARTS - 1:
            lo = split
        shift = per if p == PARTS - 1 else 0
        return pltpu.make_async_copy(hid_s.at[pl.ds(lo + shift, hi - lo)], ys_hbm.at[pl.ds(lo, hi - lo)], out_sem.at[p])

    def feed_forward(acc_s, u_s):
        def turn_step(turn, carry):
            p, it = turn // n_part, lax.rem(turn, n_part)
            r = pl.ds(pl.multiple_of(p * part, 16), part)

            @pl.when(turn == (PARTS - 2) * n_part)
            def _():
                finish_global()

            @pl.when(it == 0)
            def _():
                acc_s[...] = hid_s[r, :].astype(F32)
                u_s[...] = jnp.zeros_like(u_s)

            def chunk(j, u):
                s = mm(hid_s[r, :], w1_s[:, j * BLK:(j + 1) * BLK])
                k = (j - 1) % UNROLL
                acc_s[...] += mm(u, w2_s[k * BLK:(k + 1) * BLK, :])
                return gelu(s).astype(BF16)

            u = u_s[...]
            for j in range(UNROLL):
                if j % 3 == 2:
                    k = (j + 1) // 3 % 3
                    for c in group(k, turn + (k == 0)):
                        c.wait()
                u = chunk(j, u)
                if j % 3 == 2:
                    k = j // 3
                    for c in group(k, turn + 1):
                        c.start()
            u_s[...] = u

            @pl.when(it == n_part - 1)
            def _():
                hid_s[r, :] = (acc_s[...] + mm(u_s[...], w2_s[(UNROLL - 1) * BLK:, :])).astype(BF16)

            for q in range(PARTS):
                @pl.when(turn == (q + 1) * n_part - 1)
                def _():
                    out_copy(q).start()
                    if q == PARTS - 2:
                        for k in range(1, n_dev):
                            yg_copy(k, lax.rem(me + k, n_dev), me).start()
                        yg_s[pl.ds(me * per, per), :] = hid_s[split:split + per, :]

            return carry

        for c in group(0, n_part):
            c.wait()
        lax.fori_loop(0, PARTS * n_part, turn_step, 0)

    pl.run_scoped(
        front,
        pltpu.VMEM((dim, heads * head), BF16), pltpu.VMEM((n_blk, stack, head), BF16), pltpu.VMEM((stack, ext), F32),
        pltpu.VMEM((unit, rows), F32), pltpu.VMEM((unit, rows), F32),
        pltpu.VMEM((unit, 128), F32), pltpu.VMEM((unit, 128), F32), pltpu.VMEM((unit, rows), BF16), pltpu.VMEM((unit, rows), BF16),
        pltpu.VMEM((n_blk, stack, head), F32), pltpu.VMEM((n_blk, stack, 128), F32), pltpu.VMEM((n_blk, stack, 128), F32),
        pltpu.VMEM((unit, 128), F32), pltpu.VMEM((unit, 128), F32),
        pltpu.VMEM((rows, heads * head), BF16), pltpu.VMEM((n_dev * slab, head), BF16))
    pl.run_scoped(feed_forward, pltpu.VMEM((part, dim), F32), pltpu.VMEM((part, BLK), BF16))
    for k in range(1, n_dev):
        src = lax.rem(me + n_dev - k, n_dev)
        yg_copy(k, src, src).wait_recv()
    last = pltpu.make_async_copy(yg_s, yg_hbm, out_sem.at[PARTS])
    last.start()
    for k in range(1, n_dev):
        yg_copy(k, lax.rem(me + k, n_dev), me).wait_send()
    for k in (1, 2):
        for c in group(k, 0):
            c.wait()
    for p in range(PARTS):
        out_copy(p).wait()
    last.wait()


def gelu(x):
    scale = math.sqrt(2.0 / math.pi)
    part = 0.5 * x
    return part + part * jnp.tanh(x * (scale + (scale * 0.044715) * (x * x)))


def layer(x, wq, wk, wv, wo, w1, w2, rel_bias, gp, n_dev):
    rows, dim = x.shape
    heads, head = wq.shape[1:]
    width = (rel_bias.shape[1] - 1) // 2
    n_glob = gp.shape[1]
    per = n_glob // n_dev
    slab = heads * per
    any_spec = pl.BlockSpec(memory_space=pl.ANY)
    vmem_spec = pl.BlockSpec(memory_space=pltpu.VMEM)
    dma = pltpu.SemaphoreType.DMA
    return pl.pallas_call(
        functools.partial(layer_kernel, n_dev, heads, width),
        name='layer',
        out_shape=(jax.ShapeDtypeStruct((rows, dim), BF16), jax.ShapeDtypeStruct((n_glob, dim), BF16)),
        in_specs=[any_spec] * 7 + [vmem_spec] * 2,
        out_specs=(any_spec, any_spec),
        scratch_shapes=[
            pltpu.VMEM(x.shape, BF16), pltpu.VMEM(wq.shape, BF16), pltpu.VMEM(wk.shape, BF16),
            pltpu.VMEM(wv.shape, BF16), pltpu.VMEM(wo.shape, BF16),
            pltpu.VMEM((rows, 2 * head), BF16), pltpu.VMEM((2, 3 * BLK, 2 * head), BF16),
            pltpu.VMEM((8, BLK + 2 * width), F32), pltpu.VMEM((8, rows + 2 * width), F32),
            pltpu.VMEM((n_glob, dim), BF16), pltpu.VMEM((n_glob // 2, dim), BF16), pltpu.VMEM((n_glob // 2, dim), BF16),
            pltpu.VMEM((2, n_glob // 4, dim), BF16), pltpu.VMEM((n_glob // 2, dim), BF16), pltpu.VMEM((2, n_glob // 4, dim), BF16),
            pltpu.VMEM((n_glob, dim), BF16),
            pltpu.VMEM((n_dev * slab, head), F32), pltpu.VMEM((n_dev, slab, head), F32),
            pltpu.VMEM((n_dev, 8, slab), F32), pltpu.VMEM((n_dev, 8, slab), F32),
            pltpu.VMEM((rows + per, dim), BF16), pltpu.VMEM((n_glob, dim), BF16),
            pltpu.VMEM((dim, UNROLL * BLK), BF16), pltpu.VMEM((UNROLL * BLK, dim), BF16),
            dma((5,)), dma((6,)), dma((6,)), dma((4,)), dma((4,)), dma((n_dev,)), dma((n_dev,)), dma((n_dev,)), dma((n_dev,)),
            dma((n_dev,)), dma((n_dev,)), dma((3,)), dma((4,)), dma((PARTS + 1,)),
        ],
        compiler_params=pltpu.CompilerParams(collective_id=0, has_side_effects=True, vmem_limit_bytes=67043328),
    )(x, wq, wk, wv, wo, w1, w2, rel_bias, gp)


def place_kernel(ys_hbm, yg_hbm, gp_ref, y_hbm, yo_hbm, ys_s, y_s, yg_s, in_sem, out_sem):
    n = ys_s.shape[0]
    n_glob = gp_ref.shape[1]
    gets = [pltpu.make_async_copy(ys_hbm.at[pl.ds(i * PIECE, PIECE)], ys_s.at[i], in_sem.at[i]) for i in range(n)]
    puts = [pltpu.make_async_copy(y_s.at[i], y_hbm.at[pl.ds(i * PIECE, PIECE)], out_sem.at[i]) for i in range(n)]
    get_g = pltpu.make_async_copy(yg_hbm, yg_s, in_sem.at[n])
    put_g = pltpu.make_async_copy(yg_s, yo_hbm, out_sem.at[n])
    get_g.start()
    for c in gets:
        c.start()
    get_g.wait()
    put_g.start()
    for i in range(n):
        first = (lax.axis_index('sp') * n + i) * PIECE
        hit = gp_ref[...] == first + lax.broadcasted_iota(jnp.int32, (PIECE, n_glob), 0)
        sel = hit.astype(F32)
        placed = mm(sel.astype(BF16), yg_s[...]).astype(BF16)
        is_glob = jnp.max(sel, axis=1, keepdims=True) > 0.0
        gets[i].wait()
        y_s[i] = jnp.where(is_glob, placed, ys_s[i])
        puts[i].start()
    for c in puts:
        c.wait()
    put_g.wait()


def place(ys, yg, gp):
    rows, dim = ys.shape
    n = rows // PIECE
    any_spec = pl.BlockSpec(memory_space=pl.ANY)
    dma = pltpu.SemaphoreType.DMA
    return pl.pallas_call(
        place_kernel,
        name='place',
        out_shape=(jax.ShapeDtypeStruct(ys.shape, BF16), jax.ShapeDtypeStruct(yg.shape, BF16)),
        in_specs=[any_spec, any_spec, pl.BlockSpec(memory_space=pltpu.VMEM)],
        out_specs=(any_spec, any_spec),
        scratch_shapes=[pltpu.VMEM((n, PIECE, dim), BF16), pltpu.VMEM((n, PIECE, dim), BF16), pltpu.VMEM(yg.shape, BF16),
                        dma((n + 1,)), dma((n + 1,))],
        compiler_params=pltpu.CompilerParams(vmem_limit_bytes=60 << 20),
    )(ys, yg, gp)


def solution(mesh):
    n_dev = mesh.shape['sp']

    def shard_layer(hidden_in, w_query, w_key, w_value, w_out, w_up, w_down, rel_bias, glob_pos):
        dim = hidden_in.shape[1]
        heads, head = w_query.shape[1], w_query.shape[2]
        gp = glob_pos.reshape(1, -1)
        ys, yg = layer(hidden_in, w_query, w_key.reshape(dim, head), w_value.reshape(dim, head),
                       w_out.reshape(heads * head, dim), w_up, w_down, rel_bias, gp, n_dev)
        return place(ys, yg, gp)

    return jax.shard_map(
        shard_layer, mesh=mesh,
        in_specs=(P(('dp', 'sp'), None), P(), P(), P(), P(), P(), P(), P(), P('dp')),
        out_specs=(P(('dp', 'sp'), None), P('dp', None)),
        check_vma=False)
```

```python
import functools
import math

import jax
import jax.numpy as jnp
from jax import lax
from jax.experimental import pallas as pl
from jax.experimental.pallas import tpu as pltpu
from jax.sharding import PartitionSpec as P

BF16 = jnp.bfloat16
F32 = jnp.float32
NEG = -math.inf
BLK = 256
ROW = 32
PIECE = 256
PARTS = 3
TILE = 768


def mm(a, b):
    return jnp.dot(a, b, preferred_element_type=F32)


def mm_nt(a, b):
    return lax.dot_general(a, b, (((1,), (1,)), ((), ())), preferred_element_type=F32)


def remote(src, dst, send, recv, dev):
    return pltpu.make_async_remote_copy(
        src_ref=src, dst_ref=dst, send_sem=send, recv_sem=recv,
        device_id={'sp': dev}, device_id_type=pl.DeviceIdType.MESH)


def entry_barrier(me, n_dev):
    barrier = pltpu.get_barrier_semaphore()
    for k in range(1, n_dev):
        pl.semaphore_signal(barrier, inc=1, device_id={'sp': lax.rem(me + k, n_dev)}, device_id_type=pl.DeviceIdType.MESH)
    pl.semaphore_wait(barrier, n_dev - 1)


def diagonal(n):
    return lax.broadcasted_iota(jnp.int32, (n, n), 0) == lax.broadcasted_iota(jnp.int32, (n, n), 1)


def row_to_column(row):
    n = row.shape[1]
    return jnp.sum(jnp.where(diagonal(n), jnp.broadcast_to(row, (n, n)), 0.0), axis=1, keepdims=True)


def column_to_row(col):
    n = col.shape[0]
    return jnp.sum(jnp.where(diagonal(n), jnp.broadcast_to(col, (n, n)), 0.0), axis=0, keepdims=True)


def lane_max(s):
    best = s[:, :128]
    for c in range(128, s.shape[1], 128):
        best = jnp.maximum(best, s[:, c:c + 128])
    return best


def layer_kernel(n_dev, heads, width,
                 x_hbm, wq_hbm, wk_hbm, wv_hbm, wo_hbm, w1_hbm, w2_hbm, rb_ref, gp_ref, ys_hbm, yg_hbm,
                 x_s, wo_s, halo_s, row_s, mask_s, xp_recv, xa_recv, xb_recv, xg_all, rs_send, rs_recv, st_send, st_recv,
                 hid_s, yg_s, att_s,
                 in_sem, x_ssem, x_rsem, halo_ssem, halo_rsem, rs_ssem, rs_rsem, st_ssem, st_rsem, yg_ssem, yg_rsem,
                 w1_sem, w2_sem, out_sem):
    rows, dim = x_s.shape
    head = wk_hbm.shape[1]
    n_glob = gp_ref.shape[1]
    per = n_glob // n_dev
    slab = heads * per
    n_blk = rows // BLK
    stack = heads * BLK
    unit = stack // 2
    ext = BLK + 2 * width
    part = (rows + per) // PARTS
    split = part * (PARTS - 1) - per
    n_tile = w1_hbm.shape[1] // TILE
    me = lax.axis_index('sp')
    start = me * rows
    core = lax.rem(me, 2)
    chip = me // 2
    partner = me + 1 - 2 * core
    x_peer = 2 * (chip + 1 - 2 * lax.rem(chip, 2)) + core
    y_peer = 2 * lax.rem(chip + 2, 4) + core
    half = n_glob // 2
    quart = n_glob // 4

    def rs_copies(k):
        peer = lax.rem(me + k, n_dev)
        return (remote(rs_send.at[pl.ds(peer * slab, slab)], rs_recv.at[k], rs_ssem.at[k], rs_rsem.at[k], peer),
                remote(st_send.at[peer], st_recv.at[k], st_ssem.at[k], st_rsem.at[k], peer))

    def front(wq3_s, wq_s, wk_s, wv_s, kv_s, xg_send, xh_s, xh2_s, q_s, bias_s, s0, s1, t0, t1, p0, p1, o_s, m_s, l_s, mg_s, lg_s, qg_s):
        loads = [pltpu.make_async_copy(src, dst, in_sem.at[i]) for i, (src, dst) in enumerate(
            [(x_hbm, x_s), (wk_hbm, wk_s), (wv_hbm, wv_s), (wq_hbm, wq3_s), (wo_hbm, wo_s)])]
        for c in loads[:3]:
            c.start()
        entry_barrier(me, n_dev)

        gp_col = row_to_column(gp_ref[...].astype(F32)).astype(jnp.int32)
        own = gp_col == start + lax.broadcasted_iota(jnp.int32, (n_glob, rows), 1)
        pos = start - width + lax.broadcasted_iota(jnp.int32, (1, rows + 2 * width), 1)
        hit = jnp.max((gp_col == pos).astype(F32), axis=0, keepdims=True) > 0.0
        bad = hit | (pos < 0) | (pos >= rows * n_dev)
        mask_s[...] = jnp.broadcast_to(jnp.where(bad, NEG, 0.0), mask_s.shape)

        row_s[...] = jnp.full(row_s.shape, NEG, F32)
        row_s[:heads, :2 * width] = rb_ref[:, :2 * width]
        last = jnp.broadcast_to(rb_ref[:, 2 * width:], (heads, 128))
        row_s[:heads, 2 * width:2 * width + 128] = jnp.where(lax.broadcasted_iota(jnp.int32, (heads, 128), 1) == 0, last, NEG)
        for h in range(heads):
            wide = jnp.broadcast_to(row_s[h:h + 1, :], (BLK, ext))
            bias_s[h * BLK:(h + 1) * BLK, :] = pltpu.roll(wide, 0, 1, stride=1, stride_axis=0)

        loads[0].wait()
        loads[3].start()
        x = x_s[...]

        xg_send[...] = mm(own.astype(F32).astype(BF16), x).astype(BF16)
        pair = remote(xg_send.at[pl.ds((1 - core) * half, half)], xp_recv, x_ssem.at[0], x_rsem.at[0], partner)
        pair.start()

        loads[1].wait()
        loads[2].wait()
        kv_s[:, :head] = mm(x, wk_s[...]).astype(BF16)
        kv_s[:, head:] = mm(x, wv_s[...]).astype(BF16)

        near, far = 1 - core, core
        has_far = (me > 0) & (me < n_dev - 1)
        far_peer = lax.rem(me + n_dev - 1 + 2 * core, n_dev)

        def halo_copies(mine, theirs, peer, sem):
            return [remote(kv_s.at[pl.ds(mine * width + i * BLK, BLK)],
                           halo_s.at[theirs, pl.ds((i + theirs - 2 * i * theirs) * BLK, BLK)],
                           halo_ssem.at[sem + i], halo_rsem.at[sem + i], peer) for i in range(2)]

        loads[4].start()
        to_near = halo_copies(near, core, partner, 0)
        to_far = halo_copies(far, 1 - core, far_peer, 2)
        for c in to_near:
            c.start()

        loads[3].wait()
        wq_s[...] = wq3_s[...].reshape(wq_s.shape)
        pair.wait_recv()
        xh_s[...] = (xg_send[pl.ds(core * half, half), :].astype(F32) + xp_recv[...].astype(F32)).astype(BF16)
        swap = [remote(xh_s.at[pl.ds(0, quart)], xa_recv.at[0], x_ssem.at[1], x_rsem.at[1], x_peer),
                remote(xh_s.at[pl.ds(quart, quart)], xa_recv.at[1], x_ssem.at[2], x_rsem.at[2], y_peer)]
        for c in swap:
            c.start()

        for h in range(heads):
            qh = (mm(x, wq_s[:, h * head:(h + 1) * head]) * head ** -0.5).astype(BF16)
            for b in range(n_blk):
                q_s[b, h * BLK:(h + 1) * BLK, :] = qh[b * BLK:(b + 1) * BLK]

        class Local:
            def __init__(self, b, g, before=None):
                self.b, self.r0, self.before = b, g * unit, before
                self.lo, self.hi = max(0, b * BLK - width), min(rows, (b + 1) * BLK + width)

            def score(self, s_ref, t_ref):
                n, c0 = self.hi - self.lo, self.lo - self.b * BLK + width
                s = mm_nt(q_s[self.b, self.r0:self.r0 + unit], kv_s[self.lo:self.hi, :head])
                s = s + bias_s[self.r0:self.r0 + unit, c0:c0 + n] + mask_s[0:1, width + self.lo:width + self.hi]
                s_ref[:, :n] = s
                t_ref[...] = lane_max(s)

            def soft(self, s_ref, t_ref, p_ref):
                n = self.hi - self.lo
                for r in range(0, unit, ROW):
                    rs, ra = slice(r, r + ROW), slice(self.r0 + r, self.r0 + r + ROW)
                    top = jnp.max(t_ref[rs, :], axis=1, keepdims=True)
                    p = jnp.exp(s_ref[rs, :n] - top)
                    p_ref[rs, :n] = p.astype(BF16)
                    m_s[self.b, ra, :] = jnp.broadcast_to(top, (ROW, 128))
                    l_s[self.b, ra, :] = jnp.broadcast_to(jnp.sum(p, axis=1, keepdims=True), (ROW, 128))

            def value(self, p_ref):
                o_s[self.b, self.r0:self.r0 + unit] = mm(p_ref[:, :self.hi - self.lo], kv_s[self.lo:self.hi, head:])

        class Global:
            def __init__(self, g, before=None):
                self.r0, self.before = g * unit, before

            def score(self, s_ref, t_ref):
                s = mm_nt(qg_s[self.r0:self.r0 + unit, :], kv_s[:, :head])
                s_ref[...] = s
                t_ref[...] = lane_max(s)

            def soft(self, s_ref, t_ref, p_ref):
                for r in range(0, unit, ROW):
                    rs = slice(r, r + ROW)
                    top = jnp.max(t_ref[rs, :], axis=1, keepdims=True)
                    p = jnp.exp(s_ref[rs, :] - top)
                    p_ref[rs, :] = p.astype(BF16)
                    mg_s[rs, :] = jnp.broadcast_to(top, (ROW, 128))
                    lg_s[rs, :] = jnp.broadcast_to(jnp.sum(p, axis=1, keepdims=True), (ROW, 128))
                for j in range(unit // slab):
                    cut, to = slice(j * slab, (j + 1) * slab), self.r0 // slab + j
                    st_send[to, 0:1, :] = jnp.sum(jnp.where(diagonal(slab), mg_s[cut, :], 0.0), axis=0, keepdims=True)
                    st_send[to, 1:2, :] = jnp.sum(jnp.where(diagonal(slab), lg_s[cut, :], 0.0), axis=0, keepdims=True)

            def value(self, p_ref):
                rs_send[self.r0:self.r0 + unit, :] = mm(p_ref[...], kv_s[:, head:])

        class Far:
            def __init__(self, side, inner, g, before=None):
                self.side, self.inner, self.r0, self.before = side, inner, g * unit, before
                self.b = 1 + side * (n_blk - 3) if inner else side * (n_blk - 1)
                self.k0, self.n = (BLK, 2 * BLK) if inner else (0, 3 * BLK)

            def score(self, s_ref, t_ref):
                side, n = self.side, self.n
                near_mask = BLK + side * (rows + BLK)
                if self.inner:
                    cuts = [(side * (ext - BLK), near_mask)]
                else:
                    cuts = [(side * (ext - BLK), side * (rows + width + BLK)), (BLK + side * (ext - 3 * BLK), near_mask)]
                s = mm_nt(q_s[self.b, self.r0:self.r0 + unit], halo_s[side, self.k0:, :head])
                best = lane_max(s[:, n - BLK:])
                s_ref[:, n - BLK:n] = s[:, n - BLK:]
                for i, (c0, m0) in enumerate(cuts):
                    cut = (s[:, i * BLK:(i + 1) * BLK] + bias_s[self.r0:self.r0 + unit, pl.ds(pl.multiple_of(c0, BLK), BLK)]
                           + mask_s[0:1, pl.ds(pl.multiple_of(m0, BLK), BLK)])
                    s_ref[:, i * BLK:(i + 1) * BLK] = cut
                    best = jnp.maximum(best, lane_max(cut))
                t_ref[...] = best

            def soft(self, s_ref, t_ref, p_ref):
                n = self.n
                for r in range(0, unit, ROW):
                    rs, ra = slice(r, r + ROW), slice(self.r0 + r, self.r0 + r + ROW)
                    m1 = m_s[self.b, ra, :]
                    top = jnp.maximum(m1, jnp.broadcast_to(jnp.max(t_ref[rs, :], axis=1, keepdims=True), (ROW, 128)))
                    s = s_ref[rs, :n]
                    p = jnp.exp(s - jnp.concatenate([top] * (n // 128), axis=1))
                    p_ref[rs, :n] = p.astype(BF16)
                    fac = jnp.exp(m1 - top)
                    inv = 1.0 / (l_s[self.b, ra, :] * fac + jnp.broadcast_to(jnp.sum(p, axis=1, keepdims=True), (ROW, 128)))
                    m_s[self.b, ra, :] = fac * inv
                    l_s[self.b, ra, :] = inv

            def value(self, p_ref):
                at = pl.ds(pl.multiple_of(self.b * BLK, BLK), BLK)
                new = mm(p_ref[:, :self.n], halo_s[self.side, self.k0:, head:])
                for h in range(unit // BLK):
                    ra = slice(self.r0 + h * BLK, self.r0 + (h + 1) * BLK)
                    fac, inv = m_s[self.b, ra, :], l_s[self.b, ra, :]
                    o = (o_s[self.b, ra, :] * jnp.concatenate([fac] * (head // 128), axis=1)
                         + new[h * BLK:(h + 1) * BLK] * jnp.concatenate([inv] * (head // 128), axis=1))
                    col = (self.r0 // BLK + h) * head
                    att_s[at, col:col + head] = o.astype(BF16)

        swap2 = [remote(xh2_s.at[pl.ds(0, quart)], xb_recv.at[0], x_ssem.at[3], x_rsem.at[3], y_peer),
                 remote(xh2_s.at[pl.ds(quart, quart)], xb_recv.at[1], x_ssem.at[4], x_rsem.at[4], x_peer)]
        mine = core * half
        spread = remote(xg_all.at[pl.ds(mine, half)], xg_all.at[pl.ds(mine, half)], x_ssem.at[5], x_rsem.at[5], partner)

        def second_swap():
            for c in swap:
                c.wait_recv()
            xh2_s[:quart, :] = (xh_s[:quart, :].astype(F32) + xa_recv[0].astype(F32)).astype(BF16)
            xh2_s[quart:, :] = (xh_s[quart:, :].astype(F32) + xa_recv[1].astype(F32)).astype(BF16)
            for c in swap2:
                c.start()

            @pl.when(has_far)
            def _():
                for c in to_far:
                    c.start()

            @pl.when(jnp.logical_not(has_far))
            def _():
                halo_s[core, :2 * BLK, :] = jnp.zeros((2 * BLK, 2 * head), BF16)

        def share():
            for c in swap2:
                c.wait_recv()
            xg_all[pl.ds(mine, quart), :] = (xh2_s[:quart, :].astype(F32) + xb_recv[0].astype(F32)).astype(BF16)
            xg_all[pl.ds(mine + quart, quart), :] = (xh2_s[quart:, :].astype(F32) + xb_recv[1].astype(F32)).astype(BF16)
            spread.start()

        def project_global():
            theirs = xg_all.at[pl.ds(half - mine, half)]
            remote(theirs, theirs, x_ssem.at[5], x_rsem.at[5], partner).wait_recv()
            xg = xg_all[...]
            for h in range(heads):
                qh = (mm(xg, wq_s[:, h * head:(h + 1) * head]) * head ** -0.5).astype(BF16)
                for j in range(n_dev):
                    at = (j * heads + h) * per
                    qg_s[at:at + per, :] = qh[j * per:(j + 1) * per]
            for j, w in enumerate((wk_s, wv_s)):
                both = mm(xg, w[...]).astype(BF16)
                for side in range(2):
                    halo_s[side, 2 * BLK:, j * head:(j + 1) * head] = both

        def near_ready():
            for c in to_near:
                c.wait_recv()

        def start_partials():
            for k in range(1, n_dev):
                for c in rs_copies(k):
                    c.start()

        def wait_far():
            @pl.when(has_far)
            def _():
                for c in to_far:
                    c.wait_recv()

        hooks = {2: second_swap, 7: share}
        units = [Local(i // 2, i % 2, hooks.get(i)) for i in range(2 * n_blk)]
        units += [Global(0, project_global), Global(1)]
        units += [Far(near, False, 0, near_ready), Far(near, False, 1, start_partials), Far(near, True, 0), Far(near, True, 1)]
        units += [Far(far, False, 0, wait_far), Far(far, False, 1), Far(far, True, 0), Far(far, True, 1)]
        s_refs, t_refs, p_refs = (s0, s1), (t0, t1), (p0, p1)
        for i, u in enumerate(units):
            for k in ((0, 1) if i == 0 else (i + 1,)):
                if k < len(units):
                    if units[k].before is not None:
                        units[k].before()
                    units[k].score(s_refs[k % 2], t_refs[k % 2])
            u.soft(s_refs[i % 2], t_refs[i % 2], p_refs[i % 2])
            u.value(p_refs[i % 2])

        for c in [pair] + swap + swap2 + [spread] + to_near:
            c.wait_send()

        @pl.when(has_far)
        def _():
            for c in to_far:
                c.wait_send()

    def finish_global():
        for k in range(1, n_dev):
            for c in rs_copies(k):
                c.wait()
        rs_recv[0] = rs_send[pl.ds(me * slab, slab), :]
        st_recv[0] = st_send[me]
        top = st_recv[0, 0:1, :]
        for k in range(1, n_dev):
            top = jnp.maximum(top, st_recv[k, 0:1, :])
        tot = jnp.zeros((1, slab), F32)
        o = jnp.zeros((slab, head), F32)
        for k in range(n_dev):
            fac = jnp.exp(st_recv[k, 0:1, :] - top)
            tot = tot + st_recv[k, 1:2, :] * fac
            o = o + rs_recv[k] * row_to_column(fac)
        o = (o / row_to_column(tot)).astype(BF16)
        hg = xg_all[pl.ds(me * per, per), :].astype(F32)
        for h in range(heads):
            hg = hg + mm(o[h * per:(h + 1) * per], wo_s[h * head:(h + 1) * head, :])
        hid_s[split:split + per, :] = hg.astype(BF16)

    def yg_copy(k, peer, owner):
        return remote(hid_s.at[pl.ds(split, per)], yg_s.at[pl.ds(owner * per, per)], yg_ssem.at[k], yg_rsem.at[k], peer)

    def out_copy(p):
        lo, hi = p * part, min((p + 1) * part, split) if p < PARTS - 1 else rows
        if p == PARTS - 1:
            lo = split
        shift = per if p == PARTS - 1 else 0
        return pltpu.make_async_copy(hid_s.at[pl.ds(lo + shift, hi - lo)], ys_hbm.at[pl.ds(lo, hi - lo)], out_sem.at[p])

    def feed_forward(acc_s, u_s, w1_s, w2_s):
        def w_copies(i):
            at = pl.ds(i * TILE, TILE)
            return (pltpu.make_async_copy(w1_hbm.at[:, at], w1_s.at[i], w1_sem.at[i]),
                    pltpu.make_async_copy(w2_hbm.at[at, :], w2_s.at[i], w2_sem.at[i]))

        for i in range(n_tile):
            for c in w_copies(i):
                c.start()

        pltpu.make_async_copy(wo_hbm, wo_s, in_sem.at[4]).wait()
        for b in range(n_blk):
            r0, r1 = b * BLK, (b + 1) * BLK
            res = (x_s[r0:r1, :].astype(F32) + mm(att_s[r0:r1, :], wo_s[...])).astype(BF16)
            cut = min(max(split - r0, 0), BLK)
            if cut:
                hid_s[r0:r0 + cut, :] = res[:cut]
            if cut < BLK:
                hid_s[r0 + cut + per:r1 + per, :] = res[cut:]

        for p in range(PARTS):
            r0, r1 = p * part, (p + 1) * part
            if p == PARTS - 2:
                finish_global()
            acc_s[...] = hid_s[r0:r1, :].astype(F32)
            u_s[...] = jnp.zeros_like(u_s)

            def step(i, carry):
                if p == 0:
                    for c in w_copies(i):
                        c.wait()
                before = jnp.maximum(i - 1, 0)
                s = mm(hid_s[r0:r1, :], w1_s[i, :, :BLK])
                acc_s[...] += mm(u_s[...], w2_s[before, TILE - BLK:, :])
                u = gelu(s).astype(BF16)
                for c in range(BLK, TILE, BLK):
                    s = mm(hid_s[r0:r1, :], w1_s[i, :, c:c + BLK])
                    acc_s[...] += mm(u, w2_s[i, c - BLK:c, :])
                    u = gelu(s).astype(BF16)
                u_s[...] = u
                return carry

            lax.fori_loop(0, n_tile, step, 0)
            hid_s[r0:r1, :] = (acc_s[...] + mm(u_s[...], w2_s[n_tile - 1, TILE - BLK:, :])).astype(BF16)
            out_copy(p).start()
            if p == PARTS - 2:
                for k in range(1, n_dev):
                    yg_copy(k, lax.rem(me + k, n_dev), me).start()
                yg_s[pl.ds(me * per, per), :] = hid_s[split:split + per, :]

    pl.run_scoped(
        front,
        pltpu.VMEM(wq_hbm.shape, BF16), pltpu.VMEM((dim, heads * head), BF16), pltpu.VMEM((dim, head), BF16), pltpu.VMEM((dim, head), BF16),
        pltpu.VMEM((rows, 2 * head), BF16),
        pltpu.VMEM((n_glob, dim), BF16), pltpu.VMEM((half, dim), BF16), pltpu.VMEM((half, dim), BF16),
        pltpu.VMEM((n_blk, stack, head), BF16), pltpu.VMEM((stack, ext), F32),
        pltpu.VMEM((unit, rows), F32), pltpu.VMEM((unit, rows), F32), pltpu.VMEM((unit, 128), F32), pltpu.VMEM((unit, 128), F32),
        pltpu.VMEM((unit, rows), BF16), pltpu.VMEM((unit, rows), BF16),
        pltpu.VMEM((n_blk, stack, head), F32), pltpu.VMEM((n_blk, stack, 128), F32), pltpu.VMEM((n_blk, stack, 128), F32),
        pltpu.VMEM((unit, 128), F32), pltpu.VMEM((unit, 128), F32), pltpu.VMEM((n_dev * slab, head), BF16))
    pl.run_scoped(feed_forward, pltpu.VMEM((part, dim), F32), pltpu.VMEM((part, BLK), BF16),
                  pltpu.VMEM((n_tile, dim, TILE), BF16), pltpu.VMEM((n_tile, TILE, dim), BF16))
    for k in range(1, n_dev):
        src = lax.rem(me + n_dev - k, n_dev)
        yg_copy(k, src, src).wait_recv()
    last = pltpu.make_async_copy(yg_s, yg_hbm, out_sem.at[PARTS])
    last.start()
    for k in range(1, n_dev):
        yg_copy(k, lax.rem(me + k, n_dev), me).wait_send()
    for p in range(PARTS):
        out_copy(p).wait()
    last.wait()


def gelu(x):
    scale = math.sqrt(2.0 / math.pi)
    part = 0.5 * x
    return part + part * jnp.tanh(x * (scale + (scale * 0.044715) * (x * x)))


def layer(x, wq, wk, wv, wo, w1, w2, rel_bias, gp, n_dev):
    rows, dim = x.shape
    heads, head = wq.shape[1:]
    width = (rel_bias.shape[1] - 1) // 2
    n_glob = gp.shape[1]
    per = n_glob // n_dev
    slab = heads * per
    any_spec = pl.BlockSpec(memory_space=pl.ANY)
    vmem_spec = pl.BlockSpec(memory_space=pltpu.VMEM)
    dma = pltpu.SemaphoreType.DMA
    return pl.pallas_call(
        functools.partial(layer_kernel, n_dev, heads, width),
        name='layer',
        out_shape=(jax.ShapeDtypeStruct((rows, dim), BF16), jax.ShapeDtypeStruct((n_glob, dim), BF16)),
        in_specs=[any_spec] * 7 + [vmem_spec] * 2,
        out_specs=(any_spec, any_spec),
        scratch_shapes=[
            pltpu.VMEM(x.shape, BF16), pltpu.VMEM(wo.shape, BF16), pltpu.VMEM((2, 3 * BLK, 2 * head), BF16),
            pltpu.VMEM((8, BLK + 2 * width), F32), pltpu.VMEM((8, rows + 2 * width), F32),
            pltpu.VMEM((n_glob // 2, dim), BF16), pltpu.VMEM((2, n_glob // 4, dim), BF16), pltpu.VMEM((2, n_glob // 4, dim), BF16),
            pltpu.VMEM((n_glob, dim), BF16),
            pltpu.VMEM((n_dev * slab, head), F32), pltpu.VMEM((n_dev, slab, head), F32),
            pltpu.VMEM((n_dev, 8, slab), F32), pltpu.VMEM((n_dev, 8, slab), F32),
            pltpu.VMEM((rows + per, dim), BF16), pltpu.VMEM((n_glob, dim), BF16), pltpu.VMEM((rows, heads * head), BF16),
            dma((5,)), dma((6,)), dma((6,)), dma((4,)), dma((4,)), dma((n_dev,)), dma((n_dev,)), dma((n_dev,)), dma((n_dev,)),
            dma((n_dev,)), dma((n_dev,)), dma((w1.shape[1] // TILE,)), dma((w1.shape[1] // TILE,)), dma((PARTS + 1,)),
        ],
        compiler_params=pltpu.CompilerParams(collective_id=0, has_side_effects=True, vmem_limit_bytes=67043328),
    )(x, wq, wk, wv, wo, w1, w2, rel_bias, gp)


def place_kernel(ys_hbm, yg_hbm, gp_ref, y_hbm, yo_hbm, ys_s, y_s, yg_s, in_sem, out_sem):
    n = ys_s.shape[0]
    n_glob = gp_ref.shape[1]
    gets = [pltpu.make_async_copy(ys_hbm.at[pl.ds(i * PIECE, PIECE)], ys_s.at[i], in_sem.at[i]) for i in range(n)]
    puts = [pltpu.make_async_copy(y_s.at[i], y_hbm.at[pl.ds(i * PIECE, PIECE)], out_sem.at[i]) for i in range(n)]
    get_g = pltpu.make_async_copy(yg_hbm, yg_s, in_sem.at[n])
    put_g = pltpu.make_async_copy(yg_s, yo_hbm, out_sem.at[n])
    get_g.start()
    for c in gets:
        c.start()
    get_g.wait()
    put_g.start()
    for i in range(n):
        first = (lax.axis_index('sp') * n + i) * PIECE
        hit = gp_ref[...] == first + lax.broadcasted_iota(jnp.int32, (PIECE, n_glob), 0)
        sel = hit.astype(F32)
        placed = mm(sel.astype(BF16), yg_s[...]).astype(BF16)
        is_glob = jnp.max(sel, axis=1, keepdims=True) > 0.0
        gets[i].wait()
        y_s[i] = jnp.where(is_glob, placed, ys_s[i])
        puts[i].start()
    for c in puts:
        c.wait()
    put_g.wait()


def place(ys, yg, gp):
    rows, dim = ys.shape
    n = rows // PIECE
    any_spec = pl.BlockSpec(memory_space=pl.ANY)
    dma = pltpu.SemaphoreType.DMA
    return pl.pallas_call(
        place_kernel,
        name='place',
        out_shape=(jax.ShapeDtypeStruct(ys.shape, BF16), jax.ShapeDtypeStruct(yg.shape, BF16)),
        in_specs=[any_spec, any_spec, pl.BlockSpec(memory_space=pltpu.VMEM)],
        out_specs=(any_spec, any_spec),
        scratch_shapes=[pltpu.VMEM((n, PIECE, dim), BF16), pltpu.VMEM((n, PIECE, dim), BF16), pltpu.VMEM(yg.shape, BF16),
                        dma((n + 1,)), dma((n + 1,))],
        compiler_params=pltpu.CompilerParams(vmem_limit_bytes=60 << 20),
    )(ys, yg, gp)


def solution(mesh):
    n_dev = mesh.shape['sp']

    def shard_layer(hidden_in, w_query, w_key, w_value, w_out, w_up, w_down, rel_bias, glob_pos):
        dim = hidden_in.shape[1]
        heads, head = w_query.shape[1], w_query.shape[2]
        gp = glob_pos.reshape(1, -1)
        ys, yg = layer(hidden_in, w_query, w_key.reshape(dim, head), w_value.reshape(dim, head),
                       w_out.reshape(heads * head, dim), w_up, w_down, rel_bias, gp, n_dev)
        return place(ys, yg, gp)

    return jax.shard_map(
        shard_layer, mesh=mesh,
        in_specs=(P(('dp', 'sp'), None), P(), P(), P(), P(), P(), P(), P(), P('dp')),
        out_specs=(P(('dp', 'sp'), None), P('dp', None)),
        check_vma=False)
```

```python
import functools
import math

import jax
import jax.numpy as jnp
from jax import lax
from jax.experimental import pallas as pl
from jax.experimental.pallas import tpu as pltpu
from jax.sharding import PartitionSpec as P

BF16 = jnp.bfloat16
F32 = jnp.float32
NEG = -math.inf
BLK = 256
ROW = 32
PIECE = 256
PARTS = 3
TILE = 768
WIDE = 3


def mm(a, b):
    return jnp.dot(a, b, preferred_element_type=F32)


def mm_nt(a, b):
    return lax.dot_general(a, b, (((1,), (1,)), ((), ())), preferred_element_type=F32)


def remote(src, dst, send, recv, dev):
    return pltpu.make_async_remote_copy(
        src_ref=src, dst_ref=dst, send_sem=send, recv_sem=recv,
        device_id={'sp': dev}, device_id_type=pl.DeviceIdType.MESH)


def announce(me, n_dev):
    barrier = pltpu.get_barrier_semaphore()
    for k in range(1, n_dev):
        pl.semaphore_signal(barrier, inc=1, device_id={'sp': lax.rem(me + k, n_dev)}, device_id_type=pl.DeviceIdType.MESH)
    return barrier


def diagonal(n):
    return lax.broadcasted_iota(jnp.int32, (n, n), 0) == lax.broadcasted_iota(jnp.int32, (n, n), 1)


def row_to_column(row):
    n = row.shape[1]
    return jnp.sum(jnp.where(diagonal(n), jnp.broadcast_to(row, (n, n)), 0.0), axis=1, keepdims=True)


def column_to_row(col):
    n = col.shape[0]
    return jnp.sum(jnp.where(diagonal(n), jnp.broadcast_to(col, (n, n)), 0.0), axis=0, keepdims=True)


def lane_max(s):
    best = s[:, :128]
    for c in range(128, s.shape[1], 128):
        best = jnp.maximum(best, s[:, c:c + 128])
    return best


def layer_kernel(n_dev, heads, width,
                 x_hbm, wq_hbm, wk_hbm, wv_hbm, wo_hbm, w1_hbm, w2_hbm, rb_ref, gp_ref, ys_hbm, yg_hbm,
                 x_s, wo_s, halo_s, row_s, mask_s, xp_recv, xa_recv, xb_recv, xg_all, rs_send, rs_recv, st_send, st_recv,
                 hid_s, yg_s, att_s,
                 in_sem, x_ssem, x_rsem, halo_ssem, halo_rsem, rs_ssem, rs_rsem, st_ssem, st_rsem, yg_ssem, yg_rsem,
                 w1_sem, w2_sem, out_sem):
    rows, dim = x_s.shape
    head = wk_hbm.shape[1]
    n_glob = gp_ref.shape[1]
    per = n_glob // n_dev
    slab = heads * per
    n_blk = rows // BLK
    stack = heads * BLK
    unit = stack // 2
    ext = BLK + 2 * width
    part = (rows + per) // PARTS
    split = part * (PARTS - 1) - per
    n_tile = w1_hbm.shape[1] // TILE
    me = lax.axis_index('sp')
    start = me * rows
    core = lax.rem(me, 2)
    chip = me // 2
    partner = me + 1 - 2 * core
    x_peer = 2 * (chip + 1 - 2 * lax.rem(chip, 2)) + core
    y_peer = 2 * lax.rem(chip + 2, 4) + core
    half = n_glob // 2
    quart = n_glob // 4

    def rs_copies(k):
        peer = lax.rem(me + k, n_dev)
        return (remote(rs_send.at[pl.ds(peer * slab, slab)], rs_recv.at[k], rs_ssem.at[k], rs_rsem.at[k], peer),
                remote(st_send.at[peer], st_recv.at[k], st_ssem.at[k], st_rsem.at[k], peer))

    def front(wq3_s, wq_s, wk_s, wv_s, kv_s, xg_send, xh_s, xh2_s, q_s, bias_s, s0, s1, t0, t1, p0, p1, o_s, m_s, l_s, mg_s, lg_s, qg_s):
        loads = [pltpu.make_async_copy(src, dst, in_sem.at[i]) for i, (src, dst) in enumerate(
            [(x_hbm, x_s), (wk_hbm, wk_s), (wv_hbm, wv_s), (wq_hbm, wq3_s), (wo_hbm, wo_s)])]
        for c in loads[:3]:
            c.start()
        barrier = announce(me, n_dev)

        gp_col = row_to_column(gp_ref[...].astype(F32)).astype(jnp.int32)
        own = gp_col == start + lax.broadcasted_iota(jnp.int32, (n_glob, rows), 1)
        pos = start - width + lax.broadcasted_iota(jnp.int32, (1, rows + 2 * width), 1)
        hit = jnp.max((gp_col == pos).astype(F32), axis=0, keepdims=True) > 0.0
        bad = hit | (pos < 0) | (pos >= rows * n_dev)
        mask_s[...] = jnp.broadcast_to(jnp.where(bad, NEG, 0.0), mask_s.shape)

        row_s[...] = jnp.full(row_s.shape, NEG, F32)
        row_s[:heads, :2 * width] = rb_ref[:, :2 * width]
        last = jnp.broadcast_to(rb_ref[:, 2 * width:], (heads, 128))
        row_s[:heads, 2 * width:2 * width + 128] = jnp.where(lax.broadcasted_iota(jnp.int32, (heads, 128), 1) == 0, last, NEG)
        for h in range(heads):
            wide = jnp.broadcast_to(row_s[h:h + 1, :], (BLK, ext))
            bias_s[h * BLK:(h + 1) * BLK, :] = pltpu.roll(wide, 0, 1, stride=1, stride_axis=0)

        loads[0].wait()
        loads[3].start()
        x = x_s[...]

        xg_send[...] = mm(own.astype(F32).astype(BF16), x).astype(BF16)
        pair = remote(xg_send.at[pl.ds((1 - core) * half, half)], xp_recv, x_ssem.at[0], x_rsem.at[0], partner)
        pl.semaphore_wait(barrier, n_dev - 1)
        pair.start()

        loads[1].wait()
        loads[2].wait()
        kv_s[:, :head] = mm(x, wk_s[...]).astype(BF16)
        kv_s[:, head:] = mm(x, wv_s[...]).astype(BF16)

        near, far = 1 - core, core
        has_far = (me > 0) & (me < n_dev - 1)
        far_peer = lax.rem(me + n_dev - 1 + 2 * core, n_dev)

        def halo_copies(mine, theirs, peer, sem):
            return [remote(kv_s.at[pl.ds(mine * width + (i + theirs - 2 * i * theirs) * BLK, BLK)],
                           halo_s.at[theirs, pl.ds(i * BLK, BLK)],
                           halo_ssem.at[sem + i], halo_rsem.at[sem + i], peer) for i in range(2)]

        loads[4].start()
        to_near = halo_copies(near, core, partner, 0)
        to_far = halo_copies(far, 1 - core, far_peer, 2)
        for c in to_near:
            c.start()

        loads[3].wait()
        wq_s[...] = wq3_s[...].reshape(wq_s.shape)
        pair.wait_recv()
        xh_s[...] = (xg_send[pl.ds(core * half, half), :].astype(F32) + xp_recv[...].astype(F32)).astype(BF16)
        swap = [remote(xh_s.at[pl.ds(0, quart)], xa_recv.at[0], x_ssem.at[1], x_rsem.at[1], x_peer),
                remote(xh_s.at[pl.ds(quart, quart)], xa_recv.at[1], x_ssem.at[2], x_rsem.at[2], y_peer)]
        for c in swap:
            c.start()

        for h in range(heads):
            qh = (mm(x, wq_s[:, h * head:(h + 1) * head]) * head ** -0.5).astype(BF16)
            for b in range(n_blk):
                q_s[b, h * BLK:(h + 1) * BLK, :] = qh[b * BLK:(b + 1) * BLK]

        class Local:
            def __init__(self, b, g, before=None):
                self.b, self.r0, self.before = b, g * unit, before
                self.lo, self.hi = max(0, b * BLK - width), min(rows, (b + 1) * BLK + width)

            def score(self, s_ref, t_ref):
                n, c0 = self.hi - self.lo, self.lo - self.b * BLK + width
                s = mm_nt(q_s[self.b, self.r0:self.r0 + unit], kv_s[self.lo:self.hi, :head])
                s = s + bias_s[self.r0:self.r0 + unit, c0:c0 + n] + mask_s[0:1, width + self.lo:width + self.hi]
                s_ref[:, :n] = s
                t_ref[...] = lane_max(s)

            def soft(self, s_ref, t_ref, p_ref):
                n = self.hi - self.lo
                for r in range(0, unit, ROW):
                    rs, ra = slice(r, r + ROW), slice(self.r0 + r, self.r0 + r + ROW)
                    top = jnp.max(t_ref[rs, :], axis=1, keepdims=True)
                    p = jnp.exp(s_ref[rs, :n] - top)
                    p_ref[rs, :n] = p.astype(BF16)
                    m_s[self.b, ra, :] = jnp.broadcast_to(top, (ROW, 128))
                    l_s[self.b, ra, :] = jnp.broadcast_to(jnp.sum(p, axis=1, keepdims=True), (ROW, 128))

            def value(self, p_ref):
                o_s[self.b, self.r0:self.r0 + unit] = mm(p_ref[:, :self.hi - self.lo], kv_s[self.lo:self.hi, head:])

        class Global:
            def __init__(self, g, before=None):
                self.r0, self.before = g * unit, before

            def score(self, s_ref, t_ref):
                s = mm_nt(qg_s[self.r0:self.r0 + unit, :], kv_s[:, :head])
                s_ref[...] = s
                t_ref[...] = lane_max(s)

            def soft(self, s_ref, t_ref, p_ref):
                for r in range(0, unit, ROW):
                    rs = slice(r, r + ROW)
                    top = jnp.max(t_ref[rs, :], axis=1, keepdims=True)
                    p = jnp.exp(s_ref[rs, :] - top)
                    p_ref[rs, :] = p.astype(BF16)
                    mg_s[rs, :] = jnp.broadcast_to(top, (ROW, 128))
                    lg_s[rs, :] = jnp.broadcast_to(jnp.sum(p, axis=1, keepdims=True), (ROW, 128))
                for j in range(unit // slab):
                    cut, to = slice(j * slab, (j + 1) * slab), self.r0 // slab + j
                    st_send[to, 0:1, :] = jnp.sum(jnp.where(diagonal(slab), mg_s[cut, :], 0.0), axis=0, keepdims=True)
                    st_send[to, 1:2, :] = jnp.sum(jnp.where(diagonal(slab), lg_s[cut, :], 0.0), axis=0, keepdims=True)

            def value(self, p_ref):
                rs_send[self.r0:self.r0 + unit, :] = mm(p_ref[...], kv_s[:, head:])

        class Far:
            def __init__(self, side, inner, g, before=None):
                self.side, self.inner, self.r0, self.before = side, inner, g * unit, before
                self.b = 1 + side * (n_blk - 3) if inner else side * (n_blk - 1)
                self.k0, self.n = (BLK, 2 * BLK) if inner else (0, 3 * BLK)

            def score(self, s_ref, t_ref):
                side, n = self.side, self.n
                near_mask = BLK + side * (rows + BLK)
                if self.inner:
                    cuts = [(side * (ext - BLK), near_mask)]
                else:
                    cuts = [(side * (ext - BLK), side * (rows + width + BLK)), (BLK + side * (ext - 3 * BLK), near_mask)]
                s = mm_nt(q_s[self.b, self.r0:self.r0 + unit], halo_s[side, self.k0:, :head])
                best = lane_max(s[:, n - BLK:])
                s_ref[:, n - BLK:n] = s[:, n - BLK:]
                for i, (c0, m0) in enumerate(cuts):
                    cut = (s[:, i * BLK:(i + 1) * BLK] + bias_s[self.r0:self.r0 + unit, pl.ds(pl.multiple_of(c0, BLK), BLK)]
                           + mask_s[0:1, pl.ds(pl.multiple_of(m0, BLK), BLK)])
                    s_ref[:, i * BLK:(i + 1) * BLK] = cut
                    best = jnp.maximum(best, lane_max(cut))
                t_ref[...] = best

            def soft(self, s_ref, t_ref, p_ref):
                n = self.n
                for r in range(0, unit, ROW):
                    rs, ra = slice(r, r + ROW), slice(self.r0 + r, self.r0 + r + ROW)
                    m1 = m_s[self.b, ra, :]
                    top = jnp.maximum(m1, jnp.broadcast_to(jnp.max(t_ref[rs, :], axis=1, keepdims=True), (ROW, 128)))
                    s = s_ref[rs, :n]
                    p = jnp.exp(s - jnp.concatenate([top] * (n // 128), axis=1))
                    p_ref[rs, :n] = p.astype(BF16)
                    fac = jnp.exp(m1 - top)
                    inv = 1.0 / (l_s[self.b, ra, :] * fac + jnp.broadcast_to(jnp.sum(p, axis=1, keepdims=True), (ROW, 128)))
                    m_s[self.b, ra, :] = fac * inv
                    l_s[self.b, ra, :] = inv

            def value(self, p_ref):
                at = pl.ds(pl.multiple_of(self.b * BLK, BLK), BLK)
                new = mm(p_ref[:, :self.n], halo_s[self.side, self.k0:, head:])
                for h in range(unit // BLK):
                    ra = slice(self.r0 + h * BLK, self.r0 + (h + 1) * BLK)
                    fac, inv = m_s[self.b, ra, :], l_s[self.b, ra, :]
                    o = (o_s[self.b, ra, :] * jnp.concatenate([fac] * (head // 128), axis=1)
                         + new[h * BLK:(h + 1) * BLK] * jnp.concatenate([inv] * (head // 128), axis=1))
                    col = (self.r0 // BLK + h) * head
                    att_s[at, col:col + head] = o.astype(BF16)

        swap2 = [remote(xh2_s.at[pl.ds(0, quart)], xb_recv.at[0], x_ssem.at[3], x_rsem.at[3], y_peer),
                 remote(xh2_s.at[pl.ds(quart, quart)], xb_recv.at[1], x_ssem.at[4], x_rsem.at[4], x_peer)]
        mine = core * half
        spread = remote(xg_all.at[pl.ds(mine, half)], xg_all.at[pl.ds(mine, half)], x_ssem.at[5], x_rsem.at[5], partner)

        def second_swap():
            for c in swap:
                c.wait_recv()
            xh2_s[:quart, :] = (xh_s[:quart, :].astype(F32) + xa_recv[0].astype(F32)).astype(BF16)
            xh2_s[quart:, :] = (xh_s[quart:, :].astype(F32) + xa_recv[1].astype(F32)).astype(BF16)
            for c in swap2:
                c.start()

            @pl.when(has_far)
            def _():
                for c in to_far[::-1]:
                    c.start()

            @pl.when(jnp.logical_not(has_far))
            def _():
                halo_s[core, :2 * BLK, :] = jnp.zeros((2 * BLK, 2 * head), BF16)

        def share():
            for c in swap2:
                c.wait_recv()
            xg_all[pl.ds(mine, quart), :] = (xh2_s[:quart, :].astype(F32) + xb_recv[0].astype(F32)).astype(BF16)
            xg_all[pl.ds(mine + quart, quart), :] = (xh2_s[quart:, :].astype(F32) + xb_recv[1].astype(F32)).astype(BF16)
            spread.start()

        def project_global():
            theirs = xg_all.at[pl.ds(half - mine, half)]
            remote(theirs, theirs, x_ssem.at[5], x_rsem.at[5], partner).wait_recv()
            xg = xg_all[...]
            for h in range(heads):
                qh = (mm(xg, wq_s[:, h * head:(h + 1) * head]) * head ** -0.5).astype(BF16)
                for j in range(n_dev):
                    at = (j * heads + h) * per
                    qg_s[at:at + per, :] = qh[j * per:(j + 1) * per]
            for j, w in enumerate((wk_s, wv_s)):
                both = mm(xg, w[...]).astype(BF16)
                for side in range(2):
                    halo_s[side, 2 * BLK:, j * head:(j + 1) * head] = both

        def near_ready():
            for c in to_near:
                c.wait_recv()

        def wait_far(i):
            @pl.when(has_far)
            def _():
                to_far[i].wait_recv()

        def inner_ready():
            wait_far(1)

        def outer_ready():
            wait_far(0)
            for k in range(1, n_dev):
                for c in rs_copies(k):
                    c.start()

        hooks = {2: second_swap, 7: share}
        units = [Local(i // 2, i % 2, hooks.get(i)) for i in range(2 * n_blk)]
        units += [Global(0, project_global), Global(1)]
        units += [Far(near, False, 0, near_ready), Far(near, False, 1), Far(near, True, 0), Far(near, True, 1)]
        units += [Far(far, True, 0, inner_ready), Far(far, True, 1), Far(far, False, 0, outer_ready), Far(far, False, 1)]
        s_refs, t_refs, p_refs = (s0, s1), (t0, t1), (p0, p1)
        for i, u in enumerate(units):
            for k in ((0, 1) if i == 0 else (i + 1,)):
                if k < len(units):
                    if units[k].before is not None:
                        units[k].before()
                    units[k].score(s_refs[k % 2], t_refs[k % 2])
            u.soft(s_refs[i % 2], t_refs[i % 2], p_refs[i % 2])
            u.value(p_refs[i % 2])

        for c in [pair] + swap + swap2 + [spread] + to_near:
            c.wait_send()

        @pl.when(has_far)
        def _():
            for c in to_far:
                c.wait_send()

    def finish_global():
        for k in range(1, n_dev):
            for c in rs_copies(k):
                c.wait()
        rs_recv[0] = rs_send[pl.ds(me * slab, slab), :]
        st_recv[0] = st_send[me]
        top = st_recv[0, 0:1, :]
        for k in range(1, n_dev):
            top = jnp.maximum(top, st_recv[k, 0:1, :])
        tot = jnp.zeros((1, slab), F32)
        o = jnp.zeros((slab, head), F32)
        for k in range(n_dev):
            fac = jnp.exp(st_recv[k, 0:1, :] - top)
            tot = tot + st_recv[k, 1:2, :] * fac
            o = o + rs_recv[k] * row_to_column(fac)
        o = (o / row_to_column(tot)).astype(BF16)
        hg = xg_all[pl.ds(me * per, per), :].astype(F32)
        for h in range(heads):
            hg = hg + mm(o[h * per:(h + 1) * per], wo_s[h * head:(h + 1) * head, :])
        hid_s[split:split + per, :] = hg.astype(BF16)

    def yg_copy(k, peer, owner):
        return remote(hid_s.at[pl.ds(split, per)], yg_s.at[pl.ds(owner * per, per)], yg_ssem.at[k], yg_rsem.at[k], peer)

    def out_copy(p):
        lo, hi = p * part, min((p + 1) * part, split) if p < PARTS - 1 else rows
        if p == PARTS - 1:
            lo = split
        shift = per if p == PARTS - 1 else 0
        return pltpu.make_async_copy(hid_s.at[pl.ds(lo + shift, hi - lo)], ys_hbm.at[pl.ds(lo, hi - lo)], out_sem.at[p])

    def feed_forward(acc_s, u_s, w1_s, w2_s):
        def w_copies(i):
            at = pl.ds(i * TILE, TILE)
            return (pltpu.make_async_copy(w1_hbm.at[:, at], w1_s.at[i], w1_sem.at[i]),
                    pltpu.make_async_copy(w2_hbm.at[at, :], w2_s.at[i], w2_sem.at[i]))

        for i in range(n_tile):
            for c in w_copies(i):
                c.start()

        pltpu.make_async_copy(wo_hbm, wo_s, in_sem.at[4]).wait()
        for b in range(n_blk):
            r0, r1 = b * BLK, (b + 1) * BLK
            res = (x_s[r0:r1, :].astype(F32) + mm(att_s[r0:r1, :], wo_s[...])).astype(BF16)
            cut = min(max(split - r0, 0), BLK)
            if cut:
                hid_s[r0:r0 + cut, :] = res[:cut]
            if cut < BLK:
                hid_s[r0 + cut + per:r1 + per, :] = res[cut:]

        def chunks(r, i, count):
            u = u_s[...]
            for c in range(count):
                g, at = i + c // (TILE // BLK), c % (TILE // BLK) * BLK
                s = mm(hid_s[r, :], w1_s[g, :, at:at + BLK])
                if c == 0:
                    acc_s[...] += mm(u, w2_s[jnp.maximum(i - 1, 0), TILE - BLK:, :])
                else:
                    b = c - 1
                    at = b % (TILE // BLK) * BLK
                    acc_s[...] += mm(u, w2_s[i + b // (TILE // BLK), at:at + BLK, :])
                u = gelu(s).astype(BF16)
            u_s[...] = u

        def run_part(r, steps, step):
            acc_s[...] = hid_s[r, :].astype(F32)
            u_s[...] = jnp.zeros_like(u_s)
            lax.fori_loop(0, steps, step, 0)
            hid_s[r, :] = (acc_s[...] + mm(u_s[...], w2_s[n_tile - 1, TILE - BLK:, :])).astype(BF16)

        def first(i, carry):
            for c in w_copies(i):
                c.wait()
            chunks(slice(0, part), i, TILE // BLK)
            return carry

        run_part(slice(0, part), n_tile, first)
        out_copy(0).start()
        finish_global()

        def later(p, carry):
            r = pl.ds(pl.multiple_of(p * part, 16), part)

            def step(i, carry):
                chunks(r, i * WIDE, WIDE * (TILE // BLK))
                return carry

            run_part(r, n_tile // WIDE, step)

            @pl.when(p == PARTS - 2)
            def _():
                for k in range(1, n_dev):
                    yg_copy(k, lax.rem(me + k, n_dev), me).start()
                yg_s[pl.ds(me * per, per), :] = hid_s[split:split + per, :]

            for q in range(1, PARTS):
                @pl.when(p == q)
                def _():
                    out_copy(q).start()

            return carry

        lax.fori_loop(1, PARTS, later, 0)

    pl.run_scoped(
        front,
        pltpu.VMEM(wq_hbm.shape, BF16), pltpu.VMEM((dim, heads * head), BF16), pltpu.VMEM((dim, head), BF16), pltpu.VMEM((dim, head), BF16),
        pltpu.VMEM((rows, 2 * head), BF16),
        pltpu.VMEM((n_glob, dim), BF16), pltpu.VMEM((half, dim), BF16), pltpu.VMEM((half, dim), BF16),
        pltpu.VMEM((n_blk, stack, head), BF16), pltpu.VMEM((stack, ext), F32),
        pltpu.VMEM((unit, rows), F32), pltpu.VMEM((unit, rows), F32), pltpu.VMEM((unit, 128), F32), pltpu.VMEM((unit, 128), F32),
        pltpu.VMEM((unit, rows), BF16), pltpu.VMEM((unit, rows), BF16),
        pltpu.VMEM((n_blk, stack, head), F32), pltpu.VMEM((n_blk, stack, 128), F32), pltpu.VMEM((n_blk, stack, 128), F32),
        pltpu.VMEM((unit, 128), F32), pltpu.VMEM((unit, 128), F32), pltpu.VMEM((n_dev * slab, head), BF16))
    pl.run_scoped(feed_forward, pltpu.VMEM((part, dim), F32), pltpu.VMEM((part, BLK), BF16),
                  pltpu.VMEM((n_tile, dim, TILE), BF16), pltpu.VMEM((n_tile, TILE, dim), BF16))
    for k in range(1, n_dev):
        src = lax.rem(me + n_dev - k, n_dev)
        yg_copy(k, src, src).wait_recv()
    last = pltpu.make_async_copy(yg_s, yg_hbm, out_sem.at[PARTS])
    last.start()
    for k in range(1, n_dev):
        yg_copy(k, lax.rem(me + k, n_dev), me).wait_send()
    for p in range(PARTS):
        out_copy(p).wait()
    last.wait()


def gelu(x):
    scale = math.sqrt(2.0 / math.pi)
    part = 0.5 * x
    return part + part * jnp.tanh(x * (scale + (scale * 0.044715) * (x * x)))


def layer(x, wq, wk, wv, wo, w1, w2, rel_bias, gp, n_dev):
    rows, dim = x.shape
    heads, head = wq.shape[1:]
    width = (rel_bias.shape[1] - 1) // 2
    n_glob = gp.shape[1]
    per = n_glob // n_dev
    slab = heads * per
    any_spec = pl.BlockSpec(memory_space=pl.ANY)
    vmem_spec = pl.BlockSpec(memory_space=pltpu.VMEM)
    dma = pltpu.SemaphoreType.DMA
    return pl.pallas_call(
        functools.partial(layer_kernel, n_dev, heads, width),
        name='layer',
        out_shape=(jax.ShapeDtypeStruct((rows, dim), BF16), jax.ShapeDtypeStruct((n_glob, dim), BF16)),
        in_specs=[any_spec] * 7 + [vmem_spec] * 2,
        out_specs=(any_spec, any_spec),
        scratch_shapes=[
            pltpu.VMEM(x.shape, BF16), pltpu.VMEM(wo.shape, BF16), pltpu.VMEM((2, 3 * BLK, 2 * head), BF16),
            pltpu.VMEM((8, BLK + 2 * width), F32), pltpu.VMEM((8, rows + 2 * width), F32),
            pltpu.VMEM((n_glob // 2, dim), BF16), pltpu.VMEM((2, n_glob // 4, dim), BF16), pltpu.VMEM((2, n_glob // 4, dim), BF16),
            pltpu.VMEM((n_glob, dim), BF16),
            pltpu.VMEM((n_dev * slab, head), F32), pltpu.VMEM((n_dev, slab, head), F32),
            pltpu.VMEM((n_dev, 8, slab), F32), pltpu.VMEM((n_dev, 8, slab), F32),
            pltpu.VMEM((rows + per, dim), BF16), pltpu.VMEM((n_glob, dim), BF16), pltpu.VMEM((rows, heads * head), BF16),
            dma((5,)), dma((6,)), dma((6,)), dma((4,)), dma((4,)), dma((n_dev,)), dma((n_dev,)), dma((n_dev,)), dma((n_dev,)),
            dma((n_dev,)), dma((n_dev,)), dma((w1.shape[1] // TILE,)), dma((w1.shape[1] // TILE,)), dma((PARTS + 1,)),
        ],
        compiler_params=pltpu.CompilerParams(collective_id=0, has_side_effects=True, vmem_limit_bytes=67043328),
    )(x, wq, wk, wv, wo, w1, w2, rel_bias, gp)


def place_kernel(ys_hbm, yg_hbm, gp_ref, y_hbm, yo_hbm, ys_s, y_s, yg_s, in_sem, out_sem):
    n = ys_s.shape[0]
    n_glob = gp_ref.shape[1]
    gets = [pltpu.make_async_copy(ys_hbm.at[pl.ds(i * PIECE, PIECE)], ys_s.at[i], in_sem.at[i]) for i in range(n)]
    puts = [pltpu.make_async_copy(y_s.at[i], y_hbm.at[pl.ds(i * PIECE, PIECE)], out_sem.at[i]) for i in range(n)]
    get_g = pltpu.make_async_copy(yg_hbm, yg_s, in_sem.at[n])
    put_g = pltpu.make_async_copy(yg_s, yo_hbm, out_sem.at[n])
    get_g.start()
    for c in gets:
        c.start()
    get_g.wait()
    put_g.start()
    for i in range(n):
        first = (lax.axis_index('sp') * n + i) * PIECE
        hit = gp_ref[...] == first + lax.broadcasted_iota(jnp.int32, (PIECE, n_glob), 0)
        sel = hit.astype(F32)
        placed = mm(sel.astype(BF16), yg_s[...]).astype(BF16)
        is_glob = jnp.max(sel, axis=1, keepdims=True) > 0.0
        gets[i].wait()
        y_s[i] = jnp.where(is_glob, placed, ys_s[i])
        puts[i].start()
    for c in puts:
        c.wait()
    put_g.wait()


def place(ys, yg, gp):
    rows, dim = ys.shape
    n = rows // PIECE
    any_spec = pl.BlockSpec(memory_space=pl.ANY)
    dma = pltpu.SemaphoreType.DMA
    return pl.pallas_call(
        place_kernel,
        name='place',
        out_shape=(jax.ShapeDtypeStruct(ys.shape, BF16), jax.ShapeDtypeStruct(yg.shape, BF16)),
        in_specs=[any_spec, any_spec, pl.BlockSpec(memory_space=pltpu.VMEM)],
        out_specs=(any_spec, any_spec),
        scratch_shapes=[pltpu.VMEM((n, PIECE, dim), BF16), pltpu.VMEM((n, PIECE, dim), BF16), pltpu.VMEM(yg.shape, BF16),
                        dma((n + 1,)), dma((n + 1,))],
        compiler_params=pltpu.CompilerParams(vmem_limit_bytes=60 << 20),
    )(ys, yg, gp)


def solution(mesh):
    n_dev = mesh.shape['sp']

    def shard_layer(hidden_in, w_query, w_key, w_value, w_out, w_up, w_down, rel_bias, glob_pos):
        dim = hidden_in.shape[1]
        heads, head = w_query.shape[1], w_query.shape[2]
        gp = glob_pos.reshape(1, -1)
        ys, yg = layer(hidden_in, w_query, w_key.reshape(dim, head), w_value.reshape(dim, head),
                       w_out.reshape(heads * head, dim), w_up, w_down, rel_bias, gp, n_dev)
        return place(ys, yg, gp)

    return jax.shard_map(
        shard_layer, mesh=mesh,
        in_specs=(P(('dp', 'sp'), None), P(), P(), P(), P(), P(), P(), P(), P('dp')),
        out_specs=(P(('dp', 'sp'), None), P('dp', None)),
        check_vma=False)
```

```python
import functools
import math

import jax
import jax.numpy as jnp
from jax import lax
from jax.experimental import pallas as pl
from jax.experimental.pallas import tpu as pltpu
from jax.sharding import PartitionSpec as P

BF16 = jnp.bfloat16
F32 = jnp.float32
NEG = -math.inf
BLK = 256
ROW = 32
PIECE = 256
PARTS = 3
TILE = 768
WIDE = 3


def mm(a, b):
    return jnp.dot(a, b, preferred_element_type=F32)


def mm_nt(a, b):
    return lax.dot_general(a, b, (((1,), (1,)), ((), ())), preferred_element_type=F32)


def remote(src, dst, send, recv, dev):
    return pltpu.make_async_remote_copy(
        src_ref=src, dst_ref=dst, send_sem=send, recv_sem=recv,
        device_id={'sp': dev}, device_id_type=pl.DeviceIdType.MESH)


def announce(me, n_dev):
    barrier = pltpu.get_barrier_semaphore()
    for k in range(1, n_dev):
        pl.semaphore_signal(barrier, inc=1, device_id={'sp': lax.rem(me + k, n_dev)}, device_id_type=pl.DeviceIdType.MESH)
    return barrier


def diagonal(n):
    return lax.broadcasted_iota(jnp.int32, (n, n), 0) == lax.broadcasted_iota(jnp.int32, (n, n), 1)


def row_to_column(row):
    n = row.shape[1]
    return jnp.sum(jnp.where(diagonal(n), jnp.broadcast_to(row, (n, n)), 0.0), axis=1, keepdims=True)


def column_to_row(col):
    n = col.shape[0]
    return jnp.sum(jnp.where(diagonal(n), jnp.broadcast_to(col, (n, n)), 0.0), axis=0, keepdims=True)


def lane_max(s):
    best = s[:, :128]
    for c in range(128, s.shape[1], 128):
        best = jnp.maximum(best, s[:, c:c + 128])
    return best


def layer_kernel(n_dev, heads, width,
                 x_hbm, wq_hbm, wk_hbm, wv_hbm, wo_hbm, w1_hbm, w2_hbm, rb_ref, gp_ref, ys_hbm, yg_hbm,
                 x_s, wo_s, halo_s, row_s, mask_s, xp_recv, xa_recv, xb_recv, xg_all, rs_send, rs_recv, st_send, st_recv,
                 hid_s, yg_s, att_s,
                 in_sem, x_ssem, x_rsem, halo_ssem, halo_rsem, rs_ssem, rs_rsem, st_ssem, st_rsem, yg_ssem, yg_rsem,
                 w1_sem, w2_sem, out_sem):
    rows, dim = x_s.shape
    head = wk_hbm.shape[1]
    n_glob = gp_ref.shape[1]
    per = n_glob // n_dev
    slab = heads * per
    n_blk = rows // BLK
    stack = heads * BLK
    unit = stack // 2
    ext = BLK + 2 * width
    part = (rows + per) // PARTS
    split = part * (PARTS - 1) - per
    n_tile = w1_hbm.shape[1] // TILE
    me = lax.axis_index('sp')
    start = me * rows
    core = lax.rem(me, 2)
    chip = me // 2
    partner = me + 1 - 2 * core
    x_peer = 2 * (chip + 1 - 2 * lax.rem(chip, 2)) + core
    y_peer = 2 * lax.rem(chip + 2, 4) + core
    half = n_glob // 2
    quart = n_glob // 4

    def rs_copies(k):
        peer = lax.rem(me + k, n_dev)
        return (remote(rs_send.at[pl.ds(peer * slab, slab)], rs_recv.at[k], rs_ssem.at[k], rs_rsem.at[k], peer),
                remote(st_send.at[peer], st_recv.at[k], st_ssem.at[k], st_rsem.at[k], peer))

    def front(wq3_s, wq_s, wk_s, wv_s, kv_s, xg_send, xh_s, xh2_s, q_s, bias_s, s0, s1, t0, t1, p0, p1, o_s, m_s, l_s, mg_s, lg_s, qg_s):
        loads = [pltpu.make_async_copy(src, dst, in_sem.at[i]) for i, (src, dst) in enumerate(
            [(x_hbm, x_s), (wk_hbm, wk_s), (wv_hbm, wv_s), (wq_hbm, wq3_s), (wo_hbm, wo_s)])]
        for c in loads[:3]:
            c.start()
        barrier = announce(me, n_dev)

        gp_col = row_to_column(gp_ref[...].astype(F32)).astype(jnp.int32)
        own = gp_col == start + lax.broadcasted_iota(jnp.int32, (n_glob, rows), 1)
        pos = start - width + lax.broadcasted_iota(jnp.int32, (1, rows + 2 * width), 1)
        hit = jnp.max((gp_col == pos).astype(F32), axis=0, keepdims=True) > 0.0
        bad = hit | (pos < 0) | (pos >= rows * n_dev)
        mask_s[...] = jnp.broadcast_to(jnp.where(bad, NEG, 0.0), mask_s.shape)

        row_s[...] = jnp.full(row_s.shape, NEG, F32)
        row_s[:heads, :2 * width] = rb_ref[:, :2 * width]
        last = jnp.broadcast_to(rb_ref[:, 2 * width:], (heads, 128))
        row_s[:heads, 2 * width:2 * width + 128] = jnp.where(lax.broadcasted_iota(jnp.int32, (heads, 128), 1) == 0, last, NEG)
        for h in range(heads):
            wide = jnp.broadcast_to(row_s[h:h + 1, :], (BLK, ext))
            bias_s[h * BLK:(h + 1) * BLK, :] = pltpu.roll(wide, 0, 1, stride=1, stride_axis=0)

        loads[0].wait()
        loads[3].start()
        x = x_s[...]

        xg_send[...] = mm(own.astype(F32).astype(BF16), x).astype(BF16)
        pair = remote(xg_send.at[pl.ds((1 - core) * half, half)], xp_recv, x_ssem.at[0], x_rsem.at[0], partner)
        pl.semaphore_wait(barrier, n_dev - 1)
        pair.start()

        loads[1].wait()
        loads[2].wait()
        kv_s[:, :head] = mm(x, wk_s[...]).astype(BF16)
        kv_s[:, head:] = mm(x, wv_s[...]).astype(BF16)

        near, far = 1 - core, core
        has_far = (me > 0) & (me < n_dev - 1)
        far_peer = lax.rem(me + n_dev - 1 + 2 * core, n_dev)

        def halo_copies(mine, theirs, peer, sem, pieces):
            out = []
            for k, (at, size) in enumerate(pieces):
                blk = at // BLK + theirs - 2 * (at // BLK) * theirs
                out.append(remote(kv_s.at[pl.ds(mine * width + blk * BLK + at % BLK, size)], halo_s.at[theirs, pl.ds(at, size)],
                                  halo_ssem.at[sem + k], halo_rsem.at[sem + k], peer))
            return out

        loads[4].start()
        to_near = halo_copies(near, core, partner, 0, ((0, BLK), (BLK, BLK)))
        to_far = halo_copies(far, 1 - core, far_peer, 2, ((0, BLK), (BLK, BLK // 2), (BLK + BLK // 2, BLK // 2)))
        for c in to_near:
            c.start()

        pair.wait_recv()
        xh_s[...] = (xg_send[pl.ds(core * half, half), :].astype(F32) + xp_recv[...].astype(F32)).astype(BF16)
        swap = [remote(xh_s.at[pl.ds(0, quart)], xa_recv.at[0], x_ssem.at[1], x_rsem.at[1], x_peer),
                remote(xh_s.at[pl.ds(quart, quart)], xa_recv.at[1], x_ssem.at[2], x_rsem.at[2], y_peer)]
        for c in swap:
            c.start()

        @pl.when(has_far)
        def _():
            to_far[1].start()

        loads[3].wait()
        wq_s[...] = wq3_s[...].reshape(wq_s.shape)
        for h in range(heads):
            qh = (mm(x, wq_s[:, h * head:(h + 1) * head]) * head ** -0.5).astype(BF16)
            for b in range(n_blk):
                q_s[b, h * BLK:(h + 1) * BLK, :] = qh[b * BLK:(b + 1) * BLK]

        class Local:
            def __init__(self, b, g, before=None):
                self.b, self.r0, self.before = b, g * unit, before
                self.lo, self.hi = max(0, b * BLK - width), min(rows, (b + 1) * BLK + width)

            def score(self, s_ref, t_ref):
                n, c0 = self.hi - self.lo, self.lo - self.b * BLK + width
                s = mm_nt(q_s[self.b, self.r0:self.r0 + unit], kv_s[self.lo:self.hi, :head])
                s = s + bias_s[self.r0:self.r0 + unit, c0:c0 + n] + mask_s[0:1, width + self.lo:width + self.hi]
                s_ref[:, :n] = s
                t_ref[...] = lane_max(s)

            def soft(self, s_ref, t_ref, p_ref):
                n = self.hi - self.lo
                for r in range(0, unit, ROW):
                    rs, ra = slice(r, r + ROW), slice(self.r0 + r, self.r0 + r + ROW)
                    top = jnp.max(t_ref[rs, :], axis=1, keepdims=True)
                    p = jnp.exp(s_ref[rs, :n] - top)
                    p_ref[rs, :n] = p.astype(BF16)
                    m_s[self.b, ra, :] = jnp.broadcast_to(top, (ROW, 128))
                    l_s[self.b, ra, :] = jnp.broadcast_to(jnp.sum(p, axis=1, keepdims=True), (ROW, 128))

            def value(self, p_ref):
                o_s[self.b, self.r0:self.r0 + unit] = mm(p_ref[:, :self.hi - self.lo], kv_s[self.lo:self.hi, head:])

        class Global:
            def __init__(self, g, before=None):
                self.r0, self.before = g * unit, before

            def score(self, s_ref, t_ref):
                s = mm_nt(qg_s[self.r0:self.r0 + unit, :], kv_s[:, :head])
                s_ref[...] = s
                t_ref[...] = lane_max(s)

            def soft(self, s_ref, t_ref, p_ref):
                for r in range(0, unit, ROW):
                    rs = slice(r, r + ROW)
                    top = jnp.max(t_ref[rs, :], axis=1, keepdims=True)
                    p = jnp.exp(s_ref[rs, :] - top)
                    p_ref[rs, :] = p.astype(BF16)
                    mg_s[rs, :] = jnp.broadcast_to(top, (ROW, 128))
                    lg_s[rs, :] = jnp.broadcast_to(jnp.sum(p, axis=1, keepdims=True), (ROW, 128))
                for j in range(unit // slab):
                    cut, to = slice(j * slab, (j + 1) * slab), self.r0 // slab + j
                    st_send[to, 0:1, :] = jnp.sum(jnp.where(diagonal(slab), mg_s[cut, :], 0.0), axis=0, keepdims=True)
                    st_send[to, 1:2, :] = jnp.sum(jnp.where(diagonal(slab), lg_s[cut, :], 0.0), axis=0, keepdims=True)

            def value(self, p_ref):
                rs_send[self.r0:self.r0 + unit, :] = mm(p_ref[...], kv_s[:, head:])

        class Far:
            def __init__(self, side, inner, g, before=None):
                self.side, self.inner, self.r0, self.before = side, inner, g * unit, before
                self.b = 1 + side * (n_blk - 3) if inner else side * (n_blk - 1)
                self.k0, self.n = (BLK, 2 * BLK) if inner else (0, 3 * BLK)

            def score(self, s_ref, t_ref):
                side, n = self.side, self.n
                near_mask = BLK + side * (rows + BLK)
                if self.inner:
                    cuts = [(side * (ext - BLK), near_mask)]
                else:
                    cuts = [(side * (ext - BLK), side * (rows + width + BLK)), (BLK + side * (ext - 3 * BLK), near_mask)]
                s = mm_nt(q_s[self.b, self.r0:self.r0 + unit], halo_s[side, self.k0:, :head])
                best = lane_max(s[:, n - BLK:])
                s_ref[:, n - BLK:n] = s[:, n - BLK:]
                for i, (c0, m0) in enumerate(cuts):
                    cut = (s[:, i * BLK:(i + 1) * BLK] + bias_s[self.r0:self.r0 + unit, pl.ds(pl.multiple_of(c0, BLK), BLK)]
                           + mask_s[0:1, pl.ds(pl.multiple_of(m0, BLK), BLK)])
                    s_ref[:, i * BLK:(i + 1) * BLK] = cut
                    best = jnp.maximum(best, lane_max(cut))
                t_ref[...] = best

            def soft(self, s_ref, t_ref, p_ref):
                n = self.n
                for r in range(0, unit, ROW):
                    rs, ra = slice(r, r + ROW), slice(self.r0 + r, self.r0 + r + ROW)
                    m1 = m_s[self.b, ra, :]
                    top = jnp.maximum(m1, jnp.broadcast_to(jnp.max(t_ref[rs, :], axis=1, keepdims=True), (ROW, 128)))
                    s = s_ref[rs, :n]
                    p = jnp.exp(s - jnp.concatenate([top] * (n // 128), axis=1))
                    p_ref[rs, :n] = p.astype(BF16)
                    fac = jnp.exp(m1 - top)
                    inv = 1.0 / (l_s[self.b, ra, :] * fac + jnp.broadcast_to(jnp.sum(p, axis=1, keepdims=True), (ROW, 128)))
                    m_s[self.b, ra, :] = fac * inv
                    l_s[self.b, ra, :] = inv

            def value(self, p_ref):
                at = pl.ds(pl.multiple_of(self.b * BLK, BLK), BLK)
                new = mm(p_ref[:, :self.n], halo_s[self.side, self.k0:, head:])
                for h in range(unit // BLK):
                    ra = slice(self.r0 + h * BLK, self.r0 + (h + 1) * BLK)
                    fac, inv = m_s[self.b, ra, :], l_s[self.b, ra, :]
                    o = (o_s[self.b, ra, :] * jnp.concatenate([fac] * (head // 128), axis=1)
                         + new[h * BLK:(h + 1) * BLK] * jnp.concatenate([inv] * (head // 128), axis=1))
                    col = (self.r0 // BLK + h) * head
                    att_s[at, col:col + head] = o.astype(BF16)

        swap2 = [remote(xh2_s.at[pl.ds(0, quart)], xb_recv.at[0], x_ssem.at[3], x_rsem.at[3], y_peer),
                 remote(xh2_s.at[pl.ds(quart, quart)], xb_recv.at[1], x_ssem.at[4], x_rsem.at[4], x_peer)]
        mine = core * half
        spread = remote(xg_all.at[pl.ds(mine, half)], xg_all.at[pl.ds(mine, half)], x_ssem.at[5], x_rsem.at[5], partner)

        def second_swap():
            for c in swap:
                c.wait_recv()
            xh2_s[:quart, :] = (xh_s[:quart, :].astype(F32) + xa_recv[0].astype(F32)).astype(BF16)
            xh2_s[quart:, :] = (xh_s[quart:, :].astype(F32) + xa_recv[1].astype(F32)).astype(BF16)
            for c in swap2:
                c.start()

            @pl.when(has_far)
            def _():
                to_far[2].start()
                to_far[0].start()

            @pl.when(jnp.logical_not(has_far))
            def _():
                halo_s[core, :2 * BLK, :] = jnp.zeros((2 * BLK, 2 * head), BF16)

        def share():
            for c in swap2:
                c.wait_recv()
            xg_all[pl.ds(mine, quart), :] = (xh2_s[:quart, :].astype(F32) + xb_recv[0].astype(F32)).astype(BF16)
            xg_all[pl.ds(mine + quart, quart), :] = (xh2_s[quart:, :].astype(F32) + xb_recv[1].astype(F32)).astype(BF16)
            spread.start()

        def project_global():
            theirs = xg_all.at[pl.ds(half - mine, half)]
            remote(theirs, theirs, x_ssem.at[5], x_rsem.at[5], partner).wait_recv()
            xg = xg_all[...]
            for h in range(heads):
                qh = (mm(xg, wq_s[:, h * head:(h + 1) * head]) * head ** -0.5).astype(BF16)
                for j in range(n_dev):
                    at = (j * heads + h) * per
                    qg_s[at:at + per, :] = qh[j * per:(j + 1) * per]
            for j, w in enumerate((wk_s, wv_s)):
                both = mm(xg, w[...]).astype(BF16)
                for side in range(2):
                    halo_s[side, 2 * BLK:, j * head:(j + 1) * head] = both

        def near_ready():
            for c in to_near:
                c.wait_recv()

        def wait_far(i):
            @pl.when(has_far)
            def _():
                to_far[i].wait_recv()

        def inner_ready():
            wait_far(1)
            wait_far(2)

        def outer_ready():
            wait_far(0)
            for k in range(1, n_dev):
                for c in rs_copies(k):
                    c.start()

        hooks = {2: second_swap, 7: share}
        units = [Local(i // 2, i % 2, hooks.get(i)) for i in range(2 * n_blk)]
        units += [Global(0, project_global), Global(1)]
        units += [Far(near, False, 0, near_ready), Far(near, False, 1), Far(near, True, 0), Far(near, True, 1)]
        units += [Far(far, True, 0, inner_ready), Far(far, True, 1), Far(far, False, 0, outer_ready), Far(far, False, 1)]
        s_refs, t_refs, p_refs = (s0, s1), (t0, t1), (p0, p1)
        for i, u in enumerate(units):
            for k in ((0, 1) if i == 0 else (i + 1,)):
                if k < len(units):
                    if units[k].before is not None:
                        units[k].before()
                    units[k].score(s_refs[k % 2], t_refs[k % 2])
            u.soft(s_refs[i % 2], t_refs[i % 2], p_refs[i % 2])
            u.value(p_refs[i % 2])

        for c in [pair] + swap + swap2 + [spread] + to_near:
            c.wait_send()

        @pl.when(has_far)
        def _():
            for c in to_far:
                c.wait_send()

    def finish_global():
        for k in range(1, n_dev):
            for c in rs_copies(k):
                c.wait()
        rs_recv[0] = rs_send[pl.ds(me * slab, slab), :]
        st_recv[0] = st_send[me]
        top = st_recv[0, 0:1, :]
        for k in range(1, n_dev):
            top = jnp.maximum(top, st_recv[k, 0:1, :])
        tot = jnp.zeros((1, slab), F32)
        o = jnp.zeros((slab, head), F32)
        for k in range(n_dev):
            fac = jnp.exp(st_recv[k, 0:1, :] - top)
            tot = tot + st_recv[k, 1:2, :] * fac
            o = o + rs_recv[k] * row_to_column(fac)
        o = (o / row_to_column(tot)).astype(BF16)
        hg = xg_all[pl.ds(me * per, per), :].astype(F32)
        for h in range(heads):
            hg = hg + mm(o[h * per:(h + 1) * per], wo_s[h * head:(h + 1) * head, :])
        hid_s[split:split + per, :] = hg.astype(BF16)

    def yg_copy(k, peer, owner):
        return remote(hid_s.at[pl.ds(split, per)], yg_s.at[pl.ds(owner * per, per)], yg_ssem.at[k], yg_rsem.at[k], peer)

    def out_copy(p):
        lo, hi = p * part, min((p + 1) * part, split) if p < PARTS - 1 else rows
        if p == PARTS - 1:
            lo = split
        shift = per if p == PARTS - 1 else 0
        return pltpu.make_async_copy(hid_s.at[pl.ds(lo + shift, hi - lo)], ys_hbm.at[pl.ds(lo, hi - lo)], out_sem.at[p])

    def feed_forward(acc_s, u_s, w1_s, w2_s):
        def w_copies(i):
            at = pl.ds(i * TILE, TILE)
            return (pltpu.make_async_copy(w1_hbm.at[:, at], w1_s.at[i], w1_sem.at[i]),
                    pltpu.make_async_copy(w2_hbm.at[at, :], w2_s.at[i], w2_sem.at[i]))

        for i in range(n_tile):
            for c in w_copies(i):
                c.start()

        pltpu.make_async_copy(wo_hbm, wo_s, in_sem.at[4]).wait()
        for b in range(n_blk):
            r0, r1 = b * BLK, (b + 1) * BLK
            res = (x_s[r0:r1, :].astype(F32) + mm(att_s[r0:r1, :], wo_s[...])).astype(BF16)
            cut = min(max(split - r0, 0), BLK)
            if cut:
                hid_s[r0:r0 + cut, :] = res[:cut]
            if cut < BLK:
                hid_s[r0 + cut + per:r1 + per, :] = res[cut:]

        def chunks(r, i, count):
            u = u_s[...]
            for c in range(count):
                g, at = i + c // (TILE // BLK), c % (TILE // BLK) * BLK
                s = mm(hid_s[r, :], w1_s[g, :, at:at + BLK])
                if c == 0:
                    acc_s[...] += mm(u, w2_s[jnp.maximum(i - 1, 0), TILE - BLK:, :])
                else:
                    b = c - 1
                    at = b % (TILE // BLK) * BLK
                    acc_s[...] += mm(u, w2_s[i + b // (TILE // BLK), at:at + BLK, :])
                u = gelu(s).astype(BF16)
            u_s[...] = u

        def run_part(r, steps, step):
            acc_s[...] = hid_s[r, :].astype(F32)
            u_s[...] = jnp.zeros_like(u_s)
            lax.fori_loop(0, steps, step, 0)
            hid_s[r, :] = (acc_s[...] + mm(u_s[...], w2_s[n_tile - 1, TILE - BLK:, :])).astype(BF16)

        def first(i, carry):
            for c in w_copies(i):
                c.wait()
            chunks(slice(0, part), i, TILE // BLK)
            return carry

        run_part(slice(0, part), n_tile, first)
        out_copy(0).start()
        finish_global()

        def later(p, carry):
            r = pl.ds(pl.multiple_of(p * part, 16), part)

            def step(i, carry):
                chunks(r, i * WIDE, WIDE * (TILE // BLK))
                return carry

            run_part(r, n_tile // WIDE, step)

            @pl.when(p == PARTS - 2)
            def _():
                for k in range(1, n_dev):
                    yg_copy(k, lax.rem(me + k, n_dev), me).start()
                yg_s[pl.ds(me * per, per), :] = hid_s[split:split + per, :]

            for q in range(1, PARTS):
                @pl.when(p == q)
                def _():
                    out_copy(q).start()

            return carry

        lax.fori_loop(1, PARTS, later, 0)

    pl.run_scoped(
        front,
        pltpu.VMEM(wq_hbm.shape, BF16), pltpu.VMEM((dim, heads * head), BF16), pltpu.VMEM((dim, head), BF16), pltpu.VMEM((dim, head), BF16),
        pltpu.VMEM((rows, 2 * head), BF16),
        pltpu.VMEM((n_glob, dim), BF16), pltpu.VMEM((half, dim), BF16), pltpu.VMEM((half, dim), BF16),
        pltpu.VMEM((n_blk, stack, head), BF16), pltpu.VMEM((stack, ext), F32),
        pltpu.VMEM((unit, rows), F32), pltpu.VMEM((unit, rows), F32), pltpu.VMEM((unit, 128), F32), pltpu.VMEM((unit, 128), F32),
        pltpu.VMEM((unit, rows), BF16), pltpu.VMEM((unit, rows), BF16),
        pltpu.VMEM((n_blk, stack, head), F32), pltpu.VMEM((n_blk, stack, 128), F32), pltpu.VMEM((n_blk, stack, 128), F32),
        pltpu.VMEM((unit, 128), F32), pltpu.VMEM((unit, 128), F32), pltpu.VMEM((n_dev * slab, head), BF16))
    pl.run_scoped(feed_forward, pltpu.VMEM((part, dim), F32), pltpu.VMEM((part, BLK), BF16),
                  pltpu.VMEM((n_tile, dim, TILE), BF16), pltpu.VMEM((n_tile, TILE, dim), BF16))
    for k in range(1, n_dev):
        src = lax.rem(me + n_dev - k, n_dev)
        yg_copy(k, src, src).wait_recv()
    last = pltpu.make_async_copy(yg_s, yg_hbm, out_sem.at[PARTS])
    last.start()
    for k in range(1, n_dev):
        yg_copy(k, lax.rem(me + k, n_dev), me).wait_send()
    for p in range(PARTS):
        out_copy(p).wait()
    last.wait()


def gelu(x):
    scale = math.sqrt(2.0 / math.pi)
    part = 0.5 * x
    return part + part * jnp.tanh(x * (scale + (scale * 0.044715) * (x * x)))


def layer(x, wq, wk, wv, wo, w1, w2, rel_bias, gp, n_dev):
    rows, dim = x.shape
    heads, head = wq.shape[1:]
    width = (rel_bias.shape[1] - 1) // 2
    n_glob = gp.shape[1]
    per = n_glob // n_dev
    slab = heads * per
    any_spec = pl.BlockSpec(memory_space=pl.ANY)
    vmem_spec = pl.BlockSpec(memory_space=pltpu.VMEM)
    dma = pltpu.SemaphoreType.DMA
    return pl.pallas_call(
        functools.partial(layer_kernel, n_dev, heads, width),
        name='layer',
        out_shape=(jax.ShapeDtypeStruct((rows, dim), BF16), jax.ShapeDtypeStruct((n_glob, dim), BF16)),
        in_specs=[any_spec] * 7 + [vmem_spec] * 2,
        out_specs=(any_spec, any_spec),
        scratch_shapes=[
            pltpu.VMEM(x.shape, BF16), pltpu.VMEM(wo.shape, BF16), pltpu.VMEM((2, 3 * BLK, 2 * head), BF16),
            pltpu.VMEM((8, BLK + 2 * width), F32), pltpu.VMEM((8, rows + 2 * width), F32),
            pltpu.VMEM((n_glob // 2, dim), BF16), pltpu.VMEM((2, n_glob // 4, dim), BF16), pltpu.VMEM((2, n_glob // 4, dim), BF16),
            pltpu.VMEM((n_glob, dim), BF16),
            pltpu.VMEM((n_dev * slab, head), F32), pltpu.VMEM((n_dev, slab, head), F32),
            pltpu.VMEM((n_dev, 8, slab), F32), pltpu.VMEM((n_dev, 8, slab), F32),
            pltpu.VMEM((rows + per, dim), BF16), pltpu.VMEM((n_glob, dim), BF16), pltpu.VMEM((rows, heads * head), BF16),
            dma((5,)), dma((6,)), dma((6,)), dma((5,)), dma((5,)), dma((n_dev,)), dma((n_dev,)), dma((n_dev,)), dma((n_dev,)),
            dma((n_dev,)), dma((n_dev,)), dma((w1.shape[1] // TILE,)), dma((w1.shape[1] // TILE,)), dma((PARTS + 1,)),
        ],
        compiler_params=pltpu.CompilerParams(collective_id=0, has_side_effects=True, vmem_limit_bytes=67043328),
    )(x, wq, wk, wv, wo, w1, w2, rel_bias, gp)


def place_kernel(ys_hbm, yg_hbm, gp_ref, y_hbm, yo_hbm, ys_s, y_s, yg_s, in_sem, out_sem):
    n = ys_s.shape[0]
    n_glob = gp_ref.shape[1]
    gets = [pltpu.make_async_copy(ys_hbm.at[pl.ds(i * PIECE, PIECE)], ys_s.at[i], in_sem.at[i]) for i in range(n)]
    puts = [pltpu.make_async_copy(y_s.at[i], y_hbm.at[pl.ds(i * PIECE, PIECE)], out_sem.at[i]) for i in range(n)]
    get_g = pltpu.make_async_copy(yg_hbm, yg_s, in_sem.at[n])
    put_g = pltpu.make_async_copy(yg_s, yo_hbm, out_sem.at[n])
    get_g.start()
    for c in gets:
        c.start()
    get_g.wait()
    put_g.start()
    for i in range(n):
        first = (lax.axis_index('sp') * n + i) * PIECE
        hit = gp_ref[...] == first + lax.broadcasted_iota(jnp.int32, (PIECE, n_glob), 0)
        sel = hit.astype(F32)
        placed = mm(sel.astype(BF16), yg_s[...]).astype(BF16)
        is_glob = jnp.max(sel, axis=1, keepdims=True) > 0.0
        gets[i].wait()
        y_s[i] = jnp.where(is_glob, placed, ys_s[i])
        puts[i].start()
    for c in puts:
        c.wait()
    put_g.wait()


def place(ys, yg, gp):
    rows, dim = ys.shape
    n = rows // PIECE
    any_spec = pl.BlockSpec(memory_space=pl.ANY)
    dma = pltpu.SemaphoreType.DMA
    return pl.pallas_call(
        place_kernel,
        name='place',
        out_shape=(jax.ShapeDtypeStruct(ys.shape, BF16), jax.ShapeDtypeStruct(yg.shape, BF16)),
        in_specs=[any_spec, any_spec, pl.BlockSpec(memory_space=pltpu.VMEM)],
        out_specs=(any_spec, any_spec),
        scratch_shapes=[pltpu.VMEM((n, PIECE, dim), BF16), pltpu.VMEM((n, PIECE, dim), BF16), pltpu.VMEM(yg.shape, BF16),
                        dma((n + 1,)), dma((n + 1,))],
        compiler_params=pltpu.CompilerParams(vmem_limit_bytes=60 << 20),
    )(ys, yg, gp)


def solution(mesh):
    n_dev = mesh.shape['sp']

    def shard_layer(hidden_in, w_query, w_key, w_value, w_out, w_up, w_down, rel_bias, glob_pos):
        dim = hidden_in.shape[1]
        heads, head = w_query.shape[1], w_query.shape[2]
        gp = glob_pos.reshape(1, -1)
        ys, yg = layer(hidden_in, w_query, w_key.reshape(dim, head), w_value.reshape(dim, head),
                       w_out.reshape(heads * head, dim), w_up, w_down, rel_bias, gp, n_dev)
        return place(ys, yg, gp)

    return jax.shard_map(
        shard_layer, mesh=mesh,
        in_specs=(P(('dp', 'sp'), None), P(), P(), P(), P(), P(), P(), P(), P('dp')),
        out_specs=(P(('dp', 'sp'), None), P('dp', None)),
        check_vma=False)
```

```python
import functools
import math

import jax
import jax.numpy as jnp
from jax import lax
from jax.experimental import pallas as pl
from jax.experimental.pallas import tpu as pltpu
from jax.sharding import PartitionSpec as P

BF16 = jnp.bfloat16
F32 = jnp.float32
NEG = -math.inf
BLK = 256
ROW = 32
PIECE = 256
PARTS = 3
TILE = 768
WIDE = 3


def mm(a, b):
    return jnp.dot(a, b, preferred_element_type=F32)


def mm_nt(a, b):
    return lax.dot_general(a, b, (((1,), (1,)), ((), ())), preferred_element_type=F32)


def remote(src, dst, send, recv, dev):
    return pltpu.make_async_remote_copy(
        src_ref=src, dst_ref=dst, send_sem=send, recv_sem=recv,
        device_id={'sp': dev}, device_id_type=pl.DeviceIdType.MESH)


def announce(me, n_dev):
    barrier = pltpu.get_barrier_semaphore()
    for k in range(1, n_dev):
        pl.semaphore_signal(barrier, inc=1, device_id={'sp': lax.rem(me + k, n_dev)}, device_id_type=pl.DeviceIdType.MESH)
    return barrier


def diagonal(n):
    return lax.broadcasted_iota(jnp.int32, (n, n), 0) == lax.broadcasted_iota(jnp.int32, (n, n), 1)


def row_to_column(row):
    n = row.shape[1]
    return jnp.sum(jnp.where(diagonal(n), jnp.broadcast_to(row, (n, n)), 0.0), axis=1, keepdims=True)


def column_to_row(col):
    n = col.shape[0]
    return jnp.sum(jnp.where(diagonal(n), jnp.broadcast_to(col, (n, n)), 0.0), axis=0, keepdims=True)


def lane_max(s):
    best = s[:, :128]
    for c in range(128, s.shape[1], 128):
        best = jnp.maximum(best, s[:, c:c + 128])
    return best


def layer_kernel(n_dev, heads, width,
                 x_hbm, wq_hbm, wk_hbm, wv_hbm, wo_hbm, w1_hbm, w2_hbm, rb_ref, gp_ref, ys_hbm, yg_hbm,
                 x_s, wo_s, halo_s, row_s, mask_s, xp_recv, xa_recv, xb_recv, xg_all, rs_send, rs_recv, st_send, st_recv,
                 hid_s, yg_s, att_s,
                 in_sem, x_ssem, x_rsem, halo_ssem, halo_rsem, rs_ssem, rs_rsem, st_ssem, st_rsem, yg_ssem, yg_rsem,
                 w1_sem, w2_sem, out_sem):
    rows, dim = x_s.shape
    head = wk_hbm.shape[1]
    n_glob = gp_ref.shape[1]
    per = n_glob // n_dev
    slab = heads * per
    n_blk = rows // BLK
    stack = heads * BLK
    unit = stack // 2
    ext = BLK + 2 * width
    part = (rows + per) // PARTS
    split = part * (PARTS - 1) - per
    n_tile = w1_hbm.shape[1] // TILE
    me = lax.axis_index('sp')
    start = me * rows
    core = lax.rem(me, 2)
    chip = me // 2
    partner = me + 1 - 2 * core
    x_peer = 2 * (chip + 1 - 2 * lax.rem(chip, 2)) + core
    y_peer = 2 * lax.rem(chip + 2, 4) + core
    half = n_glob // 2
    quart = n_glob // 4

    def rs_copies(k):
        peer = lax.rem(me + k, n_dev)
        return (remote(rs_send.at[pl.ds(peer * slab, slab)], rs_recv.at[k], rs_ssem.at[k], rs_rsem.at[k], peer),
                remote(st_send.at[peer], st_recv.at[k], st_ssem.at[k], st_rsem.at[k], peer))

    def front(wq3_s, wq_s, wk_s, wv_s, kv_s, xg_send, xh_s, xh2_s, q_s, bias_s, s0, s1, t0, t1, p0, p1, o_s, m_s, l_s, mg_s, lg_s, qg_s):
        loads = [pltpu.make_async_copy(src, dst, in_sem.at[i]) for i, (src, dst) in enumerate(
            [(x_hbm, x_s), (wk_hbm, wk_s), (wv_hbm, wv_s), (wq_hbm, wq3_s), (wo_hbm, wo_s)])]
        for c in loads[:3]:
            c.start()
        barrier = announce(me, n_dev)

        gp_col = row_to_column(gp_ref[...].astype(F32)).astype(jnp.int32)
        own = gp_col == start + lax.broadcasted_iota(jnp.int32, (n_glob, rows), 1)
        pos = start - width + lax.broadcasted_iota(jnp.int32, (1, rows + 2 * width), 1)
        hit = jnp.max((gp_col == pos).astype(F32), axis=0, keepdims=True) > 0.0
        bad = hit | (pos < 0) | (pos >= rows * n_dev)
        mask_s[...] = jnp.broadcast_to(jnp.where(bad, NEG, 0.0), mask_s.shape)

        row_s[...] = jnp.full(row_s.shape, NEG, F32)
        row_s[:heads, :2 * width] = rb_ref[:, :2 * width]
        last = jnp.broadcast_to(rb_ref[:, 2 * width:], (heads, 128))
        row_s[:heads, 2 * width:2 * width + 128] = jnp.where(lax.broadcasted_iota(jnp.int32, (heads, 128), 1) == 0, last, NEG)
        for h in range(heads):
            wide = jnp.broadcast_to(row_s[h:h + 1, :], (BLK, ext))
            bias_s[h * BLK:(h + 1) * BLK, :] = pltpu.roll(wide, 0, 1, stride=1, stride_axis=0)

        loads[0].wait()
        loads[3].start()
        x = x_s[...]

        xg_send[...] = mm(own.astype(F32).astype(BF16), x).astype(BF16)
        pair = remote(xg_send.at[pl.ds((1 - core) * half, half)], xp_recv, x_ssem.at[0], x_rsem.at[0], partner)
        pl.semaphore_wait(barrier, n_dev - 1)
        pair.start()

        loads[1].wait()
        loads[2].wait()
        kv_s[:, :head] = mm(x, wk_s[...]).astype(BF16)
        kv_s[:, head:] = mm(x, wv_s[...]).astype(BF16)

        near, far = 1 - core, core
        has_far = (me > 0) & (me < n_dev - 1)
        far_peer = lax.rem(me + n_dev - 1 + 2 * core, n_dev)

        def halo_copies(mine, theirs, peer, sem, pieces):
            out = []
            for k, (at, size) in enumerate(pieces):
                blk = at // BLK + theirs - 2 * (at // BLK) * theirs
                out.append(remote(kv_s.at[pl.ds(mine * width + blk * BLK + at % BLK, size)], halo_s.at[theirs, pl.ds(at, size)],
                                  halo_ssem.at[sem + k], halo_rsem.at[sem + k], peer))
            return out

        loads[4].start()
        to_near = halo_copies(near, core, partner, 0, ((0, BLK), (BLK, BLK)))
        to_far = halo_copies(far, 1 - core, far_peer, 2, ((0, BLK), (BLK, BLK // 2), (BLK + BLK // 2, BLK // 2)))
        for c in to_near:
            c.start()

        pair.wait_recv()
        xh_s[...] = (xg_send[pl.ds(core * half, half), :].astype(F32) + xp_recv[...].astype(F32)).astype(BF16)
        swap = [remote(xh_s.at[pl.ds(0, quart)], xa_recv.at[0], x_ssem.at[1], x_rsem.at[1], x_peer),
                remote(xh_s.at[pl.ds(quart, quart)], xa_recv.at[1], x_ssem.at[2], x_rsem.at[2], y_peer)]
        for c in swap:
            c.start()

        @pl.when(has_far)
        def _():
            to_far[1].start()

        loads[3].wait()
        wq_s[...] = wq3_s[...].reshape(wq_s.shape)
        for h in range(heads):
            qh = (mm(x, wq_s[:, h * head:(h + 1) * head]) * head ** -0.5).astype(BF16)
            for b in range(n_blk):
                q_s[b, h * BLK:(h + 1) * BLK, :] = qh[b * BLK:(b + 1) * BLK]

        class Local:
            def __init__(self, b, g, before=None):
                self.b, self.r0, self.before = b, g * unit, before
                self.lo, self.hi = max(0, b * BLK - width), min(rows, (b + 1) * BLK + width)

            def score(self, s_ref, t_ref):
                n, c0 = self.hi - self.lo, self.lo - self.b * BLK + width
                s = mm_nt(q_s[self.b, self.r0:self.r0 + unit], kv_s[self.lo:self.hi, :head])
                s = s + bias_s[self.r0:self.r0 + unit, c0:c0 + n] + mask_s[0:1, width + self.lo:width + self.hi]
                s_ref[:, :n] = s
                t_ref[...] = lane_max(s)

            def soft(self, s_ref, t_ref, p_ref):
                n = self.hi - self.lo
                for r in range(0, unit, ROW):
                    rs, ra = slice(r, r + ROW), slice(self.r0 + r, self.r0 + r + ROW)
                    top = jnp.max(t_ref[rs, :], axis=1, keepdims=True)
                    p = jnp.exp(s_ref[rs, :n] - top)
                    p_ref[rs, :n] = p.astype(BF16)
                    m_s[self.b, ra, :] = jnp.broadcast_to(top, (ROW, 128))
                    l_s[self.b, ra, :] = jnp.broadcast_to(jnp.sum(p, axis=1, keepdims=True), (ROW, 128))

            def value(self, p_ref):
                o_s[self.b, self.r0:self.r0 + unit] = mm(p_ref[:, :self.hi - self.lo], kv_s[self.lo:self.hi, head:])

        class Global:
            def __init__(self, g, before=None):
                self.r0, self.before = g * unit, before

            def score(self, s_ref, t_ref):
                s = mm_nt(qg_s[self.r0:self.r0 + unit, :], kv_s[:, :head])
                s_ref[...] = s
                t_ref[...] = lane_max(s)

            def soft(self, s_ref, t_ref, p_ref):
                for r in range(0, unit, ROW):
                    rs = slice(r, r + ROW)
                    top = jnp.max(t_ref[rs, :], axis=1, keepdims=True)
                    p = jnp.exp(s_ref[rs, :] - top)
                    p_ref[rs, :] = p.astype(BF16)
                    mg_s[rs, :] = jnp.broadcast_to(top, (ROW, 128))
                    lg_s[rs, :] = jnp.broadcast_to(jnp.sum(p, axis=1, keepdims=True), (ROW, 128))
                for j in range(unit // slab):
                    cut, to = slice(j * slab, (j + 1) * slab), self.r0 // slab + j
                    st_send[to, 0:1, :] = jnp.sum(jnp.where(diagonal(slab), mg_s[cut, :], 0.0), axis=0, keepdims=True)
                    st_send[to, 1:2, :] = jnp.sum(jnp.where(diagonal(slab), lg_s[cut, :], 0.0), axis=0, keepdims=True)

            def value(self, p_ref):
                rs_send[self.r0:self.r0 + unit, :] = mm(p_ref[...], kv_s[:, head:])

        class Far:
            def __init__(self, side, inner, g, before=None):
                self.side, self.inner, self.r0, self.before = side, inner, g * unit, before
                self.b = 1 + side * (n_blk - 3) if inner else side * (n_blk - 1)
                self.k0, self.n = (BLK, 2 * BLK) if inner else (0, 3 * BLK)

            def score(self, s_ref, t_ref):
                side, n = self.side, self.n
                near_mask = BLK + side * (rows + BLK)
                if self.inner:
                    cuts = [(side * (ext - BLK), near_mask)]
                else:
                    cuts = [(side * (ext - BLK), side * (rows + width + BLK)), (BLK + side * (ext - 3 * BLK), near_mask)]
                s = mm_nt(q_s[self.b, self.r0:self.r0 + unit], halo_s[side, self.k0:, :head])
                best = lane_max(s[:, n - BLK:])
                s_ref[:, n - BLK:n] = s[:, n - BLK:]
                for i, (c0, m0) in enumerate(cuts):
                    cut = (s[:, i * BLK:(i + 1) * BLK] + bias_s[self.r0:self.r0 + unit, pl.ds(pl.multiple_of(c0, BLK), BLK)]
                           + mask_s[0:1, pl.ds(pl.multiple_of(m0, BLK), BLK)])
                    s_ref[:, i * BLK:(i + 1) * BLK] = cut
                    best = jnp.maximum(best, lane_max(cut))
                t_ref[...] = best

            def soft(self, s_ref, t_ref, p_ref):
                n = self.n
                for r in range(0, unit, ROW):
                    rs, ra = slice(r, r + ROW), slice(self.r0 + r, self.r0 + r + ROW)
                    m1 = m_s[self.b, ra, :]
                    top = jnp.maximum(m1, jnp.broadcast_to(jnp.max(t_ref[rs, :], axis=1, keepdims=True), (ROW, 128)))
                    s = s_ref[rs, :n]
                    p = jnp.exp(s - jnp.concatenate([top] * (n // 128), axis=1))
                    p_ref[rs, :n] = p.astype(BF16)
                    fac = jnp.exp(m1 - top)
                    inv = 1.0 / (l_s[self.b, ra, :] * fac + jnp.broadcast_to(jnp.sum(p, axis=1, keepdims=True), (ROW, 128)))
                    m_s[self.b, ra, :] = fac * inv
                    l_s[self.b, ra, :] = inv

            def value(self, p_ref):
                at = pl.ds(pl.multiple_of(self.b * BLK, BLK), BLK)
                new = mm(p_ref[:, :self.n], halo_s[self.side, self.k0:, head:])
                for h in range(unit // BLK):
                    ra = slice(self.r0 + h * BLK, self.r0 + (h + 1) * BLK)
                    fac, inv = m_s[self.b, ra, :], l_s[self.b, ra, :]
                    o = (o_s[self.b, ra, :] * jnp.concatenate([fac] * (head // 128), axis=1)
                         + new[h * BLK:(h + 1) * BLK] * jnp.concatenate([inv] * (head // 128), axis=1))
                    col = (self.r0 // BLK + h) * head
                    att_s[at, col:col + head] = o.astype(BF16)

        swap2 = [remote(xh2_s.at[pl.ds(0, quart)], xb_recv.at[0], x_ssem.at[3], x_rsem.at[3], y_peer),
                 remote(xh2_s.at[pl.ds(quart, quart)], xb_recv.at[1], x_ssem.at[4], x_rsem.at[4], x_peer)]
        mine = core * half
        spread = remote(xg_all.at[pl.ds(mine, half)], xg_all.at[pl.ds(mine, half)], x_ssem.at[5], x_rsem.at[5], partner)

        def second_swap():
            for c in swap:
                c.wait_recv()
            xh2_s[:quart, :] = (xh_s[:quart, :].astype(F32) + xa_recv[0].astype(F32)).astype(BF16)
            xh2_s[quart:, :] = (xh_s[quart:, :].astype(F32) + xa_recv[1].astype(F32)).astype(BF16)
            for c in swap2:
                c.start()

            @pl.when(has_far)
            def _():
                to_far[2].start()
                to_far[0].start()

            @pl.when(jnp.logical_not(has_far))
            def _():
                halo_s[core, :2 * BLK, :] = jnp.zeros((2 * BLK, 2 * head), BF16)

        def share():
            for c in swap2:
                c.wait_recv()
            xg_all[pl.ds(mine, quart), :] = (xh2_s[:quart, :].astype(F32) + xb_recv[0].astype(F32)).astype(BF16)
            xg_all[pl.ds(mine + quart, quart), :] = (xh2_s[quart:, :].astype(F32) + xb_recv[1].astype(F32)).astype(BF16)
            spread.start()

        def project_global():
            theirs = xg_all.at[pl.ds(half - mine, half)]
            remote(theirs, theirs, x_ssem.at[5], x_rsem.at[5], partner).wait_recv()
            xg = xg_all[...]
            for h in range(heads):
                qh = (mm(xg, wq_s[:, h * head:(h + 1) * head]) * head ** -0.5).astype(BF16)
                for j in range(n_dev):
                    at = (j * heads + h) * per
                    qg_s[at:at + per, :] = qh[j * per:(j + 1) * per]
            for j, w in enumerate((wk_s, wv_s)):
                both = mm(xg, w[...]).astype(BF16)
                for side in range(2):
                    halo_s[side, 2 * BLK:, j * head:(j + 1) * head] = both

        def near_ready():
            for c in to_near:
                c.wait_recv()

        def wait_far(i):
            @pl.when(has_far)
            def _():
                to_far[i].wait_recv()

        def inner_ready():
            wait_far(1)
            wait_far(2)

        def outer_ready():
            wait_far(0)
            for k in range(1, n_dev):
                for c in rs_copies(k):
                    c.start()

        hooks = {2: second_swap, 7: share}
        units = [Local(i // 2, i % 2, hooks.get(i)) for i in range(2 * n_blk)]
        units += [Global(0, project_global), Global(1)]
        units += [Far(near, False, 0, near_ready), Far(near, False, 1), Far(near, True, 0), Far(near, True, 1)]
        units += [Far(far, True, 0, inner_ready), Far(far, True, 1), Far(far, False, 0, outer_ready), Far(far, False, 1)]
        s_refs, t_refs, p_refs = (s0, s1), (t0, t1), (p0, p1)
        for i, u in enumerate(units):
            for k in ((0, 1) if i == 0 else (i + 1,)):
                if k < len(units):
                    if units[k].before is not None:
                        units[k].before()
                    units[k].score(s_refs[k % 2], t_refs[k % 2])
            u.soft(s_refs[i % 2], t_refs[i % 2], p_refs[i % 2])
            u.value(p_refs[i % 2])

        for c in [pair] + swap + swap2 + [spread] + to_near:
            c.wait_send()

        @pl.when(has_far)
        def _():
            for c in to_far:
                c.wait_send()

    def finish_global():
        for k in range(1, n_dev):
            for c in rs_copies(k):
                c.wait()
        rs_recv[0] = rs_send[pl.ds(me * slab, slab), :]
        st_recv[0] = st_send[me]
        top = st_recv[0, 0:1, :]
        for k in range(1, n_dev):
            top = jnp.maximum(top, st_recv[k, 0:1, :])
        tot = jnp.zeros((1, slab), F32)
        o = jnp.zeros((slab, head), F32)
        for k in range(n_dev):
            fac = jnp.exp(st_recv[k, 0:1, :] - top)
            tot = tot + st_recv[k, 1:2, :] * fac
            o = o + rs_recv[k] * row_to_column(fac)
        o = (o / row_to_column(tot)).astype(BF16)
        hg = xg_all[pl.ds(me * per, per), :].astype(F32)
        for h in range(heads):
            hg = hg + mm(o[h * per:(h + 1) * per], wo_s[h * head:(h + 1) * head, :])
        hid_s[split:split + per, :] = hg.astype(BF16)

    def yg_copy(k, peer, owner):
        return remote(hid_s.at[pl.ds(split, per)], yg_s.at[pl.ds(owner * per, per)], yg_ssem.at[k], yg_rsem.at[k], peer)

    def out_copy(p):
        lo, hi = p * part, min((p + 1) * part, split) if p < PARTS - 1 else rows
        if p == PARTS - 1:
            lo = split
        shift = per if p == PARTS - 1 else 0
        return pltpu.make_async_copy(hid_s.at[pl.ds(lo + shift, hi - lo)], ys_hbm.at[pl.ds(lo, hi - lo)], out_sem.at[p])

    def feed_forward(acc_s, u_s, w1_s, w2_s):
        def w_copies(i):
            at = pl.ds(i * TILE, TILE)
            return (pltpu.make_async_copy(w1_hbm.at[:, at], w1_s.at[i], w1_sem.at[i]),
                    pltpu.make_async_copy(w2_hbm.at[at, :], w2_s.at[i], w2_sem.at[i]))

        for i in range(n_tile):
            for c in w_copies(i):
                c.start()

        pltpu.make_async_copy(wo_hbm, wo_s, in_sem.at[4]).wait()
        for b in range(n_blk):
            r0, r1 = b * BLK, (b + 1) * BLK
            res = (x_s[r0:r1, :].astype(F32) + mm(att_s[r0:r1, :], wo_s[...])).astype(BF16)
            cut = min(max(split - r0, 0), BLK)
            if cut:
                hid_s[r0:r0 + cut, :] = res[:cut]
            if cut < BLK:
                hid_s[r0 + cut + per:r1 + per, :] = res[cut:]

        def chunks(r, i, count):
            u = u_s[...]
            for c in range(count):
                g, at = i + c // (TILE // BLK), c % (TILE // BLK) * BLK
                s = mm(hid_s[r, :], w1_s[g, :, at:at + BLK])
                if c == 0:
                    acc_s[...] += mm(u, w2_s[jnp.maximum(i - 1, 0), TILE - BLK:, :])
                else:
                    b = c - 1
                    at = b % (TILE // BLK) * BLK
                    acc_s[...] += mm(u, w2_s[i + b // (TILE // BLK), at:at + BLK, :])
                u = gelu(s).astype(BF16)
            u_s[...] = u

        def run_part(r, steps, step):
            acc_s[...] = hid_s[r, :].astype(F32)
            u_s[...] = jnp.zeros_like(u_s)
            lax.fori_loop(0, steps, step, 0)
            hid_s[r, :] = (acc_s[...] + mm(u_s[...], w2_s[n_tile - 1, TILE - BLK:, :])).astype(BF16)

        def later(p, carry):
            r = pl.ds(pl.multiple_of(p * part, 16), part)

            def step(i, carry):
                @pl.when(p == 0)
                def _():
                    for k in range(WIDE):
                        for c in w_copies(i * WIDE + k):
                            c.wait()

                chunks(r, i * WIDE, WIDE * (TILE // BLK))
                return carry

            run_part(r, n_tile // WIDE, step)

            @pl.when(p == 0)
            def _():
                finish_global()

            @pl.when(p == PARTS - 2)
            def _():
                for k in range(1, n_dev):
                    yg_copy(k, lax.rem(me + k, n_dev), me).start()
                yg_s[pl.ds(me * per, per), :] = hid_s[split:split + per, :]

            for q in range(PARTS):
                @pl.when(p == q)
                def _():
                    out_copy(q).start()

            return carry

        lax.fori_loop(0, PARTS, later, 0)

    pl.run_scoped(
        front,
        pltpu.VMEM(wq_hbm.shape, BF16), pltpu.VMEM((dim, heads * head), BF16), pltpu.VMEM((dim, head), BF16), pltpu.VMEM((dim, head), BF16),
        pltpu.VMEM((rows, 2 * head), BF16),
        pltpu.VMEM((n_glob, dim), BF16), pltpu.VMEM((half, dim), BF16), pltpu.VMEM((half, dim), BF16),
        pltpu.VMEM((n_blk, stack, head), BF16), pltpu.VMEM((stack, ext), F32),
        pltpu.VMEM((unit, rows), F32), pltpu.VMEM((unit, rows), F32), pltpu.VMEM((unit, 128), F32), pltpu.VMEM((unit, 128), F32),
        pltpu.VMEM((unit, rows), BF16), pltpu.VMEM((unit, rows), BF16),
        pltpu.VMEM((n_blk, stack, head), F32), pltpu.VMEM((n_blk, stack, 128), F32), pltpu.VMEM((n_blk, stack, 128), F32),
        pltpu.VMEM((unit, 128), F32), pltpu.VMEM((unit, 128), F32), pltpu.VMEM((n_dev * slab, head), BF16))
    pl.run_scoped(feed_forward, pltpu.VMEM((part, dim), F32), pltpu.VMEM((part, BLK), BF16),
                  pltpu.VMEM((n_tile, dim, TILE), BF16), pltpu.VMEM((n_tile, TILE, dim), BF16))
    for k in range(1, n_dev):
        src = lax.rem(me + n_dev - k, n_dev)
        yg_copy(k, src, src).wait_recv()
    last = pltpu.make_async_copy(yg_s, yg_hbm, out_sem.at[PARTS])
    last.start()
    for k in range(1, n_dev):
        yg_copy(k, lax.rem(me + k, n_dev), me).wait_send()
    for p in range(PARTS):
        out_copy(p).wait()
    last.wait()


def gelu(x):
    scale = math.sqrt(2.0 / math.pi)
    part = 0.5 * x
    return part + part * jnp.tanh(x * (scale + (scale * 0.044715) * (x * x)))


def layer(x, wq, wk, wv, wo, w1, w2, rel_bias, gp, n_dev):
    rows, dim = x.shape
    heads, head = wq.shape[1:]
    width = (rel_bias.shape[1] - 1) // 2
    n_glob = gp.shape[1]
    per = n_glob // n_dev
    slab = heads * per
    any_spec = pl.BlockSpec(memory_space=pl.ANY)
    vmem_spec = pl.BlockSpec(memory_space=pltpu.VMEM)
    dma = pltpu.SemaphoreType.DMA
    return pl.pallas_call(
        functools.partial(layer_kernel, n_dev, heads, width),
        name='layer',
        out_shape=(jax.ShapeDtypeStruct((rows, dim), BF16), jax.ShapeDtypeStruct((n_glob, dim), BF16)),
        in_specs=[any_spec] * 7 + [vmem_spec] * 2,
        out_specs=(any_spec, any_spec),
        scratch_shapes=[
            pltpu.VMEM(x.shape, BF16), pltpu.VMEM(wo.shape, BF16), pltpu.VMEM((2, 3 * BLK, 2 * head), BF16),
            pltpu.VMEM((8, BLK + 2 * width), F32), pltpu.VMEM((8, rows + 2 * width), F32),
            pltpu.VMEM((n_glob // 2, dim), BF16), pltpu.VMEM((2, n_glob // 4, dim), BF16), pltpu.VMEM((2, n_glob // 4, dim), BF16),
            pltpu.VMEM((n_glob, dim), BF16),
            pltpu.VMEM((n_dev * slab, head), F32), pltpu.VMEM((n_dev, slab, head), F32),
            pltpu.VMEM((n_dev, 8, slab), F32), pltpu.VMEM((n_dev, 8, slab), F32),
            pltpu.VMEM((rows + per, dim), BF16), pltpu.VMEM((n_glob, dim), BF16), pltpu.VMEM((rows, heads * head), BF16),
            dma((5,)), dma((6,)), dma((6,)), dma((5,)), dma((5,)), dma((n_dev,)), dma((n_dev,)), dma((n_dev,)), dma((n_dev,)),
            dma((n_dev,)), dma((n_dev,)), dma((w1.shape[1] // TILE,)), dma((w1.shape[1] // TILE,)), dma((PARTS + 1,)),
        ],
        compiler_params=pltpu.CompilerParams(collective_id=0, has_side_effects=True, vmem_limit_bytes=67043328),
    )(x, wq, wk, wv, wo, w1, w2, rel_bias, gp)


def place_kernel(ys_hbm, yg_hbm, gp_ref, y_hbm, yo_hbm, ys_s, y_s, yg_s, in_sem, out_sem):
    n = ys_s.shape[0]
    n_glob = gp_ref.shape[1]
    gets = [pltpu.make_async_copy(ys_hbm.at[pl.ds(i * PIECE, PIECE)], ys_s.at[i], in_sem.at[i]) for i in range(n)]
    puts = [pltpu.make_async_copy(y_s.at[i], y_hbm.at[pl.ds(i * PIECE, PIECE)], out_sem.at[i]) for i in range(n)]
    get_g = pltpu.make_async_copy(yg_hbm, yg_s, in_sem.at[n])
    put_g = pltpu.make_async_copy(yg_s, yo_hbm, out_sem.at[n])
    get_g.start()
    for c in gets:
        c.start()
    get_g.wait()
    put_g.start()
    for i in range(n):
        first = (lax.axis_index('sp') * n + i) * PIECE
        hit = gp_ref[...] == first + lax.broadcasted_iota(jnp.int32, (PIECE, n_glob), 0)
        sel = hit.astype(F32)
        placed = mm(sel.astype(BF16), yg_s[...]).astype(BF16)
        is_glob = jnp.max(sel, axis=1, keepdims=True) > 0.0
        gets[i].wait()
        y_s[i] = jnp.where(is_glob, placed, ys_s[i])
        puts[i].start()
    for c in puts:
        c.wait()
    put_g.wait()


def place(ys, yg, gp):
    rows, dim = ys.shape
    n = rows // PIECE
    any_spec = pl.BlockSpec(memory_space=pl.ANY)
    dma = pltpu.SemaphoreType.DMA
    return pl.pallas_call(
        place_kernel,
        name='place',
        out_shape=(jax.ShapeDtypeStruct(ys.shape, BF16), jax.ShapeDtypeStruct(yg.shape, BF16)),
        in_specs=[any_spec, any_spec, pl.BlockSpec(memory_space=pltpu.VMEM)],
        out_specs=(any_spec, any_spec),
        scratch_shapes=[pltpu.VMEM((n, PIECE, dim), BF16), pltpu.VMEM((n, PIECE, dim), BF16), pltpu.VMEM(yg.shape, BF16),
                        dma((n + 1,)), dma((n + 1,))],
        compiler_params=pltpu.CompilerParams(vmem_limit_bytes=60 << 20),
    )(ys, yg, gp)


def solution(mesh):
    n_dev = mesh.shape['sp']

    def shard_layer(hidden_in, w_query, w_key, w_value, w_out, w_up, w_down, rel_bias, glob_pos):
        dim = hidden_in.shape[1]
        heads, head = w_query.shape[1], w_query.shape[2]
        gp = glob_pos.reshape(1, -1)
        ys, yg = layer(hidden_in, w_query, w_key.reshape(dim, head), w_value.reshape(dim, head),
                       w_out.reshape(heads * head, dim), w_up, w_down, rel_bias, gp, n_dev)
        return place(ys, yg, gp)

    return jax.shard_map(
        shard_layer, mesh=mesh,
        in_specs=(P(('dp', 'sp'), None), P(), P(), P(), P(), P(), P(), P(), P('dp')),
        out_specs=(P(('dp', 'sp'), None), P('dp', None)),
        check_vma=False)
```

```python
import functools
import math

import jax
import jax.numpy as jnp
from jax import lax
from jax.experimental import pallas as pl
from jax.experimental.pallas import tpu as pltpu
from jax.sharding import PartitionSpec as P

BF16 = jnp.bfloat16
F32 = jnp.float32
NEG = -math.inf
BLK = 256
ROW = 32
PIECE = 256
PARTS = 3
TILE = 768
WIDE = 3


def mm(a, b):
    return jnp.dot(a, b, preferred_element_type=F32)


def mm_nt(a, b):
    return lax.dot_general(a, b, (((1,), (1,)), ((), ())), preferred_element_type=F32)


def remote(src, dst, send, recv, dev):
    return pltpu.make_async_remote_copy(
        src_ref=src, dst_ref=dst, send_sem=send, recv_sem=recv,
        device_id={'sp': dev}, device_id_type=pl.DeviceIdType.MESH)


def announce(me, n_dev):
    barrier = pltpu.get_barrier_semaphore()
    for k in range(1, n_dev):
        pl.semaphore_signal(barrier, inc=1, device_id={'sp': lax.rem(me + k, n_dev)}, device_id_type=pl.DeviceIdType.MESH)
    return barrier


def diagonal(n):
    return lax.broadcasted_iota(jnp.int32, (n, n), 0) == lax.broadcasted_iota(jnp.int32, (n, n), 1)


def row_to_column(row):
    n = row.shape[1]
    return jnp.sum(jnp.where(diagonal(n), jnp.broadcast_to(row, (n, n)), 0.0), axis=1, keepdims=True)


def column_to_row(col):
    n = col.shape[0]
    return jnp.sum(jnp.where(diagonal(n), jnp.broadcast_to(col, (n, n)), 0.0), axis=0, keepdims=True)


def lane_max(s):
    best = s[:, :128]
    for c in range(128, s.shape[1], 128):
        best = jnp.maximum(best, s[:, c:c + 128])
    return best


def layer_kernel(n_dev, heads, width,
                 x_hbm, wq_hbm, wk_hbm, wv_hbm, wo_hbm, w1_hbm, w2_hbm, rb_ref, gp_ref, ys_hbm, yg_hbm,
                 x_s, wo_s, halo_s, row_s, mask_s, xp_recv, xa_recv, xb_recv, xg_all, rs_send, rs_recv, st_send, st_recv,
                 hid_s, yg_s, att_s,
                 in_sem, x_ssem, x_rsem, halo_ssem, halo_rsem, rs_ssem, rs_rsem, st_ssem, st_rsem, yg_ssem, yg_rsem,
                 w1_sem, w2_sem, out_sem):
    rows, dim = x_s.shape
    head = wk_hbm.shape[1]
    n_glob = gp_ref.shape[1]
    per = n_glob // n_dev
    slab = heads * per
    n_blk = rows // BLK
    stack = heads * BLK
    unit = stack // 2
    ext = BLK + 2 * width
    part = (rows + per) // PARTS
    split = part * (PARTS - 1) - per
    n_tile = w1_hbm.shape[1] // TILE
    me = lax.axis_index('sp')
    start = me * rows
    core = lax.rem(me, 2)
    chip = me // 2
    partner = me + 1 - 2 * core
    x_peer = 2 * (chip + 1 - 2 * lax.rem(chip, 2)) + core
    y_peer = 2 * lax.rem(chip + 2, 4) + core
    half = n_glob // 2
    quart = n_glob // 4

    def rs_copies(k):
        peer = lax.rem(me + k, n_dev)
        return (remote(rs_send.at[pl.ds(peer * slab, slab)], rs_recv.at[k], rs_ssem.at[k], rs_rsem.at[k], peer),
                remote(st_send.at[peer], st_recv.at[k], st_ssem.at[k], st_rsem.at[k], peer))

    def front(wq3_s, wq_s, wk_s, wv_s, kv_s, xg_send, xh_s, xh2_s, q_s, bias_s, s0, s1, t0, t1, p0, p1, o_s, m_s, l_s, mg_s, lg_s, qg_s):
        loads = [pltpu.make_async_copy(src, dst, in_sem.at[i]) for i, (src, dst) in enumerate(
            [(x_hbm, x_s), (wk_hbm, wk_s), (wv_hbm, wv_s), (wq_hbm, wq3_s), (wo_hbm, wo_s)])]
        for c in loads[:3]:
            c.start()
        barrier = announce(me, n_dev)

        gp_col = row_to_column(gp_ref[...].astype(F32)).astype(jnp.int32)
        own = gp_col == start + lax.broadcasted_iota(jnp.int32, (n_glob, rows), 1)
        pos = start - width + lax.broadcasted_iota(jnp.int32, (1, rows + 2 * width), 1)
        hit = jnp.max((gp_col == pos).astype(F32), axis=0, keepdims=True) > 0.0
        bad = hit | (pos < 0) | (pos >= rows * n_dev)
        mask_s[...] = jnp.broadcast_to(jnp.where(bad, NEG, 0.0), mask_s.shape)

        row_s[...] = jnp.full(row_s.shape, NEG, F32)
        row_s[:heads, :2 * width] = rb_ref[:, :2 * width]
        last = jnp.broadcast_to(rb_ref[:, 2 * width:], (heads, 128))
        row_s[:heads, 2 * width:2 * width + 128] = jnp.where(lax.broadcasted_iota(jnp.int32, (heads, 128), 1) == 0, last, NEG)
        for h in range(heads):
            wide = jnp.broadcast_to(row_s[h:h + 1, :], (BLK, ext))
            bias_s[h * BLK:(h + 1) * BLK, :] = pltpu.roll(wide, 0, 1, stride=1, stride_axis=0)

        loads[0].wait()
        loads[3].start()
        x = x_s[...]

        xg_send[...] = mm(own.astype(F32).astype(BF16), x).astype(BF16)
        pair = remote(xg_send.at[pl.ds((1 - core) * half, half)], xp_recv, x_ssem.at[0], x_rsem.at[0], partner)
        pl.semaphore_wait(barrier, n_dev - 1)
        pair.start()

        loads[1].wait()
        loads[2].wait()
        kv_s[:, :head] = mm(x, wk_s[...]).astype(BF16)
        kv_s[:, head:] = mm(x, wv_s[...]).astype(BF16)

        near, far = 1 - core, core
        has_far = (me > 0) & (me < n_dev - 1)
        far_peer = lax.rem(me + n_dev - 1 + 2 * core, n_dev)

        def halo_copies(mine, theirs, peer, sem, pieces):
            out = []
            for k, (at, size) in enumerate(pieces):
                blk = at // BLK + theirs - 2 * (at // BLK) * theirs
                out.append(remote(kv_s.at[pl.ds(mine * width + blk * BLK + at % BLK, size)], halo_s.at[theirs, pl.ds(at, size)],
                                  halo_ssem.at[sem + k], halo_rsem.at[sem + k], peer))
            return out

        loads[4].start()
        to_near = halo_copies(near, core, partner, 0, ((0, BLK), (BLK, BLK)))
        to_far = halo_copies(far, 1 - core, far_peer, 2, ((0, BLK), (BLK, BLK // 2), (BLK + BLK // 2, BLK // 2)))
        for c in to_near:
            c.start()

        pair.wait_recv()
        xh_s[...] = (xg_send[pl.ds(core * half, half), :].astype(F32) + xp_recv[...].astype(F32)).astype(BF16)
        swap = [remote(xh_s.at[pl.ds(0, quart)], xa_recv.at[0], x_ssem.at[1], x_rsem.at[1], x_peer),
                remote(xh_s.at[pl.ds(quart, quart)], xa_recv.at[1], x_ssem.at[2], x_rsem.at[2], y_peer)]
        for c in swap:
            c.start()

        @pl.when(has_far)
        def _():
            to_far[1].start()

        loads[3].wait()
        wq_s[...] = wq3_s[...].reshape(wq_s.shape)
        for h in range(heads):
            qh = (mm(x, wq_s[:, h * head:(h + 1) * head]) * head ** -0.5).astype(BF16)
            for b in range(n_blk):
                q_s[b, h * BLK:(h + 1) * BLK, :] = qh[b * BLK:(b + 1) * BLK]

        class Local:
            def __init__(self, b, g, before=None):
                self.b, self.r0, self.before = b, g * unit, before
                self.lo, self.hi = max(0, b * BLK - width), min(rows, (b + 1) * BLK + width)

            def score(self, s_ref, t_ref):
                n, c0 = self.hi - self.lo, self.lo - self.b * BLK + width
                s = mm_nt(q_s[self.b, self.r0:self.r0 + unit], kv_s[self.lo:self.hi, :head])
                s = s + bias_s[self.r0:self.r0 + unit, c0:c0 + n] + mask_s[0:1, width + self.lo:width + self.hi]
                s_ref[:, :n] = s
                t_ref[...] = lane_max(s)

            def soft(self, s_ref, t_ref, p_ref):
                n = self.hi - self.lo
                for r in range(0, unit, ROW):
                    rs, ra = slice(r, r + ROW), slice(self.r0 + r, self.r0 + r + ROW)
                    top = jnp.max(t_ref[rs, :], axis=1, keepdims=True)
                    p = jnp.exp(s_ref[rs, :n] - top)
                    p_ref[rs, :n] = p.astype(BF16)
                    m_s[self.b, ra, :] = jnp.broadcast_to(top, (ROW, 128))
                    l_s[self.b, ra, :] = jnp.broadcast_to(jnp.sum(p, axis=1, keepdims=True), (ROW, 128))

            def value(self, p_ref):
                o_s[self.b, self.r0:self.r0 + unit] = mm(p_ref[:, :self.hi - self.lo], kv_s[self.lo:self.hi, head:])

        class Global:
            def __init__(self, g, before=None):
                self.r0, self.before = g * unit, before

            def score(self, s_ref, t_ref):
                s = mm_nt(qg_s[self.r0:self.r0 + unit, :], kv_s[:, :head])
                s_ref[...] = s
                t_ref[...] = lane_max(s)

            def soft(self, s_ref, t_ref, p_ref):
                for r in range(0, unit, ROW):
                    rs = slice(r, r + ROW)
                    top = jnp.max(t_ref[rs, :], axis=1, keepdims=True)
                    p = jnp.exp(s_ref[rs, :] - top)
                    p_ref[rs, :] = p.astype(BF16)
                    mg_s[rs, :] = jnp.broadcast_to(top, (ROW, 128))
                    lg_s[rs, :] = jnp.broadcast_to(jnp.sum(p, axis=1, keepdims=True), (ROW, 128))
                for j in range(unit // slab):
                    cut, to = slice(j * slab, (j + 1) * slab), self.r0 // slab + j
                    st_send[to, 0:1, :] = jnp.sum(jnp.where(diagonal(slab), mg_s[cut, :], 0.0), axis=0, keepdims=True)
                    st_send[to, 1:2, :] = jnp.sum(jnp.where(diagonal(slab), lg_s[cut, :], 0.0), axis=0, keepdims=True)

            def value(self, p_ref):
                rs_send[self.r0:self.r0 + unit, :] = mm(p_ref[...], kv_s[:, head:])

        class Far:
            def __init__(self, side, inner, g, before=None):
                self.side, self.inner, self.r0, self.before = side, inner, g * unit, before
                self.b = 1 + side * (n_blk - 3) if inner else side * (n_blk - 1)
                self.k0, self.n = (BLK, 2 * BLK) if inner else (0, 3 * BLK)

            def score(self, s_ref, t_ref):
                side, n = self.side, self.n
                near_mask = BLK + side * (rows + BLK)
                if self.inner:
                    cuts = [(side * (ext - BLK), near_mask)]
                else:
                    cuts = [(side * (ext - BLK), side * (rows + width + BLK)), (BLK + side * (ext - 3 * BLK), near_mask)]
                s = mm_nt(q_s[self.b, self.r0:self.r0 + unit], halo_s[side, self.k0:, :head])
                best = lane_max(s[:, n - BLK:])
                s_ref[:, n - BLK:n] = s[:, n - BLK:]
                for i, (c0, m0) in enumerate(cuts):
                    cut = (s[:, i * BLK:(i + 1) * BLK] + bias_s[self.r0:self.r0 + unit, pl.ds(pl.multiple_of(c0, BLK), BLK)]
                           + mask_s[0:1, pl.ds(pl.multiple_of(m0, BLK), BLK)])
                    s_ref[:, i * BLK:(i + 1) * BLK] = cut
                    best = jnp.maximum(best, lane_max(cut))
                t_ref[...] = best

            def soft(self, s_ref, t_ref, p_ref):
                n = self.n
                for r in range(0, unit, ROW):
                    rs, ra = slice(r, r + ROW), slice(self.r0 + r, self.r0 + r + ROW)
                    m1 = m_s[self.b, ra, :]
                    top = jnp.maximum(m1, jnp.broadcast_to(jnp.max(t_ref[rs, :], axis=1, keepdims=True), (ROW, 128)))
                    s = s_ref[rs, :n]
                    p = jnp.exp(s - jnp.concatenate([top] * (n // 128), axis=1))
                    p_ref[rs, :n] = p.astype(BF16)
                    fac = jnp.exp(m1 - top)
                    inv = 1.0 / (l_s[self.b, ra, :] * fac + jnp.broadcast_to(jnp.sum(p, axis=1, keepdims=True), (ROW, 128)))
                    m_s[self.b, ra, :] = fac * inv
                    l_s[self.b, ra, :] = inv

            def value(self, p_ref):
                at = pl.ds(pl.multiple_of(self.b * BLK, BLK), BLK)
                new = mm(p_ref[:, :self.n], halo_s[self.side, self.k0:, head:])
                for h in range(unit // BLK):
                    ra = slice(self.r0 + h * BLK, self.r0 + (h + 1) * BLK)
                    fac, inv = m_s[self.b, ra, :], l_s[self.b, ra, :]
                    o = (o_s[self.b, ra, :] * jnp.concatenate([fac] * (head // 128), axis=1)
                         + new[h * BLK:(h + 1) * BLK] * jnp.concatenate([inv] * (head // 128), axis=1))
                    col = (self.r0 // BLK + h) * head
                    att_s[at, col:col + head] = o.astype(BF16)

        swap2 = [remote(xh2_s.at[pl.ds(0, quart)], xb_recv.at[0], x_ssem.at[3], x_rsem.at[3], y_peer),
                 remote(xh2_s.at[pl.ds(quart, quart)], xb_recv.at[1], x_ssem.at[4], x_rsem.at[4], x_peer)]
        mine = core * half
        spread = remote(xg_all.at[pl.ds(mine, half)], xg_all.at[pl.ds(mine, half)], x_ssem.at[5], x_rsem.at[5], partner)

        def second_swap():
            for c in swap:
                c.wait_recv()
            xh2_s[:quart, :] = (xh_s[:quart, :].astype(F32) + xa_recv[0].astype(F32)).astype(BF16)
            xh2_s[quart:, :] = (xh_s[quart:, :].astype(F32) + xa_recv[1].astype(F32)).astype(BF16)
            for c in swap2:
                c.start()

            @pl.when(has_far)
            def _():
                to_far[2].start()
                to_far[0].start()

            @pl.when(jnp.logical_not(has_far))
            def _():
                halo_s[core, :2 * BLK, :] = jnp.zeros((2 * BLK, 2 * head), BF16)

        def share():
            for c in swap2:
                c.wait_recv()
            xg_all[pl.ds(mine, quart), :] = (xh2_s[:quart, :].astype(F32) + xb_recv[0].astype(F32)).astype(BF16)
            xg_all[pl.ds(mine + quart, quart), :] = (xh2_s[quart:, :].astype(F32) + xb_recv[1].astype(F32)).astype(BF16)
            spread.start()

        def project_global():
            theirs = xg_all.at[pl.ds(half - mine, half)]
            remote(theirs, theirs, x_ssem.at[5], x_rsem.at[5], partner).wait_recv()
            xg = xg_all[...]
            for h in range(heads):
                qh = (mm(xg, wq_s[:, h * head:(h + 1) * head]) * head ** -0.5).astype(BF16)
                for j in range(n_dev):
                    at = (j * heads + h) * per
                    qg_s[at:at + per, :] = qh[j * per:(j + 1) * per]
            for j, w in enumerate((wk_s, wv_s)):
                both = mm(xg, w[...]).astype(BF16)
                for side in range(2):
                    halo_s[side, 2 * BLK:, j * head:(j + 1) * head] = both

        def near_ready():
            for c in to_near:
                c.wait_recv()

        def wait_far(i):
            @pl.when(has_far)
            def _():
                to_far[i].wait_recv()

        def inner_ready():
            wait_far(1)
            wait_far(2)

        def outer_ready():
            wait_far(0)
            for k in range(1, n_dev):
                for c in rs_copies(k):
                    c.start()

        hooks = {2: second_swap, 7: share}
        units = [Local(i // 2, i % 2, hooks.get(i)) for i in range(2 * n_blk)]
        units += [Global(0, project_global), Global(1)]
        units += [Far(near, False, 0, near_ready), Far(near, False, 1), Far(near, True, 0), Far(near, True, 1)]
        units += [Far(far, True, 0, inner_ready), Far(far, True, 1), Far(far, False, 0, outer_ready), Far(far, False, 1)]
        s_refs, t_refs, p_refs = (s0, s1), (t0, t1), (p0, p1)
        for i, u in enumerate(units):
            for k in ((0, 1) if i == 0 else (i + 1,)):
                if k < len(units):
                    if units[k].before is not None:
                        units[k].before()
                    units[k].score(s_refs[k % 2], t_refs[k % 2])
            u.soft(s_refs[i % 2], t_refs[i % 2], p_refs[i % 2])
            u.value(p_refs[i % 2])

        for c in [pair] + swap + swap2 + [spread] + to_near:
            c.wait_send()

        @pl.when(has_far)
        def _():
            for c in to_far:
                c.wait_send()

    def finish_global():
        for k in range(1, n_dev):
            for c in rs_copies(k):
                c.wait()
        rs_recv[0] = rs_send[pl.ds(me * slab, slab), :]
        st_recv[0] = st_send[me]
        top = st_recv[0, 0:1, :]
        for k in range(1, n_dev):
            top = jnp.maximum(top, st_recv[k, 0:1, :])
        tot = jnp.zeros((1, slab), F32)
        o = jnp.zeros((slab, head), F32)
        for k in range(n_dev):
            fac = jnp.exp(st_recv[k, 0:1, :] - top)
            tot = tot + st_recv[k, 1:2, :] * fac
            o = o + rs_recv[k] * row_to_column(fac)
        o = (o / row_to_column(tot)).astype(BF16)
        hg = xg_all[pl.ds(me * per, per), :].astype(F32)
        for h in range(heads):
            hg = hg + mm(o[h * per:(h + 1) * per], wo_s[h * head:(h + 1) * head, :])
        hid_s[split:split + per, :] = hg.astype(BF16)

    def yg_copy(k, peer, owner):
        return remote(hid_s.at[pl.ds(split, per)], yg_s.at[pl.ds(owner * per, per)], yg_ssem.at[k], yg_rsem.at[k], peer)

    def out_copy(p):
        lo, hi = p * part, min((p + 1) * part, split) if p < PARTS - 1 else rows
        if p == PARTS - 1:
            lo = split
        shift = per if p == PARTS - 1 else 0
        return pltpu.make_async_copy(hid_s.at[pl.ds(lo + shift, hi - lo)], ys_hbm.at[pl.ds(lo, hi - lo)], out_sem.at[p])

    def feed_forward(acc_s, u_s, w1_s, w2_s):
        def w_copies(i):
            at = pl.ds(i * TILE, TILE)
            return (pltpu.make_async_copy(w1_hbm.at[:, at], w1_s.at[i], w1_sem.at[i]),
                    pltpu.make_async_copy(w2_hbm.at[at, :], w2_s.at[i], w2_sem.at[i]))

        for i in range(n_tile):
            for c in w_copies(i):
                c.start()

        pltpu.make_async_copy(wo_hbm, wo_s, in_sem.at[4]).wait()
        for b in range(n_blk):
            r0, r1 = b * BLK, (b + 1) * BLK
            res = (x_s[r0:r1, :].astype(F32) + mm(att_s[r0:r1, :], wo_s[...])).astype(BF16)
            cut = min(max(split - r0, 0), BLK)
            if cut:
                hid_s[r0:r0 + cut, :] = res[:cut]
            if cut < BLK:
                hid_s[r0 + cut + per:r1 + per, :] = res[cut:]

        def chunks(r, i, count):
            u = u_s[...]
            for c in range(count):
                g, at = i + c // (TILE // BLK), c % (TILE // BLK) * BLK
                s = mm(hid_s[r, :], w1_s[g, :, at:at + BLK])
                if c == 0:
                    acc_s[...] += mm(u, w2_s[jnp.maximum(i - 1, 0), TILE - BLK:, :])
                else:
                    b = c - 1
                    at = b % (TILE // BLK) * BLK
                    acc_s[...] += mm(u, w2_s[i + b // (TILE // BLK), at:at + BLK, :])
                u = gelu(s).astype(BF16)
            u_s[...] = u

        def run_part(r, steps, step):
            acc_s[...] = hid_s[r, :].astype(F32)
            u_s[...] = jnp.zeros_like(u_s)
            lax.fori_loop(0, steps, step, 0)
            hid_s[r, :] = (acc_s[...] + mm(u_s[...], w2_s[n_tile - 1, TILE - BLK:, :])).astype(BF16)

        def later(p, carry):
            r = pl.ds(pl.multiple_of(p * part, 16), part)

            def narrow(k, carry):
                for c in w_copies(k):
                    c.wait()
                chunks(r, k, TILE // BLK)
                return carry

            def step(i, carry):
                fresh = (p == 0) & (i == 0)

                @pl.when(fresh)
                def _():
                    lax.fori_loop(0, WIDE, narrow, 0)

                @pl.when((p == 0) & (i > 0))
                def _():
                    for k in range(WIDE):
                        for c in w_copies(i * WIDE + k):
                            c.wait()

                @pl.when(jnp.logical_not(fresh))
                def _():
                    chunks(r, i * WIDE, WIDE * (TILE // BLK))

                return carry

            run_part(r, n_tile // WIDE, step)

            @pl.when(p == 0)
            def _():
                finish_global()

            @pl.when(p == PARTS - 2)
            def _():
                for k in range(1, n_dev):
                    yg_copy(k, lax.rem(me + k, n_dev), me).start()
                yg_s[pl.ds(me * per, per), :] = hid_s[split:split + per, :]

            for q in range(PARTS):
                @pl.when(p == q)
                def _():
                    out_copy(q).start()

            return carry

        lax.fori_loop(0, PARTS, later, 0)

    pl.run_scoped(
        front,
        pltpu.VMEM(wq_hbm.shape, BF16), pltpu.VMEM((dim, heads * head), BF16), pltpu.VMEM((dim, head), BF16), pltpu.VMEM((dim, head), BF16),
        pltpu.VMEM((rows, 2 * head), BF16),
        pltpu.VMEM((n_glob, dim), BF16), pltpu.VMEM((half, dim), BF16), pltpu.VMEM((half, dim), BF16),
        pltpu.VMEM((n_blk, stack, head), BF16), pltpu.VMEM((stack, ext), F32),
        pltpu.VMEM((unit, rows), F32), pltpu.VMEM((unit, rows), F32), pltpu.VMEM((unit, 128), F32), pltpu.VMEM((unit, 128), F32),
        pltpu.VMEM((unit, rows), BF16), pltpu.VMEM((unit, rows), BF16),
        pltpu.VMEM((n_blk, stack, head), F32), pltpu.VMEM((n_blk, stack, 128), F32), pltpu.VMEM((n_blk, stack, 128), F32),
        pltpu.VMEM((unit, 128), F32), pltpu.VMEM((unit, 128), F32), pltpu.VMEM((n_dev * slab, head), BF16))
    pl.run_scoped(feed_forward, pltpu.VMEM((part, dim), F32), pltpu.VMEM((part, BLK), BF16),
                  pltpu.VMEM((n_tile, dim, TILE), BF16), pltpu.VMEM((n_tile, TILE, dim), BF16))
    for k in range(1, n_dev):
        src = lax.rem(me + n_dev - k, n_dev)
        yg_copy(k, src, src).wait_recv()
    last = pltpu.make_async_copy(yg_s, yg_hbm, out_sem.at[PARTS])
    last.start()
    for k in range(1, n_dev):
        yg_copy(k, lax.rem(me + k, n_dev), me).wait_send()
    for p in range(PARTS):
        out_copy(p).wait()
    last.wait()


def gelu(x):
    scale = math.sqrt(2.0 / math.pi)
    part = 0.5 * x
    return part + part * jnp.tanh(x * (scale + (scale * 0.044715) * (x * x)))


def layer(x, wq, wk, wv, wo, w1, w2, rel_bias, gp, n_dev):
    rows, dim = x.shape
    heads, head = wq.shape[1:]
    width = (rel_bias.shape[1] - 1) // 2
    n_glob = gp.shape[1]
    per = n_glob // n_dev
    slab = heads * per
    any_spec = pl.BlockSpec(memory_space=pl.ANY)
    vmem_spec = pl.BlockSpec(memory_space=pltpu.VMEM)
    dma = pltpu.SemaphoreType.DMA
    return pl.pallas_call(
        functools.partial(layer_kernel, n_dev, heads, width),
        name='layer',
        out_shape=(jax.ShapeDtypeStruct((rows, dim), BF16), jax.ShapeDtypeStruct((n_glob, dim), BF16)),
        in_specs=[any_spec] * 7 + [vmem_spec] * 2,
        out_specs=(any_spec, any_spec),
        scratch_shapes=[
            pltpu.VMEM(x.shape, BF16), pltpu.VMEM(wo.shape, BF16), pltpu.VMEM((2, 3 * BLK, 2 * head), BF16),
            pltpu.VMEM((8, BLK + 2 * width), F32), pltpu.VMEM((8, rows + 2 * width), F32),
            pltpu.VMEM((n_glob // 2, dim), BF16), pltpu.VMEM((2, n_glob // 4, dim), BF16), pltpu.VMEM((2, n_glob // 4, dim), BF16),
            pltpu.VMEM((n_glob, dim), BF16),
            pltpu.VMEM((n_dev * slab, head), F32), pltpu.VMEM((n_dev, slab, head), F32),
            pltpu.VMEM((n_dev, 8, slab), F32), pltpu.VMEM((n_dev, 8, slab), F32),
            pltpu.VMEM((rows + per, dim), BF16), pltpu.VMEM((n_glob, dim), BF16), pltpu.VMEM((rows, heads * head), BF16),
            dma((5,)), dma((6,)), dma((6,)), dma((5,)), dma((5,)), dma((n_dev,)), dma((n_dev,)), dma((n_dev,)), dma((n_dev,)),
            dma((n_dev,)), dma((n_dev,)), dma((w1.shape[1] // TILE,)), dma((w1.shape[1] // TILE,)), dma((PARTS + 1,)),
        ],
        compiler_params=pltpu.CompilerParams(collective_id=0, has_side_effects=True, vmem_limit_bytes=67043328),
    )(x, wq, wk, wv, wo, w1, w2, rel_bias, gp)


def place_kernel(ys_hbm, yg_hbm, gp_ref, y_hbm, yo_hbm, ys_s, y_s, yg_s, in_sem, out_sem):
    n = ys_s.shape[0]
    n_glob = gp_ref.shape[1]
    gets = [pltpu.make_async_copy(ys_hbm.at[pl.ds(i * PIECE, PIECE)], ys_s.at[i], in_sem.at[i]) for i in range(n)]
    puts = [pltpu.make_async_copy(y_s.at[i], y_hbm.at[pl.ds(i * PIECE, PIECE)], out_sem.at[i]) for i in range(n)]
    get_g = pltpu.make_async_copy(yg_hbm, yg_s, in_sem.at[n])
    put_g = pltpu.make_async_copy(yg_s, yo_hbm, out_sem.at[n])
    get_g.start()
    for c in gets:
        c.start()
    get_g.wait()
    put_g.start()
    for i in range(n):
        first = (lax.axis_index('sp') * n + i) * PIECE
        hit = gp_ref[...] == first + lax.broadcasted_iota(jnp.int32, (PIECE, n_glob), 0)
        sel = hit.astype(F32)
        placed = mm(sel.astype(BF16), yg_s[...]).astype(BF16)
        is_glob = jnp.max(sel, axis=1, keepdims=True) > 0.0
        gets[i].wait()
        y_s[i] = jnp.where(is_glob, placed, ys_s[i])
        puts[i].start()
    for c in puts:
        c.wait()
    put_g.wait()


def place(ys, yg, gp):
    rows, dim = ys.shape
    n = rows // PIECE
    any_spec = pl.BlockSpec(memory_space=pl.ANY)
    dma = pltpu.SemaphoreType.DMA
    return pl.pallas_call(
        place_kernel,
        name='place',
        out_shape=(jax.ShapeDtypeStruct(ys.shape, BF16), jax.ShapeDtypeStruct(yg.shape, BF16)),
        in_specs=[any_spec, any_spec, pl.BlockSpec(memory_space=pltpu.VMEM)],
        out_specs=(any_spec, any_spec),
        scratch_shapes=[pltpu.VMEM((n, PIECE, dim), BF16), pltpu.VMEM((n, PIECE, dim), BF16), pltpu.VMEM(yg.shape, BF16),
                        dma((n + 1,)), dma((n + 1,))],
        compiler_params=pltpu.CompilerParams(vmem_limit_bytes=60 << 20),
    )(ys, yg, gp)


def solution(mesh):
    n_dev = mesh.shape['sp']

    def shard_layer(hidden_in, w_query, w_key, w_value, w_out, w_up, w_down, rel_bias, glob_pos):
        dim = hidden_in.shape[1]
        heads, head = w_query.shape[1], w_query.shape[2]
        gp = glob_pos.reshape(1, -1)
        ys, yg = layer(hidden_in, w_query, w_key.reshape(dim, head), w_value.reshape(dim, head),
                       w_out.reshape(heads * head, dim), w_up, w_down, rel_bias, gp, n_dev)
        return place(ys, yg, gp)

    return jax.shard_map(
        shard_layer, mesh=mesh,
        in_specs=(P(('dp', 'sp'), None), P(), P(), P(), P(), P(), P(), P(), P('dp')),
        out_specs=(P(('dp', 'sp'), None), P('dp', None)),
        check_vma=False)
```
